8 devices in a mesh: dp: 2 (over z, y), tp: 4 (over x, core).
Axes of the slice: x: 2, y: 2, z: 1, core: 2. Of those that a mesh axis runs over, the one named last changes fastest.
Arguments:
- ids: int32 [4, 256], P('dp'), parts along dimension 0
- E: bfloat16 [32768, 2304], P('tp')
- g: bfloat16 [2304], replicated
- W: bfloat16 [2304, 4096], P(None, 'tp')
- du: bfloat16 [4, 256, 4096], P('dp', None, 'tp'), parts along dimension 0
- dres: bfloat16 [4, 256, 2304], P('dp', 'tp'), parts along dimension 0
Outputs:
- output 1: bfloat16 [4, 256, 4096], P('dp', None, 'tp'), parts along dimension 0
- output 2: bfloat16 [4, 256, 2304], P('dp', 'tp'), parts along dimension 0
- output 3: float32 [65536, 2304], P(('dp', 'tp')), parts along dimension 0
- output 4: float32 [4608, 4096], P('dp', 'tp'), parts along dimension 0
- output 5: float32 [4608], P('dp'), parts along dimension 0
There are 2 independent parts. The reference program is written for one: setup_inputs(seed, part) draws one part's arguments, and reference() takes and returns one part's arrays. A program takes and returns all parts, laid end to end along the dimension named above; an argument that names none is the same for every part.
All inputs are finite; a program needn't handle non-finite values.
Results may differ from the reference program's by a relative error of at most 0.00682878.
Values are sent between devices in bfloat16 or wider.
A program may use at most 1 GiB of HBM per device.

```python
import jax
import jax.numpy as jnp
from jax import lax

V = 32768
K = 2
T = 256
D = 2304
FC = 4096
TP = 4
NPOP = 256
EPS = 1e-6


def setup_inputs(seed: int = 0, part: int = 0) -> dict:
    key = jax.random.key(seed)
    kp = jax.random.fold_in(key, part)
    k1, k2, k3, k4, k5, k6 = jax.random.split(kp, 6)
    s1, s2, s3 = jax.random.split(key, 3)
    kd = jax.random.fold_in(kp, 7)
    d1, d2, d3, d4 = jax.random.split(kd, 4)
    vs = V // TP
    pop = jnp.arange(TP, dtype=jnp.int32) * vs + jax.random.randint(d1, (TP,), 0, vs, dtype=jnp.int32)
    pick = jax.random.randint(d2, (K, T), 0, TP, dtype=jnp.int32)
    uni = jax.random.randint(d3, (K, T), 0, V, dtype=jnp.int32)
    coin = jax.random.bernoulli(d4, 0.75, (K, T))
    ids = jnp.where(coin, pop[pick], uni).astype(jnp.int32)
    E = jax.random.normal(s1, (V, D), jnp.float32).astype(jnp.bfloat16)
    g = (1.0 + 0.4 * jax.random.normal(s2, (D,), jnp.float32)).astype(jnp.bfloat16)
    W = (jax.random.normal(s3, (D, FC), jnp.float32) * D ** -0.5).astype(jnp.bfloat16)
    du = jax.random.normal(k5, (K, T, FC), jnp.float32).astype(jnp.bfloat16)
    dres = jax.random.normal(k6, (K, T, D), jnp.float32).astype(jnp.bfloat16)
    return {"ids": ids, "E": E, "g": g, "W": W, "du": du, "dres": dres}


def reference(ids, E, g, W, du, dres):
    gf = g.astype(jnp.float32)
    fs = FC // TP
    wr = W.reshape(D, TP, fs).transpose(1, 0, 2)

    def micro(carry, inp):
        dE, dW, dg = carry
        idk, duk, dresk = inp
        x = jnp.take(E, idk, axis=0)
        xf = x.astype(jnp.float32)
        rs = lax.rsqrt(jnp.mean(xf * xf, axis=-1, keepdims=True) + EPS)
        nh = xf * rs
        n = (nh * gf).astype(jnp.bfloat16)
        u = jnp.dot(n, W, preferred_element_type=jnp.float32).astype(jnp.bfloat16)
        dur = duk.reshape(T, TP, fs).transpose(1, 0, 2)

        def add_block(acc, blk):
            dub, wb = blk
            pr = jnp.dot(dub, wb.T, preferred_element_type=jnp.float32)
            return acc + pr.astype(jnp.bfloat16).astype(jnp.float32), None

        dn, _ = lax.scan(add_block, jnp.zeros((T, D), jnp.float32), (dur, wr))
        gdn = gf * dn
        dx = dresk.astype(jnp.float32) + rs * (gdn - nh * jnp.mean(nh * gdn, axis=-1, keepdims=True))
        dxb = dx.astype(jnp.bfloat16).astype(jnp.float32)
        dE = dE.at[idk].add(dxb)
        dW = dW + jnp.dot(n.T, duk, preferred_element_type=jnp.float32)
        dg = dg + jnp.sum(dn * nh, axis=0)
        return (dE, dW, dg), (u, x)

    init = (jnp.zeros((V, D), jnp.float32), jnp.zeros((D, FC), jnp.float32), jnp.zeros((D,), jnp.float32))
    (dE, dW, dg), (u, x) = lax.scan(micro, init, (ids, du, dres))
    return u, x, dE, dW, dg
```

```python
import functools

import jax
import jax.numpy as jnp
from jax import lax
from jax.experimental import pallas as pl
from jax.experimental.pallas import tpu as pltpu
from jax.sharding import PartitionSpec as P


EPS = 1e-6
C = 64
G = 16
CB = 256
ZR = 128
Z1, Z2 = 24, 20
TB = 64

F32 = jnp.float32
BF16 = jnp.bfloat16
VMEM = pltpu.VMEM


def _sm():
    return pl.BlockSpec(memory_space=pltpu.SMEM)


def _vm():
    return pl.BlockSpec(memory_space=pltpu.VMEM)


def _any():
    return pl.BlockSpec(memory_space=pl.ANY)


def _params(mb):
    return pltpu.CompilerParams(vmem_limit_bytes=mb << 20)


def _cost(us):
    return pl.CostEstimate(flops=int(us * 4_000_000_000), bytes_accessed=1_000_000, transcendentals=0)


def _iota(shape, dim):
    return lax.broadcasted_iota(jnp.int32, shape, dim).astype(F32)


def _me():
    return lax.axis_index("tp").astype(jnp.int32)


def _index_kernel(vs, ntp, first, *refs):
    if first:
        ids_ref, e_ref, tab_ref, pos_ref, srow_ref, list_ref, cnt_ref, buf, glv, gls, gsem, sem = refs
        base = 0.0
    else:
        c_ref, ids_ref, e_ref, tab_ref, pos_ref, srow_ref, list_ref, cnt_ref, buf, glv, gls, gsem, sem = refs
        base = (c_ref[0] * C).astype(F32)
    mei = _me()
    me = mei.astype(F32)
    lo = me * vs
    nk, t = ids_ref.shape
    ntok = nk * t
    nb = ntok // TB
    idsf = ids_ref[...].astype(F32)
    idr = jnp.concatenate([idsf[k:k + 1] for k in range(nk)], axis=1)

    def column(row, b):
        w = (b * TB) // 128 * 128
        part = jnp.broadcast_to(row[:, w:w + 128], (TB, 128))
        hit = _iota((TB, 128), 1) == _iota((TB, 128), 0) + float(b * TB - w)
        return jnp.sum(jnp.where(hit, part, 0.0), axis=1, keepdims=True)

    def fold(a):
        return sum(a[8 * q:8 * q + 8] for q in range(1, TB // 8)) + a[:8]

    lane = _iota((TB, ntok), 1)
    thr = _iota((TB, 128), 1) * float(vs)
    rank8 = jnp.zeros((8, ntok), F32)
    below8 = jnp.zeros((8, 128), F32)
    idcs = []
    for b in range(nb):
        idc = column(idr, b)
        idcs.append(idc)
        idb = jnp.broadcast_to(idc, (TB, ntok))
        dup = (idb == idr) & (lane < _iota((TB, ntok), 0) + float(b * TB))
        seen = jnp.max(jnp.where(dup, 1.0, 0.0), axis=1, keepdims=True)
        key = jnp.where(seen > 0.5, float(vs * ntp), idc)
        rank8 = rank8 + fold(jnp.where(jnp.broadcast_to(key, (TB, ntok)) < idr, 1.0, 0.0))
        below8 = below8 + fold(jnp.where(jnp.broadcast_to(key, (TB, 128)) < thr, 1.0, 0.0))
    rank = jnp.sum(rank8, axis=0, keepdims=True)
    below = jnp.sum(below8, axis=0, keepdims=True)
    own_r = jnp.floor(idr * (1.0 / vs))
    start = jnp.zeros_like(rank)
    mine0 = jnp.zeros((1, 1), F32)
    cnt = jnp.zeros((1, 1), F32)
    mx = jnp.zeros((1, 1), F32)
    for d in range(ntp):
        ld = below[:, d:d + 1]
        nd = below[:, d + 1:d + 2] - ld
        start = jnp.where(own_r == float(d), ld, start)
        cnt = jnp.where(me == float(d), nd, cnt)
        mx = jnp.maximum(mx, nd)
    slot_r = rank - start
    my_r = jnp.where(own_r == me, slot_r, -1.0)

    slot_l = _iota((TB, 128), 1) + base
    acc = jnp.zeros((TB, 128), F32)
    mys = []
    for b in range(nb):
        my_c = column(my_r, b)
        mys.append(my_c)
        acc = jnp.maximum(acc, jnp.where(my_c == slot_l, idcs[b] - lo, 0.0))
    glv[...] = jnp.broadcast_to(jnp.max(acc, axis=0, keepdims=True), (8, 128)).astype(jnp.int32)
    cp = pltpu.make_async_copy(glv, gls, gsem)
    cp.start()
    cp.wait()

    def fetch(j, carry):
        g = pl.multiple_of((gls[0, j] // G) * G, G)
        pltpu.make_async_copy(e_ref.at[pl.ds(g, G)], buf.at[pl.ds(pl.multiple_of(j * G, G), G)], sem).start()
        return carry

    lax.fori_loop(0, C, fetch, 0, unroll=8)

    srow_ref[...] = my_r
    full = jnp.zeros((8, ntok), F32)
    lane8 = _iota((8, ntok), 1)
    for b in range(nb):
        for q in range(TB // 8):
            s = slice(8 * q, 8 * q + 8)
            full = jnp.maximum(full, jnp.where(mys[b][s] == lane8, idcs[b][s] - lo, 0.0))
    list_ref[...] = jnp.max(full, axis=0, keepdims=True).astype(jnp.int32)
    rel = (own_r.astype(jnp.int32) ^ mei).astype(F32)
    pos = jnp.where((slot_r >= base) & (slot_r < base + C), rel * C + slot_r - base, -1.0)
    for b in range(nb):
        pos_ref[b * TB:(b + 1) * TB, :] = column(pos, b)
    lane1 = lax.broadcasted_iota(jnp.int32, (1, 128), 1)
    cnt_ref[...] = jnp.where(lane1 == 0, mx, cnt).astype(jnp.int32)
    want = jnp.max(jnp.where(my_r == _iota((C, ntok), 0) + base, idr - lo, 0.0), axis=1, keepdims=True)
    want = want - jnp.floor(want * (1.0 / G)) * G + _iota((C, 1), 0) * G
    sel = jnp.where(_iota((C, C * G), 1) == want, 1.0, 0.0).astype(BF16)
    pltpu.make_async_copy(e_ref.at[pl.ds(0, C * G)], buf, sem).wait()
    for c in range(tab_ref.shape[1] // CB):
        s = slice(c * CB, (c + 1) * CB)
        tab_ref[:, s] = jnp.dot(sel, buf[:, s], preferred_element_type=F32).astype(BF16)


def _index_call(chunk, ids, E, ntp):
    vs, d = E.shape
    ntok = ids.shape[0] * ids.shape[1]
    first = chunk is None
    return pl.pallas_call(
        functools.partial(_index_kernel, vs, ntp, first),
        out_shape=(
            jax.ShapeDtypeStruct((C, d), BF16),
            jax.ShapeDtypeStruct((ntok, 1), F32),
            jax.ShapeDtypeStruct((1, ntok), F32),
            jax.ShapeDtypeStruct((1, ntok), jnp.int32),
            jax.ShapeDtypeStruct((1, 128), jnp.int32),
        ),
        in_specs=([] if first else [_sm()]) + [_vm(), pl.BlockSpec(memory_space=pltpu.HBM)],
        out_specs=(_vm(),) * 5,
        scratch_shapes=[
            VMEM((C * G, d), BF16),
            VMEM((8, 128), jnp.int32),
            pltpu.SMEM((8, 128), jnp.int32),
            pltpu.SemaphoreType.DMA,
            pltpu.SemaphoreType.DMA,
        ],
        compiler_params=_params(14),
        cost_estimate=_cost(5),
        name="index_gather",
    )(*([] if first else [chunk.reshape(1)]), ids, E)


def _expand_kernel(ts, acc, *refs):
    if acc:
        x_in, pos, t0, t1, t2, t3, x_out, xl_out = refs
    else:
        pos, t0, t1, t2, t3, x_out, xl_out = refs
    oh = jnp.where(pos[...] == _iota((pos.shape[0], 4 * C), 1), 1.0, 0.0).astype(BF16)
    for c in range(x_out.shape[1] // CB):
        s = slice(c * CB, (c + 1) * CB)
        tab = jnp.concatenate([t[:, s] for t in (t0, t1, t2, t3)], axis=0)
        tot = jnp.dot(oh, tab, preferred_element_type=F32)
        if acc:
            tot = tot + x_in[:, s].astype(F32)
        x_out[:, s] = tot.astype(BF16)
    t = 4 * ts
    for k in range(x_out.shape[0] // t):
        at = pl.multiple_of(k * t + _me() * ts, ts)
        xl_out[k] = x_out[pl.ds(at, ts), :]


def _expand(pos, tabs, ts, x=None):
    ntok, d = pos.shape[0], tabs[0].shape[1]
    ins = ([x] if x is not None else []) + [pos, *tabs]
    return pl.pallas_call(
        functools.partial(_expand_kernel, ts, x is not None),
        out_shape=(jax.ShapeDtypeStruct((ntok, d), BF16), jax.ShapeDtypeStruct((ntok // (4 * ts), ts, d), BF16)),
        in_specs=[_vm()] * len(ins),
        out_specs=(_vm(), _vm()),
        compiler_params=_params(12),
        cost_estimate=_cost(3),
        name="expand",
    )(*ins)


def _p_kernel(ts, du_ref, w_ref, *refs):
    outs, dur = refs[:-1], refs[-1]
    nk = du_ref.shape[0]

    @pl.when(pl.program_id(0) == 0)
    def _():
        for k in range(nk):
            for r in range(4):
                at = pl.multiple_of((_me() ^ r) * ts, ts)
                dur[pl.ds((k * 4 + r) * ts, ts), :] = du_ref[k, pl.ds(at, ts), :]

    out = lax.dot_general(dur[...], w_ref[...], (((1,), (1,)), ((), ())), preferred_element_type=F32)
    for i, o in enumerate(outs):
        o[...] = out[i * ts:(i + 1) * ts].astype(BF16)


def _p_terms(du, W, ts):
    nk, t, f = du.shape
    d = W.shape[0]
    cb = 3 * CB
    out = pl.pallas_call(
        functools.partial(_p_kernel, ts),
        out_shape=(jax.ShapeDtypeStruct((ts, d), BF16),) * (4 * nk),
        grid=(d // cb,),
        in_specs=[pl.BlockSpec((nk, t, f), lambda i: (0, 0, 0)), pl.BlockSpec((cb, f), lambda i: (i, 0))],
        out_specs=(pl.BlockSpec((ts, cb), lambda i: (0, i)),) * (4 * nk),
        scratch_shapes=[VMEM((nk * t, f), BF16)],
        compiler_params=_params(20),
        cost_estimate=_cost(5),
        name="p_terms",
    )(du, W)
    return [out[4 * k:4 * k + 4] for k in range(nk)]


def _fill(z, o, sems, lo, hi, wait):
    for i in range(lo, hi):
        c = pltpu.make_async_copy(z, o.at[pl.ds(i * ZR, ZR)], sems.at[i - lo])
        c.wait() if wait else c.start()


def _zero_kernel(lo, hi, de_in, o, z, sems):
    z[...] = jnp.zeros_like(z)
    _fill(z, o, sems, lo, hi, False)
    _fill(z, o, sems, lo, hi, True)


def _zeros(de, lo, hi):
    vs, d = de.shape
    return pl.pallas_call(
        functools.partial(_zero_kernel, lo, hi),
        out_shape=jax.ShapeDtypeStruct((vs, d), F32),
        in_specs=[_any()],
        out_specs=_any(),
        scratch_shapes=[VMEM((ZR, d), F32), pltpu.SemaphoreType.DMA((hi - lo,))],
        input_output_aliases={0: 0},
        compiler_params=_params(4),
        cost_estimate=_cost((hi - lo) * 0.375),
        name="zero_fill",
    )(de)


def _dx_kernel(x, p0, p1, p2, p3, dres, g, *refs):
    prev, (dx, dg) = refs[:-2], refs[-2:]
    xf = x[...].astype(F32)
    rs = lax.rsqrt(jnp.mean(xf * xf, axis=-1, keepdims=True) + EPS)
    nh = xf * rs
    dn = (p0[...].astype(F32) + p1[...].astype(F32)) + (p2[...].astype(F32) + p3[...].astype(F32))
    gdn = g[...].astype(F32) * dn
    out = dres[...].astype(F32) + rs * (gdn - nh * jnp.mean(nh * gdn, axis=-1, keepdims=True))
    dx[...] = out.astype(BF16)
    part = jnp.sum(dn * nh, axis=0, keepdims=True)
    dg[...] = part + prev[0][...] if prev else part


def _dx(x, ps, dres, g, k, prev):
    _, m, d = x.shape
    row = pl.BlockSpec((pl.Squeezed(), m, d), lambda i: (k, 0, 0))
    whole = lambda a: pl.BlockSpec(a.shape, lambda i: (0,) * a.ndim)
    return pl.pallas_call(
        _dx_kernel,
        out_shape=(jax.ShapeDtypeStruct((m, d), BF16), jax.ShapeDtypeStruct((1, d), F32)),
        grid=(1,),
        in_specs=[row, *map(whole, ps), row, whole(g), *map(whole, prev)],
        out_specs=(pl.BlockSpec((m, d), lambda i: (0, 0)), pl.BlockSpec((1, d), lambda i: (0, 0))),
        compiler_params=_params(12),
        cost_estimate=_cost(2),
        name="dx_form",
    )(x, *ps, dres, g, *prev)


def _u_kernel(zn, x_ref, g_ref, w_ref, *refs):
    u_ref, n_ref, de, z, sems = refs[-5:]
    z[...] = jnp.zeros_like(z)
    _fill(z, de, sems, 0, zn, False)
    rows = 64
    for b in range(n_ref.shape[0] // rows):
        s = slice(b * rows, (b + 1) * rows)
        xf = x_ref[s].astype(F32)
        rs = lax.rsqrt(jnp.mean(xf * xf, axis=-1, keepdims=True) + EPS)
        n_ref[s] = (xf * rs * g_ref[...].astype(F32)).astype(BF16)
    nk, t, f = u_ref.shape
    for c in range(f // CB):
        s = slice(c * CB, (c + 1) * CB)
        out = jnp.dot(n_ref[...], w_ref[:, s], preferred_element_type=F32).astype(BF16)
        for k in range(nk):
            u_ref[k, :, s] = out[k * t:(k + 1) * t]
    _fill(z, de, sems, 0, zn, True)


def _u(x, g, W, vs, nk, de):
    ntok, d = x.shape
    f = W.shape[1]
    return pl.pallas_call(
        functools.partial(_u_kernel, Z1),
        out_shape=(
            jax.ShapeDtypeStruct((nk, ntok // nk, f), BF16),
            jax.ShapeDtypeStruct((ntok, d), BF16),
            jax.ShapeDtypeStruct((vs, d), F32),
        ),
        in_specs=[_vm(), _vm(), _vm()] + [_any()] * len(de),
        out_specs=(_vm(), _vm(), _any()),
        scratch_shapes=[VMEM((ZR, d), F32), pltpu.SemaphoreType.DMA((Z1,))],
        input_output_aliases={3: 2} if de else {},
        compiler_params=_params(20),
        cost_estimate=_cost(10),
        name="u_terms",
    )(x, g, W, *de)


def _dw_kernel(lo, hi, n_ref, du_ref, de_in, dw_ref, de, z, sems):
    i = pl.program_id(0)
    nk, t, f = du_ref.shape

    @pl.when(i == 0)
    def _():
        z[...] = jnp.zeros_like(z)
        _fill(z, de, sems, lo, hi, False)

    dw_ref[...] = lax.dot_general(
        n_ref[...], du_ref[...].reshape(nk * t, f), (((0,), (0,)), ((), ())), preferred_element_type=F32
    )

    @pl.when(i == pl.num_programs(0) - 1)
    def _():
        _fill(z, de, sems, lo, hi, True)


def _dw(n, du, de, lo, hi):
    nk, t, f = du.shape
    ntok, d = n.shape
    return pl.pallas_call(
        functools.partial(_dw_kernel, lo, hi),
        out_shape=(jax.ShapeDtypeStruct((d, f), F32), jax.ShapeDtypeStruct(de.shape, F32)),
        grid=(d // CB,),
        in_specs=[
            pl.BlockSpec((ntok, CB), lambda i: (0, i)),
            pl.BlockSpec((nk, t, f), lambda i: (0, 0, 0)),
            _any(),
        ],
        out_specs=(pl.BlockSpec((CB, f), lambda i: (i, 0)), _any()),
        scratch_shapes=[VMEM((ZR, d), F32), pltpu.SemaphoreType.DMA((hi - lo,))],
        input_output_aliases={2: 1},
        compiler_params=_params(20),
        cost_estimate=_cost(10),
        name="dw_terms",
    )(n, du, de)


def _scatter_kernel(ts, nk, cnt_ref, list_ref, srow_ref, *refs):
    pieces, (de_in, de, dx, acc, sem) = refs[:-5], refs[-5:]
    ntok = nk * 4 * ts
    for k in range(nk):
        for r in range(4):
            at = pl.multiple_of(k * 4 * ts + (_me() ^ r) * ts, ts)
            dx[pl.ds(at, ts), :] = pieces[k * 4 + r][...]
    cnt = cnt_ref[0, 1]

    def chunk(i, carry):
        base = i * C
        slot = (lax.broadcasted_iota(jnp.int32, (C, ntok), 0) + base).astype(F32)
        oh = jnp.where(slot == srow_ref[...], 1.0, 0.0).astype(BF16)
        for c in range(acc.shape[1] // CB):
            s = slice(c * CB, (c + 1) * CB)
            acc[:, s] = jnp.dot(oh, dx[:, s], preferred_element_type=F32)
        here = jnp.minimum(cnt - base, C)

        def put(j, c2):
            row = list_ref[0, base + j]
            pltpu.make_async_copy(acc.at[pl.ds(j, 1)], de.at[pl.ds(row, 1)], sem).start()
            return c2

        def done(j, c2):
            pltpu.make_async_copy(acc.at[pl.ds(j, 1)], de.at[pl.ds(0, 1)], sem).wait()
            return c2

        lax.fori_loop(0, here, put, 0)
        lax.fori_loop(0, here, done, 0)
        return carry

    lax.fori_loop(0, (cnt + C - 1) // C, chunk, 0)


def _scatter(cnts, rows, srow, pieces, de, ts, nk):
    vs, d = de.shape
    ntok = srow.shape[1]
    return pl.pallas_call(
        functools.partial(_scatter_kernel, ts, nk),
        out_shape=jax.ShapeDtypeStruct((vs, d), F32),
        in_specs=[_sm(), _sm(), _vm()] + [_vm()] * len(pieces) + [_any()],
        out_specs=_any(),
        scratch_shapes=[VMEM((ntok, d), BF16), VMEM((C, d), F32), pltpu.SemaphoreType.DMA],
        input_output_aliases={3 + len(pieces): 0},
        compiler_params=_params(16),
        cost_estimate=_cost(3),
        name="scatter_rows",
    )(cnts, rows, srow, *pieces, de)


def solution(mesh):
    ntp = mesh.shape["tp"]
    ndp = mesh.shape["dp"]

    def swap(a, bit):
        return lax.ppermute(a, "tp", [(i, i ^ bit) for i in range(ntp)])

    def share(t):
        t2 = swap(t, 2)
        t1 = swap(t, 1)
        return t, t1, t2, swap(t2, 1)

    def p_terms(du, W, ts):
        ps = _p_terms(du, W, ts)
        return [(q[0], swap(q[1], 1), swap(q[2], 2), swap(q[3], 3)) for q in ps]

    def finish(x, xl, ps, g2, W, du, dres, cnts, rows, srow, vs, de):
        nk, ts, d = xl.shape
        nz = vs // ZR
        u, n, de = _u(x, g2, W, vs, nk, de)
        dx0, dg0 = _dx(xl, ps[0], dres, g2, 0, ())
        de = _zeros(de, Z1, Z1 + Z2)
        dx1, dgp = _dx(xl, ps[1], dres, g2, 1, (dg0,))
        pieces = share(dx0) + share(dx1)
        dW, de = _dw(n, du, de, Z1 + Z2, nz)
        dg = ((dgp + swap(dgp, 1)) + (swap(dgp, 2) + swap(dgp, 3))).reshape(d)
        dE = _scatter(cnts, rows, srow, pieces, de, ts, nk)
        return u, xl, dE, dW, dg

    def body(ids, E, g, W, du, dres):
        vs, d = E.shape
        ts = ids.shape[1] // ntp
        g2 = g.reshape(1, d)

        tab, pos, srow, rows, cnts = _index_call(None, ids, E, ntp)
        tabs = share(tab)
        ps = p_terms(du, W, ts)
        other = lax.ppermute(cnts, "dp", [(i, (i + 1) % ndp) for i in range(ndp)])
        x, xl = _expand(pos, tabs, ts)
        outs = finish(x, xl, ps, g2, W, du, dres, cnts, rows, srow, vs, ())
        rounds = (jnp.maximum(cnts[0, 0], other[0, 0]) + C - 1) // C

        inputs = ids, E, W, du, dres, g2

        def again(c):
            once, (_, _, de, _, _) = c
            ids, E, W, du, dres, g2, once = lax.optimization_barrier((*inputs, once))

            def more(q):
                i, x, _ = q
                tab, pos, _, _, _ = _index_call(i, ids, E, ntp)
                return i + 1, *_expand(pos, share(tab), ts, x)

            zeros = jnp.zeros(x.shape, BF16), jnp.zeros(xl.shape, BF16)
            _, xa, xla = lax.while_loop(lambda q: q[0] < rounds, more, (jnp.int32(0), *zeros))
            _, _, srow, rows, cnts = _index_call(once - 1, ids, E, ntp)
            return rounds, finish(xa, xla, p_terms(du, W, ts), g2, W, du, dres, cnts, rows, srow, vs, (de,))

        _, outs = lax.while_loop(lambda c: c[0] < rounds, again, (jnp.int32(1), outs))
        return outs

    return jax.shard_map(
        body,
        mesh=mesh,
        in_specs=(P("dp", None), P("tp", None), P(None), P(None, "tp"), P("dp", None, "tp"), P("dp", "tp", None)),
        out_specs=(P("dp", None, "tp"), P("dp", "tp", None), P(("dp", "tp"), None), P("dp", "tp"), P("dp")),
        check_vma=False,
    )
```

```python
import functools

import jax
import jax.numpy as jnp
from jax import lax
from jax.experimental import pallas as pl
from jax.experimental.pallas import tpu as pltpu
from jax.sharding import PartitionSpec as P


EPS = 1e-6
C = 64
G = 16
GS = 16
CB = 256
ZR = 128
ZP, ZU, ZZ = 8, 16, 24
TB = 64

F32 = jnp.float32
BF16 = jnp.bfloat16
VMEM = pltpu.VMEM


def _sm():
    return pl.BlockSpec(memory_space=pltpu.SMEM)


def _vm():
    return pl.BlockSpec(memory_space=pltpu.VMEM)


def _any():
    return pl.BlockSpec(memory_space=pl.ANY)


def _params(mb):
    return pltpu.CompilerParams(vmem_limit_bytes=mb << 20)


def _cost(us):
    return pl.CostEstimate(flops=int(us * 4_000_000_000), bytes_accessed=1_000_000, transcendentals=0)


def _iota(shape, dim):
    return lax.broadcasted_iota(jnp.int32, shape, dim).astype(F32)


def _me():
    return lax.axis_index("tp").astype(jnp.int32)


def _index_kernel(vs, ntp, first, *refs):
    if first:
        ids_ref, e_ref, tab_ref, pos_ref, srow_ref, list_ref, cnt_ref, buf, glv, gls, gsem, sems = refs
        base = 0.0
    else:
        c_ref, ids_ref, e_ref, tab_ref, pos_ref, srow_ref, list_ref, cnt_ref, buf, glv, gls, gsem, sems = refs
        base = (c_ref[0] * C).astype(F32)
    mei = _me()
    me = mei.astype(F32)
    lo = me * vs
    nk, t = ids_ref.shape
    ntok = nk * t
    nb = ntok // TB
    idsf = ids_ref[...].astype(F32)
    idr = jnp.concatenate([idsf[k:k + 1] for k in range(nk)], axis=1)

    def column(row, b):
        w = (b * TB) // 128 * 128
        part = jnp.broadcast_to(row[:, w:w + 128], (TB, 128))
        hit = _iota((TB, 128), 1) == _iota((TB, 128), 0) + float(b * TB - w)
        return jnp.sum(jnp.where(hit, part, 0.0), axis=1, keepdims=True)

    def fold(a):
        return sum(a[8 * q:8 * q + 8] for q in range(1, TB // 8)) + a[:8]

    lane = _iota((TB, ntok), 1)
    thr = _iota((TB, 128), 1) * float(vs)
    rank8 = jnp.zeros((8, ntok), F32)
    below8 = jnp.zeros((8, 128), F32)
    idcs = []
    for b in range(nb):
        idc = column(idr, b)
        idcs.append(idc)
        idb = jnp.broadcast_to(idc, (TB, ntok))
        dup = (idb == idr) & (lane < _iota((TB, ntok), 0) + float(b * TB))
        seen = jnp.max(jnp.where(dup, 1.0, 0.0), axis=1, keepdims=True)
        key = jnp.where(seen > 0.5, float(vs * ntp), idc)
        rank8 = rank8 + fold(jnp.where(jnp.broadcast_to(key, (TB, ntok)) < idr, 1.0, 0.0))
        below8 = below8 + fold(jnp.where(jnp.broadcast_to(key, (TB, 128)) < thr, 1.0, 0.0))
    rank = jnp.sum(rank8, axis=0, keepdims=True)
    below = jnp.sum(below8, axis=0, keepdims=True)
    own_r = jnp.floor(idr * (1.0 / vs))
    start = jnp.zeros_like(rank)
    mine0 = jnp.zeros((1, 1), F32)
    cnt = jnp.zeros((1, 1), F32)
    mx = jnp.zeros((1, 1), F32)
    for d in range(ntp):
        ld = below[:, d:d + 1]
        nd = below[:, d + 1:d + 2] - ld
        start = jnp.where(own_r == float(d), ld, start)
        cnt = jnp.where(me == float(d), nd, cnt)
        mx = jnp.maximum(mx, nd)
    slot_r = rank - start
    my_r = jnp.where(own_r == me, slot_r, -1.0)

    slot_l = _iota((TB, 128), 1) + base
    acc = jnp.zeros((TB, 128), F32)
    mys = []
    for b in range(nb):
        my_c = column(my_r, b)
        mys.append(my_c)
        acc = jnp.maximum(acc, jnp.where(my_c == slot_l, idcs[b] - lo, 0.0))
    glv[...] = jnp.broadcast_to(jnp.max(acc, axis=0, keepdims=True), (8, 128)).astype(jnp.int32)
    cp = pltpu.make_async_copy(glv, gls, gsem)
    cp.start()
    cp.wait()

    def fetch(q, j, carry):
        j = q * GS + j
        g = pl.multiple_of((gls[0, j] >> 4) << 4, G)
        at = pl.multiple_of(j * G, G)
        pltpu.make_async_copy(e_ref.at[pl.ds(g, G)], buf.at[pl.ds(at, G)], sems.at[q]).start()
        return carry

    for q in range(C // GS):
        lax.fori_loop(0, GS, functools.partial(fetch, q), 0, unroll=8)

    srow_ref[...] = my_r
    full = jnp.zeros((8, ntok), F32)
    lane8 = _iota((8, ntok), 1)
    for b in range(nb):
        for q in range(TB // 8):
            s = slice(8 * q, 8 * q + 8)
            full = jnp.maximum(full, jnp.where(mys[b][s] == lane8, idcs[b][s] - lo, 0.0))
    list_ref[...] = jnp.max(full, axis=0, keepdims=True).astype(jnp.int32)
    rel = (own_r.astype(jnp.int32) ^ mei).astype(F32)
    pos = jnp.where((slot_r >= base) & (slot_r < base + C), rel * C + slot_r - base, -1.0)
    for b in range(nb):
        pos_ref[b * TB:(b + 1) * TB, :] = column(pos, b)
    lane1 = lax.broadcasted_iota(jnp.int32, (1, 128), 1)
    cnt_ref[...] = jnp.where(lane1 == 0, mx, cnt).astype(jnp.int32)
    hit = jnp.where(my_r == _iota((C, ntok), 0) + base, idr - lo, 0.0)
    want = jnp.max(hit, axis=1, keepdims=True)
    want = want - jnp.floor(want * (1.0 / G)) * G
    for q in range(C // GS):
        r = slice(q * GS * G, (q + 1) * GS * G)
        mine = want[q * GS:(q + 1) * GS] + _iota((GS, 1), 0) * G
        sel = jnp.where(_iota((GS, GS * G), 1) == mine, 1.0, 0.0).astype(BF16)
        pltpu.make_async_copy(e_ref.at[pl.ds(0, GS * G)], buf.at[r], sems.at[q]).wait()
        tab_ref[q * GS:(q + 1) * GS, :] = jnp.dot(sel, buf[r, :], preferred_element_type=F32).astype(BF16)


def _index_call(chunk, ids, E, ntp):
    vs, d = E.shape
    ntok = ids.shape[0] * ids.shape[1]
    first = chunk is None
    return pl.pallas_call(
        functools.partial(_index_kernel, vs, ntp, first),
        out_shape=(
            jax.ShapeDtypeStruct((C, d), BF16),
            jax.ShapeDtypeStruct((ntok, 1), F32),
            jax.ShapeDtypeStruct((1, ntok), F32),
            jax.ShapeDtypeStruct((1, ntok), jnp.int32),
            jax.ShapeDtypeStruct((1, 128), jnp.int32),
        ),
        in_specs=([] if first else [_sm()]) + [_vm(), pl.BlockSpec(memory_space=pltpu.HBM)],
        out_specs=(_vm(),) * 5,
        scratch_shapes=[
            VMEM((C * G, d), BF16),
            VMEM((8, 128), jnp.int32),
            pltpu.SMEM((8, 128), jnp.int32),
            pltpu.SemaphoreType.DMA,
            pltpu.SemaphoreType.DMA((C // GS,)),
        ],
        compiler_params=_params(14),
        cost_estimate=_cost(5),
        name="index_gather",
    )(*([] if first else [chunk.reshape(1)]), ids, E)


def _expand_kernel(ts, acc, *refs):
    if acc:
        x_in, pos, t0, t1, t2, t3, x_out, xl_out = refs
    else:
        pos, t0, t1, t2, t3, x_out, xl_out = refs
    oh = jnp.where(pos[...] == _iota((pos.shape[0], 4 * C), 1), 1.0, 0.0).astype(BF16)
    for c in range(x_out.shape[1] // CB):
        s = slice(c * CB, (c + 1) * CB)
        tab = jnp.concatenate([t[:, s] for t in (t0, t1, t2, t3)], axis=0)
        tot = jnp.dot(oh, tab, preferred_element_type=F32)
        if acc:
            tot = tot + x_in[:, s].astype(F32)
        x_out[:, s] = tot.astype(BF16)
    t = 4 * ts
    for k in range(x_out.shape[0] // t):
        at = pl.multiple_of(k * t + _me() * ts, ts)
        xl_out[k] = x_out[pl.ds(at, ts), :]


def _expand(pos, tabs, ts, x=None):
    ntok, d = pos.shape[0], tabs[0].shape[1]
    ins = ([x] if x is not None else []) + [pos, *tabs]
    return pl.pallas_call(
        functools.partial(_expand_kernel, ts, x is not None),
        out_shape=(jax.ShapeDtypeStruct((ntok, d), BF16), jax.ShapeDtypeStruct((ntok // (4 * ts), ts, d), BF16)),
        in_specs=[_vm()] * len(ins),
        out_specs=(_vm(), _vm()),
        compiler_params=_params(12),
        cost_estimate=_cost(3),
        name="expand",
    )(*ins)


def _fill(z, o, sems, lo, first, n, wait):
    def step(i, carry):
        at = pl.multiple_of((lo + i) * ZR, ZR)
        c = pltpu.make_async_copy(z, o.at[pl.ds(at, ZR)], sems.at[i])
        c.wait() if wait else c.start()
        return carry

    lax.fori_loop(first, first + n, step, 0)


def _zscratch(d, n):
    return [VMEM((ZR, d), F32), pltpu.SemaphoreType.DMA((n,))]


def _p_kernel(ts, du_ref, w_ref, *refs):
    outs, (de, dur, z, sems) = refs[:-4], refs[-4:]
    nk = du_ref.shape[0]

    @pl.when(pl.program_id(0) == 0)
    def _():
        z[...] = jnp.zeros_like(z)
        for k in range(nk):
            for r in range(4):
                at = pl.multiple_of((_me() ^ r) * ts, ts)
                dur[pl.ds((k * 4 + r) * ts, ts), :] = du_ref[k, pl.ds(at, ts), :]
        _fill(z, de, sems, 0, 0, ZP, False)

    out = lax.dot_general(dur[...], w_ref[...], (((1,), (1,)), ((), ())), preferred_element_type=F32)
    for i, o in enumerate(outs):
        o[...] = out[i * ts:(i + 1) * ts].astype(BF16)

    @pl.when(pl.program_id(0) == pl.num_programs(0) - 1)
    def _():
        _fill(z, de, sems, 0, 0, ZP, True)


def _p_terms(du, W, ts, vs):
    nk, t, f = du.shape
    d = W.shape[0]
    cb = 3 * CB
    out = pl.pallas_call(
        functools.partial(_p_kernel, ts),
        out_shape=(jax.ShapeDtypeStruct((ts, d), BF16),) * (4 * nk) + (jax.ShapeDtypeStruct((vs, d), F32),),
        grid=(d // cb,),
        in_specs=[pl.BlockSpec((nk, t, f), lambda i: (0, 0, 0)), pl.BlockSpec((cb, f), lambda i: (i, 0))],
        out_specs=(pl.BlockSpec((ts, cb), lambda i: (0, i)),) * (4 * nk) + (_any(),),
        scratch_shapes=[VMEM((nk * t, f), BF16)] + _zscratch(d, ZP),
        compiler_params=_params(20),
        cost_estimate=_cost(5),
        name="p_terms",
    )(du, W)
    return [out[4 * k:4 * k + 4] for k in range(nk)], out[-1]


def _zero_kernel(lo, n, de_in, o, z, sems):
    z[...] = jnp.zeros_like(z)
    _fill(z, o, sems, lo, 0, n, False)
    _fill(z, o, sems, lo, 0, n, True)


def _zeros(de, lo, n):
    vs, d = de.shape
    return pl.pallas_call(
        functools.partial(_zero_kernel, lo, n),
        out_shape=jax.ShapeDtypeStruct((vs, d), F32),
        in_specs=[_any()],
        out_specs=_any(),
        scratch_shapes=_zscratch(d, n),
        input_output_aliases={0: 0},
        compiler_params=_params(4),
        cost_estimate=_cost(n * 0.375),
        name="zero_fill",
    )(de)


def _dx_kernel(x, p0, p1, p2, p3, dres, g, *refs):
    prev, (dx, dg) = refs[:-2], refs[-2:]
    xf = x[...].astype(F32)
    rs = lax.rsqrt(jnp.mean(xf * xf, axis=-1, keepdims=True) + EPS)
    nh = xf * rs
    dn = (p0[...].astype(F32) + p1[...].astype(F32)) + (p2[...].astype(F32) + p3[...].astype(F32))
    gdn = g[...].astype(F32) * dn
    out = dres[...].astype(F32) + rs * (gdn - nh * jnp.mean(nh * gdn, axis=-1, keepdims=True))
    dx[...] = out.astype(BF16)
    part = jnp.sum(dn * nh, axis=0, keepdims=True)
    dg[...] = part + prev[0][...] if prev else part


def _dx(x, ps, dres, g, k, prev):
    _, m, d = x.shape
    row = pl.BlockSpec((pl.Squeezed(), m, d), lambda i: (k, 0, 0))
    whole = lambda a: pl.BlockSpec(a.shape, lambda i: (0,) * a.ndim)
    return pl.pallas_call(
        _dx_kernel,
        out_shape=(jax.ShapeDtypeStruct((m, d), BF16), jax.ShapeDtypeStruct((1, d), F32)),
        grid=(1,),
        in_specs=[row, *map(whole, ps), row, whole(g), *map(whole, prev)],
        out_specs=(pl.BlockSpec((m, d), lambda i: (0, 0)), pl.BlockSpec((1, d), lambda i: (0, 0))),
        compiler_params=_params(12),
        cost_estimate=_cost(2),
        name="dx_form",
    )(x, *ps, dres, g, *prev)


def _u_kernel(x_ref, g_ref, w_ref, de_in, u_ref, n_ref, de, z, sems):
    z[...] = jnp.zeros_like(z)
    _fill(z, de, sems, ZP, 0, ZU, False)
    rows = 64
    for b in range(n_ref.shape[0] // rows):
        s = slice(b * rows, (b + 1) * rows)
        xf = x_ref[s].astype(F32)
        rs = lax.rsqrt(jnp.mean(xf * xf, axis=-1, keepdims=True) + EPS)
        n_ref[s] = (xf * rs * g_ref[...].astype(F32)).astype(BF16)
    nk, t, f = u_ref.shape
    for c in range(f // CB):
        s = slice(c * CB, (c + 1) * CB)
        out = jnp.dot(n_ref[...], w_ref[:, s], preferred_element_type=F32).astype(BF16)
        for k in range(nk):
            u_ref[k, :, s] = out[k * t:(k + 1) * t]
    _fill(z, de, sems, ZP, 0, ZU, True)


def _u(x, g, W, nk, de):
    ntok, d = x.shape
    f = W.shape[1]
    return pl.pallas_call(
        _u_kernel,
        out_shape=(
            jax.ShapeDtypeStruct((nk, ntok // nk, f), BF16),
            jax.ShapeDtypeStruct((ntok, d), BF16),
            jax.ShapeDtypeStruct(de.shape, F32),
        ),
        in_specs=[_vm(), _vm(), _vm(), _any()],
        out_specs=(_vm(), _vm(), _any()),
        scratch_shapes=_zscratch(d, ZU),
        input_output_aliases={3: 2},
        compiler_params=_params(20),
        cost_estimate=_cost(10),
        name="u_terms",
    )(x, g, W, de)


def _dw_kernel(lo, n, per, n_ref, du_ref, de_in, dw_ref, de, z, sems):
    i = pl.program_id(0)
    nk, t, f = du_ref.shape

    @pl.when(i == 0)
    def _():
        z[...] = jnp.zeros_like(z)

    _fill(z, de, sems, lo, i * per, jnp.minimum(per, n - i * per), False)
    dw_ref[...] = lax.dot_general(
        n_ref[...], du_ref[...].reshape(nk * t, f), (((0,), (0,)), ((), ())), preferred_element_type=F32
    )

    @pl.when(i == pl.num_programs(0) - 1)
    def _():
        _fill(z, de, sems, lo, 0, n, True)


def _dw(n, du, de, lo, nz):
    nk, t, f = du.shape
    ntok, d = n.shape
    steps = d // CB
    return pl.pallas_call(
        functools.partial(_dw_kernel, lo, nz, -(-nz // steps)),
        out_shape=(jax.ShapeDtypeStruct((d, f), F32), jax.ShapeDtypeStruct(de.shape, F32)),
        grid=(steps,),
        in_specs=[
            pl.BlockSpec((ntok, CB), lambda i: (0, i)),
            pl.BlockSpec((nk, t, f), lambda i: (0, 0, 0)),
            _any(),
        ],
        out_specs=(pl.BlockSpec((CB, f), lambda i: (i, 0)), _any()),
        scratch_shapes=_zscratch(d, nz),
        input_output_aliases={2: 1},
        compiler_params=_params(20),
        cost_estimate=_cost(10),
        name="dw_terms",
    )(n, du, de)


def _scatter_kernel(ts, nk, cnt_ref, list_ref, srow_ref, *refs):
    pieces, (de_in, de, dx, acc, sem) = refs[:-5], refs[-5:]
    ntok = nk * 4 * ts
    for k in range(nk):
        for r in range(4):
            at = pl.multiple_of(k * 4 * ts + (_me() ^ r) * ts, ts)
            dx[pl.ds(at, ts), :] = pieces[k * 4 + r][...]
    cnt = cnt_ref[0, 1]

    def chunk(i, carry):
        base = i * C
        slot = (lax.broadcasted_iota(jnp.int32, (C, ntok), 0) + base).astype(F32)
        oh = jnp.where(slot == srow_ref[...], 1.0, 0.0).astype(BF16)
        for c in range(acc.shape[1] // CB):
            s = slice(c * CB, (c + 1) * CB)
            acc[:, s] = jnp.dot(oh, dx[:, s], preferred_element_type=F32)
        here = jnp.minimum(cnt - base, C)

        def put(j, c2):
            row = list_ref[0, base + j]
            pltpu.make_async_copy(acc.at[pl.ds(j, 1)], de.at[pl.ds(row, 1)], sem).start()
            return c2

        def done(j, c2):
            pltpu.make_async_copy(acc.at[pl.ds(j, 1)], de.at[pl.ds(0, 1)], sem).wait()
            return c2

        lax.fori_loop(0, here, put, 0)
        lax.fori_loop(0, here, done, 0)
        return carry

    lax.fori_loop(0, (cnt + C - 1) // C, chunk, 0)


def _scatter(cnts, rows, srow, pieces, de, ts, nk):
    vs, d = de.shape
    ntok = srow.shape[1]
    return pl.pallas_call(
        functools.partial(_scatter_kernel, ts, nk),
        out_shape=jax.ShapeDtypeStruct((vs, d), F32),
        in_specs=[_sm(), _sm(), _vm()] + [_vm()] * len(pieces) + [_any()],
        out_specs=_any(),
        scratch_shapes=[VMEM((ntok, d), BF16), VMEM((C, d), F32), pltpu.SemaphoreType.DMA],
        input_output_aliases={3 + len(pieces): 0},
        compiler_params=_params(16),
        cost_estimate=_cost(3),
        name="scatter_rows",
    )(cnts, rows, srow, *pieces, de)


def solution(mesh):
    ntp = mesh.shape["tp"]
    ndp = mesh.shape["dp"]

    def swap(a, bit):
        return lax.ppermute(a, "tp", [(i, i ^ bit) for i in range(ntp)])

    def share(t):
        t2 = swap(t, 2)
        t1 = swap(t, 1)
        return t, t1, t2, swap(t2, 1)

    def p_terms(du, W, ts, vs):
        ps, de = _p_terms(du, W, ts, vs)
        return de, [(q[0], swap(q[1], 1), swap(q[2], 2), swap(q[3], 3)) for q in ps]

    def finish(x, xl, de_ps, g2, W, du, dres, cnts, rows, srow):
        nk, ts, d = xl.shape
        de, ps = de_ps
        u, n, de = _u(x, g2, W, nk, de)
        dx0, dg0 = _dx(xl, ps[0], dres, g2, 0, ())
        de = _zeros(de, ZP + ZU, ZZ)
        dx1, dgp = _dx(xl, ps[1], dres, g2, 1, (dg0,))
        pieces = share(dx0) + share(dx1)
        done = ZP + ZU + ZZ
        dW, de = _dw(n, du, de, done, de.shape[0] // ZR - done)
        dg = ((dgp + swap(dgp, 1)) + (swap(dgp, 2) + swap(dgp, 3))).reshape(d)
        dE = _scatter(cnts, rows, srow, pieces, de, ts, nk)
        return u, xl, dE, dW, dg

    def body(ids, E, g, W, du, dres):
        vs, d = E.shape
        ts = ids.shape[1] // ntp
        g2 = g.reshape(1, d)

        tab, pos, srow, rows, cnts = _index_call(None, ids, E, ntp)
        tabs = share(tab)
        de_ps = p_terms(du, W, ts, vs)
        other = lax.ppermute(cnts, "dp", [(i, (i + 1) % ndp) for i in range(ndp)])
        x, xl = _expand(pos, tabs, ts)
        outs = finish(x, xl, de_ps, g2, W, du, dres, cnts, rows, srow)
        rounds = (jnp.maximum(cnts[0, 0], other[0, 0]) + C - 1) // C

        inputs = ids, E, W, du, dres, g2

        def again(c):
            once, _ = c
            ids, E, W, du, dres, g2, once = lax.optimization_barrier((*inputs, once))

            def more(q):
                i, x, _ = q
                tab, pos, _, _, _ = _index_call(i, ids, E, ntp)
                return i + 1, *_expand(pos, share(tab), ts, x)

            zeros = jnp.zeros(x.shape, BF16), jnp.zeros(xl.shape, BF16)
            _, xa, xla = lax.while_loop(lambda q: q[0] < rounds, more, (jnp.int32(0), *zeros))
            _, _, srow, rows, cnts = _index_call(once - 1, ids, E, ntp)
            return rounds, finish(xa, xla, p_terms(du, W, ts, vs), g2, W, du, dres, cnts, rows, srow)

        _, outs = lax.while_loop(lambda c: c[0] < rounds, again, (jnp.int32(1), outs))
        return outs

    return jax.shard_map(
        body,
        mesh=mesh,
        in_specs=(P("dp", None), P("tp", None), P(None), P(None, "tp"), P("dp", None, "tp"), P("dp", "tp", None)),
        out_specs=(P("dp", None, "tp"), P("dp", "tp", None), P(("dp", "tp"), None), P("dp", "tp"), P("dp")),
        check_vma=False,
    )
```

```python
import functools

import jax
import jax.numpy as jnp
from jax import lax
from jax.experimental import pallas as pl
from jax.experimental.pallas import tpu as pltpu
from jax.sharding import PartitionSpec as P


EPS = 1e-6
C = 64
G = 16
GS = 16
C2 = 32
CB = 256
ZR = 128
ZP, ZU, ZW = 8, 14, 22
TB = 64

F32 = jnp.float32
BF16 = jnp.bfloat16
VMEM = pltpu.VMEM


def _sm():
    return pl.BlockSpec(memory_space=pltpu.SMEM)


def _vm():
    return pl.BlockSpec(memory_space=pltpu.VMEM)


def _any():
    return pl.BlockSpec(memory_space=pl.ANY)


def _params(mb):
    return pltpu.CompilerParams(vmem_limit_bytes=mb << 20)


def _cost(us):
    return pl.CostEstimate(flops=int(us * 4_000_000_000), bytes_accessed=1_000_000, transcendentals=0)


def _iota(shape, dim):
    return lax.broadcasted_iota(jnp.int32, shape, dim).astype(F32)


def _me():
    return lax.axis_index("tp").astype(jnp.int32)


def _index_kernel(vs, ntp, first, *refs):
    if first:
        ids_ref, e_ref, tab_ref, pos_ref, srow_ref, list_ref, cnt_ref, slot_ref, map_ref, buf, glv, gls, gsem, sems = refs
        base = 0.0
    else:
        c_ref, ids_ref, e_ref, tab_ref, pos_ref, srow_ref, list_ref, cnt_ref, slot_ref, map_ref, buf, glv, gls, gsem, sems = refs
        base = (c_ref[0] * C).astype(F32)
    mei = _me()
    me = mei.astype(F32)
    lo = me * vs
    nk, t = ids_ref.shape
    ntok = nk * t
    nb = ntok // TB
    idsf = ids_ref[...].astype(F32)
    idr = jnp.concatenate([idsf[k:k + 1] for k in range(nk)], axis=1)

    def column(row, b):
        w = (b * TB) // 128 * 128
        part = jnp.broadcast_to(row[:, w:w + 128], (TB, 128))
        hit = _iota((TB, 128), 1) == _iota((TB, 128), 0) + float(b * TB - w)
        return jnp.sum(jnp.where(hit, part, 0.0), axis=1, keepdims=True)

    def fold(a):
        return sum(a[8 * q:8 * q + 8] for q in range(1, TB // 8)) + a[:8]

    lane = _iota((TB, ntok), 1)
    ts = t // ntp
    part = lax.broadcasted_iota(jnp.int32, (1, ntok), 1) // ts % ntp
    chips = [jnp.where(part // 2 == c, 1.0, 0.0) for c in range(ntp // 2)]
    thr = _iota((TB, 128), 1) * float(vs)
    rank8 = jnp.zeros((8, ntok), F32)
    below8 = jnp.zeros((8, 128), F32)
    rank28 = jnp.zeros((8, ntok), F32)
    below28 = [jnp.zeros((8, 128), F32) for _ in chips]
    idcs = []
    for b in range(nb):
        idc = column(idr, b)
        idcs.append(idc)
        idb = jnp.broadcast_to(idc, (TB, ntok))
        dup = (idb == idr) & (lane < _iota((TB, ntok), 0) + float(b * TB))
        seen = jnp.max(jnp.where(dup, 1.0, 0.0), axis=1, keepdims=True)
        key = jnp.where(seen > 0.5, float(vs * ntp), idc)
        rank8 = rank8 + fold(jnp.where(jnp.broadcast_to(key, (TB, ntok)) < idr, 1.0, 0.0))
        below8 = below8 + fold(jnp.where(jnp.broadcast_to(key, (TB, 128)) < thr, 1.0, 0.0))
        c = b * TB // ts % ntp // 2
        seen = jnp.max(jnp.where(dup, chips[c], 0.0), axis=1, keepdims=True)
        key = jnp.where(seen > 0.5, float(vs * ntp), idc)
        rank28 = rank28 + fold(jnp.where(jnp.broadcast_to(key, (TB, ntok)) < idr, chips[c], 0.0))
        below28[c] = below28[c] + fold(jnp.where(jnp.broadcast_to(key, (TB, 128)) < thr, 1.0, 0.0))
    rank = jnp.sum(rank8, axis=0, keepdims=True)
    below = jnp.sum(below8, axis=0, keepdims=True)
    own_r = jnp.floor(idr * (1.0 / vs))
    start = jnp.zeros_like(rank)
    cnt = jnp.zeros((1, 1), F32)
    mx = jnp.zeros((1, 1), F32)
    for d in range(ntp):
        ld = below[:, d:d + 1]
        nd = below[:, d + 1:d + 2] - ld
        start = jnp.where(own_r == float(d), ld, start)
        cnt = jnp.where(me == float(d), nd, cnt)
        mx = jnp.maximum(mx, nd)
    slot_r = rank - start
    rank2 = jnp.sum(rank28, axis=0, keepdims=True)
    below2 = [jnp.sum(b8, axis=0, keepdims=True) for b8 in below28]
    start2 = jnp.zeros_like(rank)
    cnt2 = jnp.zeros((1, 1), F32)
    mx2 = jnp.zeros((1, 1), F32)
    for c, chip in enumerate(chips):
        for d in range(ntp):
            ld = below2[c][:, d:d + 1]
            nd = below2[c][:, d + 1:d + 2] - ld
            start2 = jnp.where((own_r == float(d)) & (chip > 0.5), ld, start2)
            if d // 2 != c:
                cnt2 = jnp.where(me == float(d), nd, cnt2)
                mx2 = jnp.maximum(mx2, nd)
    slot2_r = rank2 - start2
    my_r = jnp.where(own_r == me, slot_r, -1.0)

    slot_l = _iota((TB, 128), 1) + base
    acc = jnp.zeros((TB, 128), F32)
    mys = []
    for b in range(nb):
        my_c = column(my_r, b)
        mys.append(my_c)
        acc = jnp.maximum(acc, jnp.where(my_c == slot_l, idcs[b] - lo, 0.0))
    glv[...] = jnp.broadcast_to(jnp.max(acc, axis=0, keepdims=True), (8, 128)).astype(jnp.int32)
    cp = pltpu.make_async_copy(glv, gls, gsem)
    cp.start()
    cp.wait()

    def fetch(q, j, carry):
        j = q * GS + j
        g = pl.multiple_of((gls[0, j] >> 4) << 4, G)
        at = pl.multiple_of(j * G, G)
        pltpu.make_async_copy(e_ref.at[pl.ds(g, G)], buf.at[pl.ds(at, G)], sems.at[q]).start()
        return carry

    for q in range(C // GS):
        lax.fori_loop(0, GS, functools.partial(fetch, q), 0, unroll=8)

    srow_ref[...] = my_r
    full = jnp.zeros((8, ntok), F32)
    lane8 = _iota((8, ntok), 1)
    for b in range(nb):
        for q in range(TB // 8):
            s = slice(8 * q, 8 * q + 8)
            full = jnp.maximum(full, jnp.where(mys[b][s] == lane8, idcs[b][s] - lo, 0.0))
    list_ref[...] = jnp.max(full, axis=0, keepdims=True).astype(jnp.int32)
    rel = (own_r.astype(jnp.int32) ^ mei).astype(F32)
    pos = jnp.where((slot_r >= base) & (slot_r < base + C), rel * C + slot_r - base, -1.0)
    for b in range(nb):
        pos_ref[b * TB:(b + 1) * TB, :] = column(pos, b)
    lane1 = lax.broadcasted_iota(jnp.int32, (1, 128), 1)
    over = jnp.where((mx > C) | (mx2 > C2 - 1), 1.0, 0.0)
    cnts = jnp.where(lane1 == 0, mx, jnp.where(lane1 == 1, cnt, jnp.where(lane1 == 2, over, cnt2)))
    cnt_ref[...] = cnts.astype(jnp.int32)
    facing = (mei ^ 2).astype(F32)
    sums_r = jnp.where(own_r == facing, slot2_r, -1.0)
    rows = [jnp.zeros((1, nk * ts), F32)] * 4
    for q in range(ntp):
        at = [slice(k * t + q * ts, k * t + (q + 1) * ts) for k in range(nk)]
        mine = jnp.concatenate([my_r[:, w] for w in at], axis=1)
        sums = jnp.concatenate([sums_r[:, w] for w in at], axis=1)
        own, sib = me == float(q), me == float(q ^ 1)
        rows = [
            jnp.where(own, mine, rows[0]), jnp.where(sib, mine, rows[1]),
            jnp.where(own, sums, rows[2]), jnp.where(sib, sums, rows[3]),
        ]
    for j, r in enumerate(rows):
        slot_ref[j:j + 1, :] = r
    far = (part // 2).astype(F32) != jnp.floor(me * 0.5)
    got_r = jnp.where(far & (own_r == me), slot2_r, -1.0)
    acc2 = jnp.zeros((TB, 128), F32)
    slot_j = _iota((TB, 128), 1)
    for b in range(nb):
        acc2 = jnp.maximum(acc2, jnp.where(column(got_r, b) == slot_j, mys[b], 0.0))
    map_ref[...] = jnp.minimum(jnp.max(acc2, axis=0, keepdims=True), C - 1.0).astype(jnp.int32)
    hit = jnp.where(my_r == _iota((C, ntok), 0) + base, idr - lo, 0.0)
    want = jnp.max(hit, axis=1, keepdims=True)
    want = want - jnp.floor(want * (1.0 / G)) * G
    for q in range(C // GS):
        r = slice(q * GS * G, (q + 1) * GS * G)
        mine = want[q * GS:(q + 1) * GS] + _iota((GS, 1), 0) * G
        sel = jnp.where(_iota((GS, GS * G), 1) == mine, 1.0, 0.0).astype(BF16)
        pltpu.make_async_copy(e_ref.at[pl.ds(0, GS * G)], buf.at[r], sems.at[q]).wait()
        tab_ref[q * GS:(q + 1) * GS, :] = jnp.dot(sel, buf[r, :], preferred_element_type=F32).astype(BF16)


def _index_call(chunk, ids, E, ntp):
    vs, d = E.shape
    ntok = ids.shape[0] * ids.shape[1]
    first = chunk is None
    return pl.pallas_call(
        functools.partial(_index_kernel, vs, ntp, first),
        out_shape=(
            jax.ShapeDtypeStruct((C, d), BF16),
            jax.ShapeDtypeStruct((ntok, 1), F32),
            jax.ShapeDtypeStruct((1, ntok), F32),
            jax.ShapeDtypeStruct((1, ntok), jnp.int32),
            jax.ShapeDtypeStruct((1, 128), jnp.int32),
            jax.ShapeDtypeStruct((4, ntok // ntp), F32),
            jax.ShapeDtypeStruct((1, 128), jnp.int32),
        ),
        in_specs=([] if first else [_sm()]) + [_vm(), pl.BlockSpec(memory_space=pltpu.HBM)],
        out_specs=(_vm(),) * 7,
        scratch_shapes=[
            VMEM((C * G, d), BF16),
            VMEM((8, 128), jnp.int32),
            pltpu.SMEM((8, 128), jnp.int32),
            pltpu.SemaphoreType.DMA,
            pltpu.SemaphoreType.DMA((C // GS,)),
        ],
        compiler_params=_params(14),
        cost_estimate=_cost(5),
        name="index_gather",
    )(*([] if first else [chunk.reshape(1)]), ids, E)


def _expand_kernel(ts, acc, *refs):
    if acc:
        x_in, pos, t0, t1, t2, t3, x_out, xl_out = refs
    else:
        pos, t0, t1, t2, t3, x_out, xl_out = refs
    oh = jnp.where(pos[...] == _iota((pos.shape[0], 4 * C), 1), 1.0, 0.0).astype(BF16)
    for c in range(x_out.shape[1] // CB):
        s = slice(c * CB, (c + 1) * CB)
        tab = jnp.concatenate([t[:, s] for t in (t0, t1, t2, t3)], axis=0)
        tot = jnp.dot(oh, tab, preferred_element_type=F32)
        if acc:
            tot = tot + x_in[:, s].astype(F32)
        x_out[:, s] = tot.astype(BF16)
    t = 4 * ts
    for k in range(x_out.shape[0] // t):
        at = pl.multiple_of(k * t + _me() * ts, ts)
        xl_out[k] = x_out[pl.ds(at, ts), :]


def _expand(pos, tabs, ts, x=None):
    ntok, d = pos.shape[0], tabs[0].shape[1]
    ins = ([x] if x is not None else []) + [pos, *tabs]
    return pl.pallas_call(
        functools.partial(_expand_kernel, ts, x is not None),
        out_shape=(jax.ShapeDtypeStruct((ntok, d), BF16), jax.ShapeDtypeStruct((ntok // (4 * ts), ts, d), BF16)),
        in_specs=[_vm()] * len(ins),
        out_specs=(_vm(), _vm()),
        compiler_params=_params(12),
        cost_estimate=_cost(3),
        name="expand",
    )(*ins)


def _fill(z, o, sems, lo, first, n, wait):
    def step(i, carry):
        at = pl.multiple_of((lo + i) * ZR, ZR)
        c = pltpu.make_async_copy(z, o.at[pl.ds(at, ZR)], sems.at[i])
        c.wait() if wait else c.start()
        return carry

    lax.fori_loop(first, first + n, step, 0)


def _zscratch(d, n):
    return [VMEM((ZR, d), F32), pltpu.SemaphoreType.DMA((n,))]


def _p_kernel(ts, du_ref, w_ref, *refs):
    outs, (de, dur, z, sems) = refs[:-4], refs[-4:]
    nk = du_ref.shape[0]

    @pl.when(pl.program_id(0) == 0)
    def _():
        z[...] = jnp.zeros_like(z)
        for k in range(nk):
            for r in range(4):
                at = pl.multiple_of((_me() ^ r) * ts, ts)
                dur[pl.ds((r * nk + k) * ts, ts), :] = du_ref[k, pl.ds(at, ts), :]
        _fill(z, de, sems, 0, 0, ZP, False)

    out = lax.dot_general(dur[...], w_ref[...], (((1,), (1,)), ((), ())), preferred_element_type=F32)
    for i, o in enumerate(outs):
        o[...] = out[i * nk * ts:(i + 1) * nk * ts].astype(BF16)

    @pl.when(pl.program_id(0) == pl.num_programs(0) - 1)
    def _():
        _fill(z, de, sems, 0, 0, ZP, True)


def _p_terms(du, W, ts, vs):
    nk, t, f = du.shape
    d = W.shape[0]
    cb = 3 * CB
    out = pl.pallas_call(
        functools.partial(_p_kernel, ts),
        out_shape=(jax.ShapeDtypeStruct((nk * ts, d), BF16),) * 4 + (jax.ShapeDtypeStruct((vs, d), F32),),
        grid=(d // cb,),
        in_specs=[pl.BlockSpec((nk, t, f), lambda i: (0, 0, 0)), pl.BlockSpec((cb, f), lambda i: (i, 0))],
        out_specs=(pl.BlockSpec((nk * ts, cb), lambda i: (0, i)),) * 4 + (_any(),),
        scratch_shapes=[VMEM((nk * t, f), BF16)] + _zscratch(d, ZP),
        compiler_params=_params(20),
        cost_estimate=_cost(5),
        name="p_terms",
    )(du, W)
    return out[:4], out[4]


def _zero_kernel(lo, n, de_in, o, z, sems):
    z[...] = jnp.zeros_like(z)
    _fill(z, o, sems, lo, 0, n, False)
    _fill(z, o, sems, lo, 0, n, True)


def _zeros(de, lo, n):
    vs, d = de.shape
    return pl.pallas_call(
        functools.partial(_zero_kernel, lo, n),
        out_shape=jax.ShapeDtypeStruct((vs, d), F32),
        in_specs=[_any()],
        out_specs=_any(),
        scratch_shapes=_zscratch(d, n),
        input_output_aliases={0: 0},
        compiler_params=_params(4),
        cost_estimate=_cost(n * 0.375),
        name="zero_fill",
    )(de)


def _dx_kernel(x, p0, p1, p2, p3, dres, g, dx, dg):
    rows = 32
    tot = None
    for b in range(dx.shape[0] // rows):
        s = slice(b * rows, (b + 1) * rows)
        xf = x[s].astype(F32)
        rs = lax.rsqrt(jnp.mean(xf * xf, axis=-1, keepdims=True) + EPS)
        nh = xf * rs
        dn = (p0[s].astype(F32) + p1[s].astype(F32)) + (p2[s].astype(F32) + p3[s].astype(F32))
        gdn = g[...].astype(F32) * dn
        out = dres[s].astype(F32) + rs * (gdn - nh * jnp.mean(nh * gdn, axis=-1, keepdims=True))
        dx[s] = out.astype(BF16)
        part = jnp.sum(dn * nh, axis=0, keepdims=True)
        tot = part if tot is None else tot + part
    dg[...] = tot


def _dx(x, ps, dres, g):
    m, d = x.shape
    return pl.pallas_call(
        _dx_kernel,
        out_shape=(jax.ShapeDtypeStruct((m, d), BF16), jax.ShapeDtypeStruct((1, d), F32)),
        in_specs=[_vm()] * 7,
        out_specs=(_vm(), _vm()),
        compiler_params=_params(12),
        cost_estimate=_cost(2),
        name="dx_form",
    )(x, *ps, dres, g)


def _sums_kernel(slot_ref, dx0, dx1, dg0, dg1, out):
    m = dx0.shape[0]
    j = _iota((C2, m), 0)
    ohs = [jnp.where(slot_ref[i:i + 1, :] == j, 1.0, 0.0).astype(BF16) for i in (2, 3)]
    last = lax.broadcasted_iota(jnp.int32, (C2, CB), 0) == C2 - 1
    for c in range(out.shape[1] // CB):
        s = slice(c * CB, (c + 1) * CB)
        tot = jnp.dot(ohs[0], dx0[:, s], preferred_element_type=F32)
        tot = tot + jnp.dot(ohs[1], dx1[:, s], preferred_element_type=F32)
        out[:, s] = jnp.where(last, dg0[:, s] + dg1[:, s], tot)


def _sums(slots, dx0, dx1, dg0, dg1):
    return pl.pallas_call(
        _sums_kernel,
        out_shape=jax.ShapeDtypeStruct((C2, dx0.shape[1]), F32),
        in_specs=[_vm()] * 5,
        out_specs=_vm(),
        compiler_params=_params(6),
        cost_estimate=_cost(1),
        name="dx_sums",
    )(slots, dx0, dx1, dg0, dg1)


def _u_kernel(x_ref, g_ref, w_ref, de_in, u_ref, n_ref, de, z, sems):
    z[...] = jnp.zeros_like(z)
    _fill(z, de, sems, ZP, 0, ZU, False)
    rows = 64
    for b in range(n_ref.shape[0] // rows):
        s = slice(b * rows, (b + 1) * rows)
        xf = x_ref[s].astype(F32)
        rs = lax.rsqrt(jnp.mean(xf * xf, axis=-1, keepdims=True) + EPS)
        n_ref[s] = (xf * rs * g_ref[...].astype(F32)).astype(BF16)
    nk, t, f = u_ref.shape
    for c in range(f // CB):
        s = slice(c * CB, (c + 1) * CB)
        out = jnp.dot(n_ref[...], w_ref[:, s], preferred_element_type=F32).astype(BF16)
        for k in range(nk):
            u_ref[k, :, s] = out[k * t:(k + 1) * t]
    _fill(z, de, sems, ZP, 0, ZU, True)


def _u(x, g, W, nk, de):
    ntok, d = x.shape
    f = W.shape[1]
    return pl.pallas_call(
        _u_kernel,
        out_shape=(
            jax.ShapeDtypeStruct((nk, ntok // nk, f), BF16),
            jax.ShapeDtypeStruct((ntok, d), BF16),
            jax.ShapeDtypeStruct(de.shape, F32),
        ),
        in_specs=[_vm(), _vm(), _vm(), _any()],
        out_specs=(_vm(), _vm(), _any()),
        scratch_shapes=_zscratch(d, ZU),
        input_output_aliases={3: 2},
        compiler_params=_params(20),
        cost_estimate=_cost(10),
        name="u_terms",
    )(x, g, W, de)


def _dw_kernel(lo, n, per, n_ref, du_ref, de_in, dw_ref, de, z, sems):
    i = pl.program_id(0)
    nk, t, f = du_ref.shape

    @pl.when(i == 0)
    def _():
        z[...] = jnp.zeros_like(z)

    _fill(z, de, sems, lo, i * per, jnp.minimum(per, n - i * per), False)
    dw_ref[...] = lax.dot_general(
        n_ref[...], du_ref[...].reshape(nk * t, f), (((0,), (0,)), ((), ())), preferred_element_type=F32
    )

    @pl.when(i == pl.num_programs(0) - 1)
    def _():
        _fill(z, de, sems, lo, 0, n, True)


def _dw(n, du, de, lo, nz):
    nk, t, f = du.shape
    ntok, d = n.shape
    cb = d // 6
    steps = d // cb
    return pl.pallas_call(
        functools.partial(_dw_kernel, lo, nz, -(-nz // steps)),
        out_shape=(jax.ShapeDtypeStruct((d, f), F32), jax.ShapeDtypeStruct(de.shape, F32)),
        grid=(steps,),
        in_specs=[
            pl.BlockSpec((ntok, cb), lambda i: (0, i)),
            pl.BlockSpec((nk, t, f), lambda i: (0, 0, 0)),
            _any(),
        ],
        out_specs=(pl.BlockSpec((cb, f), lambda i: (i, 0)), _any()),
        scratch_shapes=_zscratch(d, nz),
        input_output_aliases={2: 1},
        compiler_params=_params(20),
        cost_estimate=_cost(10),
        name="dw_terms",
    )(n, du, de)


def _scatter_kernel(ts, nk, cnt_ref, list_ref, srow_ref, *refs):
    pieces, (de_in, de, dx, acc, sem) = refs[:-5], refs[-5:]
    ntok = nk * 4 * ts
    for k in range(nk):
        for r in range(4):
            at = pl.multiple_of(k * 4 * ts + (_me() ^ r) * ts, ts)
            dx[pl.ds(at, ts), :] = pieces[r][k * ts:(k + 1) * ts, :]
    cnt = cnt_ref[0, 1]

    def chunk(i, carry):
        base = i * C
        slot = (lax.broadcasted_iota(jnp.int32, (C, ntok), 0) + base).astype(F32)
        oh = jnp.where(slot == srow_ref[...], 1.0, 0.0).astype(BF16)
        for c in range(acc.shape[1] // CB):
            s = slice(c * CB, (c + 1) * CB)
            acc[:, s] = jnp.dot(oh, dx[:, s], preferred_element_type=F32)
        here = jnp.minimum(cnt - base, C)

        def put(j, c2):
            row = list_ref[0, base + j]
            pltpu.make_async_copy(acc.at[pl.ds(j, 1)], de.at[pl.ds(row, 1)], sem).start()
            return c2

        def done(j, c2):
            pltpu.make_async_copy(acc.at[pl.ds(j, 1)], de.at[pl.ds(0, 1)], sem).wait()
            return c2

        lax.fori_loop(0, here, put, 0)
        lax.fori_loop(0, here, done, 0)
        return carry

    lax.fori_loop(0, (cnt + C - 1) // C, chunk, 0)


def _scatter(cnts, rows, srow, pieces, de, ts, nk):
    vs, d = de.shape
    ntok = srow.shape[1]
    return pl.pallas_call(
        functools.partial(_scatter_kernel, ts, nk),
        out_shape=jax.ShapeDtypeStruct((vs, d), F32),
        in_specs=[_sm(), _sm(), _vm()] + [_vm()] * len(pieces) + [_any()],
        out_specs=_any(),
        scratch_shapes=[VMEM((ntok, d), BF16), VMEM((C, d), F32), pltpu.SemaphoreType.DMA],
        input_output_aliases={3 + len(pieces): 0},
        compiler_params=_params(16),
        cost_estimate=_cost(3),
        name="scatter_rows",
    )(cnts, rows, srow, *pieces, de)


def _write_kernel(cnt_ref, list_ref, map_ref, slot_ref, dx0, dx1, dg_ref, mine_ref, got_ref, de_in, de, dg_out, acc, sem):
    m = dx0.shape[0]
    j = _iota((C, m), 0)
    ohs = [jnp.where(slot_ref[i:i + 1, :] == j, 1.0, 0.0).astype(BF16) for i in (0, 1)]
    for c in range(acc.shape[1] // CB):
        s = slice(c * CB, (c + 1) * CB)
        tot = jnp.dot(ohs[0], dx0[:, s], preferred_element_type=F32)
        acc[:, s] = tot + jnp.dot(ohs[1], dx1[:, s], preferred_element_type=F32)

    def add(j, carry):
        at = pl.ds(map_ref[0, j], 1)
        acc[at, :] = acc[at, :] + got_ref[pl.ds(j, 1), :]
        return carry

    lax.fori_loop(0, jnp.minimum(cnt_ref[0, 3], C2 - 1), add, 0)
    here = jnp.minimum(cnt_ref[0, 1], C)

    def put(j, carry):
        pltpu.make_async_copy(acc.at[pl.ds(j, 1)], de.at[pl.ds(list_ref[0, j], 1)], sem).start()
        return carry

    def done(j, carry):
        pltpu.make_async_copy(acc.at[pl.ds(j, 1)], de.at[pl.ds(0, 1)], sem).wait()
        return carry

    lax.fori_loop(0, here, put, 0)
    dg_out[...] = mine_ref[C2 - 1:C2, :] + got_ref[C2 - 1:C2, :]
    lax.fori_loop(0, here, done, 0)


def _write(cnts, rows, where, slots, dx0, dx1, dgp, mine, got, de):
    vs, d = de.shape
    return pl.pallas_call(
        _write_kernel,
        out_shape=(jax.ShapeDtypeStruct((vs, d), F32), jax.ShapeDtypeStruct((1, d), F32)),
        in_specs=[_sm(), _sm(), _sm()] + [_vm()] * 6 + [_any()],
        out_specs=(_any(), _vm()),
        scratch_shapes=[VMEM((C, d), F32), pltpu.SemaphoreType.DMA],
        input_output_aliases={9: 0},
        compiler_params=_params(8),
        cost_estimate=_cost(3),
        name="write_rows",
    )(cnts, rows, where, slots, dx0, dx1, dgp, mine, got, de)


def solution(mesh):
    ntp = mesh.shape["tp"]
    ndp = mesh.shape["dp"]

    def swap(a, bit):
        return lax.ppermute(a, "tp", [(i, i ^ bit) for i in range(ntp)])

    def share(t):
        t2 = swap(t, 2)
        t1 = swap(t, 1)
        return t, t1, t2, swap(t2, 1)

    def p_terms(du, W, ts, vs):
        q, de = _p_terms(du, W, ts, vs)
        return de, (q[0], swap(q[1], 1), swap(q[2], 2), swap(q[3], 3))

    def fill_rest(de):
        n = ZP + ZU + ZW
        return _zeros(de, n, de.shape[0] // ZR - n)

    def body(ids, E, g, W, du, dres):
        vs, d = E.shape
        nk, t = ids.shape
        ts = t // ntp
        m = nk * ts
        g2 = g.reshape(1, d)

        tab, pos, _, rows, cnts, slots, where = _index_call(None, ids, E, ntp)
        tabs = share(tab)
        de, ps = p_terms(du, W, ts, vs)
        x, xl = _expand(pos, tabs, ts)
        u, n, de = _u(x, g2, W, nk, de)
        dW, de = _dw(n, du, de, ZP + ZU, ZW)
        dx, dg = _dx(xl.reshape(m, d), ps, dres.reshape(m, d), g2)
        dx1, dg1 = swap(dx, 1), swap(dg, 1)
        mine = _sums(slots, dx, dx1, dg, dg1)
        got = swap(mine, 2)
        other = lax.ppermute(cnts, "dp", [(i, (i + 1) % ndp) for i in range(ndp)])
        de = fill_rest(de)
        dE, dg = _write(cnts, rows, where, slots, dx, dx1, dg, mine, got, de)
        outs = u, xl, dE, dW, dg.reshape(d)
        over = jnp.maximum(cnts[0, 2], other[0, 2])

        inputs = ids, E, W, du, dres, g2

        def again(c):
            i0, _ = c
            ids, E, W, du, dres, g2, i0 = lax.optimization_barrier((*inputs, c[0]))
            top = lax.ppermute(cnts, "dp", [(i, (i + 1) % ndp) for i in range(ndp)])
            rounds = (jnp.maximum(cnts[0, 0], top[0, 0]) + C - 1) // C

            def more(q):
                i, x, _ = q
                tab, pos, *_ = _index_call(i, ids, E, ntp)
                return i + 1, *_expand(pos, share(tab), ts, x)

            zeros = jnp.zeros((nk * t, d), BF16), jnp.zeros((nk, ts, d), BF16)
            _, x, xl = lax.while_loop(lambda q: q[0] < rounds, more, (i0, *zeros))
            _, _, srow, rows, cs, _, _ = _index_call(i0, ids, E, ntp)
            de, ps = p_terms(du, W, ts, vs)
            u, n, de = _u(x, g2, W, nk, de)
            dW, de = _dw(n, du, de, ZP + ZU, ZW)
            dx, dg = _dx(xl.reshape(m, d), ps, dres.reshape(m, d), g2)
            dg2 = dg + swap(dg, 1)
            dg = (dg2 + swap(dg2, 2)).reshape(d)
            dE = _scatter(cs, rows, srow, share(dx), fill_rest(de), ts, nk)
            return i0 + 1, (u, xl, dE, dW, dg)

        _, outs = lax.while_loop(lambda c: c[0] < over, again, (jnp.int32(0), outs))
        return outs

    return jax.shard_map(
        body,
        mesh=mesh,
        in_specs=(P("dp", None), P("tp", None), P(None), P(None, "tp"), P("dp", None, "tp"), P("dp", "tp", None)),
        out_specs=(P("dp", None, "tp"), P("dp", "tp", None), P(("dp", "tp"), None), P("dp", "tp"), P("dp")),
        check_vma=False,
    )
```

```python
import functools

import jax
import jax.numpy as jnp
from jax import lax
from jax.experimental import pallas as pl
from jax.experimental.pallas import tpu as pltpu
from jax.sharding import PartitionSpec as P


EPS = 1e-6
C = 64
G = 2
GS = 64
C2 = 32
CB = 256
ZR = 128
ZP, ZU, ZW = 8, 14, 22
TB = 64

F32 = jnp.float32
BF16 = jnp.bfloat16
VMEM = pltpu.VMEM


def _sm():
    return pl.BlockSpec(memory_space=pltpu.SMEM)


def _vm():
    return pl.BlockSpec(memory_space=pltpu.VMEM)


def _any():
    return pl.BlockSpec(memory_space=pl.ANY)


def _params(mb):
    return pltpu.CompilerParams(vmem_limit_bytes=mb << 20)


def _cost(us):
    return pl.CostEstimate(flops=int(us * 4_000_000_000), bytes_accessed=1_000_000, transcendentals=0)


def _iota(shape, dim):
    return lax.broadcasted_iota(jnp.int32, shape, dim).astype(F32)


def _me():
    return lax.axis_index("tp").astype(jnp.int32)


def _index_kernel(vs, ntp, first, *refs):
    if first:
        ids_ref, e_ref, tab_ref, pos_ref, srow_ref, list_ref, cnt_ref, slot_ref, map_ref, buf, glv, gls, gsem, sems = refs
        base = 0.0
    else:
        c_ref, ids_ref, e_ref, tab_ref, pos_ref, srow_ref, list_ref, cnt_ref, slot_ref, map_ref, buf, glv, gls, gsem, sems = refs
        base = (c_ref[0] * C).astype(F32)
    mei = _me()
    me = mei.astype(F32)
    lo = me * vs
    nk, t = ids_ref.shape
    ntok = nk * t
    nb = ntok // TB
    idsf = ids_ref[...].astype(F32)
    idr = jnp.concatenate([idsf[k:k + 1] for k in range(nk)], axis=1)

    def column(row, b):
        w = (b * TB) // 128 * 128
        part = jnp.broadcast_to(row[:, w:w + 128], (TB, 128))
        hit = _iota((TB, 128), 1) == _iota((TB, 128), 0) + float(b * TB - w)
        return jnp.sum(jnp.where(hit, part, 0.0), axis=1, keepdims=True)

    def fold(a):
        return sum(a[8 * q:8 * q + 8] for q in range(1, TB // 8)) + a[:8]

    lane = _iota((TB, ntok), 1)
    ts = t // ntp
    part = lax.broadcasted_iota(jnp.int32, (1, ntok), 1) // ts % ntp
    chips = [jnp.where(part // 2 == c, 1.0, 0.0) for c in range(ntp // 2)]
    thr = _iota((TB, 128), 1) * float(vs)
    rank8 = jnp.zeros((8, ntok), F32)
    below8 = jnp.zeros((8, 128), F32)
    rank28 = jnp.zeros((8, ntok), F32)
    below28 = [jnp.zeros((8, 128), F32) for _ in chips]
    idcs = []
    for b in range(nb):
        idc = column(idr, b)
        idcs.append(idc)
        idb = jnp.broadcast_to(idc, (TB, ntok))
        dup = (idb == idr) & (lane < _iota((TB, ntok), 0) + float(b * TB))
        seen = jnp.max(jnp.where(dup, 1.0, 0.0), axis=1, keepdims=True)
        key = jnp.where(seen > 0.5, float(vs * ntp), idc)
        rank8 = rank8 + fold(jnp.where(jnp.broadcast_to(key, (TB, ntok)) < idr, 1.0, 0.0))
        below8 = below8 + fold(jnp.where(jnp.broadcast_to(key, (TB, 128)) < thr, 1.0, 0.0))
        c = b * TB // ts % ntp // 2
        seen = jnp.max(jnp.where(dup, chips[c], 0.0), axis=1, keepdims=True)
        key = jnp.where(seen > 0.5, float(vs * ntp), idc)
        rank28 = rank28 + fold(jnp.where(jnp.broadcast_to(key, (TB, ntok)) < idr, chips[c], 0.0))
        below28[c] = below28[c] + fold(jnp.where(jnp.broadcast_to(key, (TB, 128)) < thr, 1.0, 0.0))
    rank = jnp.sum(rank8, axis=0, keepdims=True)
    below = jnp.sum(below8, axis=0, keepdims=True)
    own_r = jnp.floor(idr * (1.0 / vs))
    start = jnp.zeros_like(rank)
    cnt = jnp.zeros((1, 1), F32)
    mx = jnp.zeros((1, 1), F32)
    for d in range(ntp):
        ld = below[:, d:d + 1]
        nd = below[:, d + 1:d + 2] - ld
        start = jnp.where(own_r == float(d), ld, start)
        cnt = jnp.where(me == float(d), nd, cnt)
        mx = jnp.maximum(mx, nd)
    slot_r = rank - start
    rank2 = jnp.sum(rank28, axis=0, keepdims=True)
    below2 = [jnp.sum(b8, axis=0, keepdims=True) for b8 in below28]
    start2 = jnp.zeros_like(rank)
    cnt2 = jnp.zeros((1, 1), F32)
    mx2 = jnp.zeros((1, 1), F32)
    for c, chip in enumerate(chips):
        for d in range(ntp):
            ld = below2[c][:, d:d + 1]
            nd = below2[c][:, d + 1:d + 2] - ld
            start2 = jnp.where((own_r == float(d)) & (chip > 0.5), ld, start2)
            if d // 2 != c:
                cnt2 = jnp.where(me == float(d), nd, cnt2)
                mx2 = jnp.maximum(mx2, nd)
    slot2_r = rank2 - start2
    my_r = jnp.where(own_r == me, slot_r, -1.0)

    slot_l = _iota((TB, 128), 1) + base
    acc = jnp.zeros((TB, 128), F32)
    mys = []
    for b in range(nb):
        my_c = column(my_r, b)
        mys.append(my_c)
        acc = jnp.maximum(acc, jnp.where(my_c == slot_l, idcs[b] - lo, 0.0))
    glv[...] = jnp.broadcast_to(jnp.max(acc, axis=0, keepdims=True), (8, 128)).astype(jnp.int32)
    cp = pltpu.make_async_copy(glv, gls, gsem)
    cp.start()
    cp.wait()

    def fetch(q, j, carry):
        j = q * GS + j
        g = pl.multiple_of((gls[0, j] >> 1) << 1, G)
        at = pl.multiple_of(j * G, G)
        pltpu.make_async_copy(e_ref.at[pl.ds(g, G)], buf.at[pl.ds(at, G)], sems.at[q]).start()
        return carry

    for q in range(C // GS):
        lax.fori_loop(0, GS, functools.partial(fetch, q), 0, unroll=8)

    srow_ref[...] = my_r
    full = jnp.zeros((8, ntok), F32)
    lane8 = _iota((8, ntok), 1)
    for b in range(nb):
        for q in range(TB // 8):
            s = slice(8 * q, 8 * q + 8)
            full = jnp.maximum(full, jnp.where(mys[b][s] == lane8, idcs[b][s] - lo, 0.0))
    list_ref[...] = jnp.max(full, axis=0, keepdims=True).astype(jnp.int32)
    rel = (own_r.astype(jnp.int32) ^ mei).astype(F32)
    pos = jnp.where((slot_r >= base) & (slot_r < base + C), rel * C + slot_r - base, -1.0)
    for b in range(nb):
        pos_ref[b * TB:(b + 1) * TB, :] = column(pos, b)
    lane1 = lax.broadcasted_iota(jnp.int32, (1, 128), 1)
    over = jnp.where((mx > C) | (mx2 > C2 - 1), 1.0, 0.0)
    rounds = jnp.floor((mx + C - 1.0) * (1.0 / C))
    cnts = jnp.where(lane1 == 0, rounds, jnp.where(lane1 == 1, cnt, jnp.where(lane1 == 2, over, cnt2)))
    cnt_ref[...] = cnts.astype(jnp.int32)
    facing = (mei ^ 2).astype(F32)
    sums_r = jnp.where(own_r == facing, slot2_r, -1.0)
    rows = [jnp.zeros((1, nk * ts), F32)] * 4
    for q in range(ntp):
        at = [slice(k * t + q * ts, k * t + (q + 1) * ts) for k in range(nk)]
        mine = jnp.concatenate([my_r[:, w] for w in at], axis=1)
        sums = jnp.concatenate([sums_r[:, w] for w in at], axis=1)
        own, sib = me == float(q), me == float(q ^ 1)
        rows = [
            jnp.where(own, mine, rows[0]), jnp.where(sib, mine, rows[1]),
            jnp.where(own, sums, rows[2]), jnp.where(sib, sums, rows[3]),
        ]
    for j, r in enumerate(rows):
        slot_ref[j:j + 1, :] = r
    far = (part // 2).astype(F32) != jnp.floor(me * 0.5)
    got_r = jnp.where(far & (own_r == me), slot2_r, -1.0)
    acc2 = jnp.zeros((TB, 128), F32)
    slot_j = _iota((TB, 128), 1)
    for b in range(nb):
        acc2 = jnp.maximum(acc2, jnp.where(column(got_r, b) == slot_j, mys[b], 0.0))
    map_ref[...] = jnp.minimum(jnp.max(acc2, axis=0, keepdims=True), C - 1.0).astype(jnp.int32)
    hit = jnp.where(my_r == _iota((C, ntok), 0) + base, idr - lo, 0.0)
    want = jnp.max(hit, axis=1, keepdims=True)
    want = want - jnp.floor(want * (1.0 / G)) * G
    for q in range(C // GS):
        r = slice(q * GS * G, (q + 1) * GS * G)
        mine = want[q * GS:(q + 1) * GS] + _iota((GS, 1), 0) * G
        sel = jnp.where(_iota((GS, GS * G), 1) == mine, 1.0, 0.0).astype(BF16)
        pltpu.make_async_copy(e_ref.at[pl.ds(0, GS * G)], buf.at[r], sems.at[q]).wait()
        tab_ref[q * GS:(q + 1) * GS, :] = jnp.dot(sel, buf[r, :], preferred_element_type=F32).astype(BF16)


def _index_call(chunk, ids, E, ntp):
    vs, d = E.shape
    ntok = ids.shape[0] * ids.shape[1]
    first = chunk is None
    return pl.pallas_call(
        functools.partial(_index_kernel, vs, ntp, first),
        out_shape=(
            jax.ShapeDtypeStruct((C, d), BF16),
            jax.ShapeDtypeStruct((ntok, 1), F32),
            jax.ShapeDtypeStruct((1, ntok), F32),
            jax.ShapeDtypeStruct((1, ntok), jnp.int32),
            jax.ShapeDtypeStruct((1, 128), jnp.int32),
            jax.ShapeDtypeStruct((4, ntok // ntp), F32),
            jax.ShapeDtypeStruct((1, 128), jnp.int32),
        ),
        in_specs=([] if first else [_sm()]) + [_vm(), pl.BlockSpec(memory_space=pltpu.HBM)],
        out_specs=(_vm(),) * 7,
        scratch_shapes=[
            VMEM((C * G, d), BF16),
            VMEM((8, 128), jnp.int32),
            pltpu.SMEM((8, 128), jnp.int32),
            pltpu.SemaphoreType.DMA,
            pltpu.SemaphoreType.DMA((C // GS,)),
        ],
        compiler_params=_params(14),
        cost_estimate=_cost(5),
        name="index_gather",
    )(*([] if first else [chunk.reshape(1)]), ids, E)


def _expand_kernel(ts, acc, *refs):
    if acc:
        x_in, pos, t0, t1, t2, t3, x_out, xl_out = refs
    else:
        pos, t0, t1, t2, t3, x_out, xl_out = refs
    oh = jnp.where(pos[...] == _iota((pos.shape[0], 4 * C), 1), 1.0, 0.0).astype(BF16)
    for c in range(x_out.shape[1] // CB):
        s = slice(c * CB, (c + 1) * CB)
        tab = jnp.concatenate([t[:, s] for t in (t0, t1, t2, t3)], axis=0)
        tot = jnp.dot(oh, tab, preferred_element_type=F32)
        if acc:
            tot = tot + x_in[:, s].astype(F32)
        x_out[:, s] = tot.astype(BF16)
    t = 4 * ts
    for k in range(x_out.shape[0] // t):
        at = pl.multiple_of(k * t + _me() * ts, ts)
        xl_out[k] = x_out[pl.ds(at, ts), :]


def _expand(pos, tabs, ts, x=None):
    ntok, d = pos.shape[0], tabs[0].shape[1]
    ins = ([x] if x is not None else []) + [pos, *tabs]
    return pl.pallas_call(
        functools.partial(_expand_kernel, ts, x is not None),
        out_shape=(jax.ShapeDtypeStruct((ntok, d), BF16), jax.ShapeDtypeStruct((ntok // (4 * ts), ts, d), BF16)),
        in_specs=[_vm()] * len(ins),
        out_specs=(_vm(), _vm()),
        compiler_params=_params(12),
        cost_estimate=_cost(3),
        name="expand",
    )(*ins)


def _fill(z, o, sems, lo, first, n, wait):
    def step(i, carry):
        at = pl.multiple_of((lo + i) * ZR, ZR)
        c = pltpu.make_async_copy(z, o.at[pl.ds(at, ZR)], sems.at[i])
        c.wait() if wait else c.start()
        return carry

    lax.fori_loop(first, first + n, step, 0)


def _zscratch(d, n):
    return [VMEM((ZR, d), F32), pltpu.SemaphoreType.DMA((n,))]


def _p_kernel(ts, du_ref, w_ref, *refs):
    outs, (de, dur, z, sems) = refs[:-4], refs[-4:]
    nk = du_ref.shape[0]

    @pl.when(pl.program_id(0) == 0)
    def _():
        z[...] = jnp.zeros_like(z)
        for k in range(nk):
            for r in range(4):
                at = pl.multiple_of((_me() ^ r) * ts, ts)
                dur[pl.ds((r * nk + k) * ts, ts), :] = du_ref[k, pl.ds(at, ts), :]
        _fill(z, de, sems, 0, 0, ZP, False)

    out = lax.dot_general(dur[...], w_ref[...], (((1,), (1,)), ((), ())), preferred_element_type=F32)
    for i, o in enumerate(outs):
        o[...] = out[i * nk * ts:(i + 1) * nk * ts].astype(BF16)

    @pl.when(pl.program_id(0) == pl.num_programs(0) - 1)
    def _():
        _fill(z, de, sems, 0, 0, ZP, True)


def _p_terms(du, W, ts, vs):
    nk, t, f = du.shape
    d = W.shape[0]
    cb = 3 * CB
    out = pl.pallas_call(
        functools.partial(_p_kernel, ts),
        out_shape=(jax.ShapeDtypeStruct((nk * ts, d), BF16),) * 4 + (jax.ShapeDtypeStruct((vs, d), F32),),
        grid=(d // cb,),
        in_specs=[pl.BlockSpec((nk, t, f), lambda i: (0, 0, 0)), pl.BlockSpec((cb, f), lambda i: (i, 0))],
        out_specs=(pl.BlockSpec((nk * ts, cb), lambda i: (0, i)),) * 4 + (_any(),),
        scratch_shapes=[VMEM((nk * t, f), BF16)] + _zscratch(d, ZP),
        compiler_params=_params(20),
        cost_estimate=_cost(5),
        name="p_terms",
    )(du, W)
    return out[:4], out[4]


def _zero_kernel(lo, n, de_in, o, z, sems):
    z[...] = jnp.zeros_like(z)
    _fill(z, o, sems, lo, 0, n, False)
    _fill(z, o, sems, lo, 0, n, True)


def _zeros(de, lo, n):
    vs, d = de.shape
    return pl.pallas_call(
        functools.partial(_zero_kernel, lo, n),
        out_shape=jax.ShapeDtypeStruct((vs, d), F32),
        in_specs=[_any()],
        out_specs=_any(),
        scratch_shapes=_zscratch(d, n),
        input_output_aliases={0: 0},
        compiler_params=_params(4),
        cost_estimate=_cost(n * 0.375),
        name="zero_fill",
    )(de)


def _dx_kernel(x, p0, p1, p2, p3, dres, g, dx, dg):
    rows = 32
    tot = None
    for b in range(dx.shape[0] // rows):
        s = slice(b * rows, (b + 1) * rows)
        xf = x[s].astype(F32)
        rs = lax.rsqrt(jnp.mean(xf * xf, axis=-1, keepdims=True) + EPS)
        nh = xf * rs
        dn = (p0[s].astype(F32) + p1[s].astype(F32)) + (p2[s].astype(F32) + p3[s].astype(F32))
        gdn = g[...].astype(F32) * dn
        out = dres[s].astype(F32) + rs * (gdn - nh * jnp.mean(nh * gdn, axis=-1, keepdims=True))
        dx[s] = out.astype(BF16)
        part = jnp.sum(dn * nh, axis=0, keepdims=True)
        tot = part if tot is None else tot + part
    dg[...] = tot


def _dx(x, ps, dres, g):
    m, d = x.shape
    return pl.pallas_call(
        _dx_kernel,
        out_shape=(jax.ShapeDtypeStruct((m, d), BF16), jax.ShapeDtypeStruct((1, d), F32)),
        in_specs=[_vm()] * 7,
        out_specs=(_vm(), _vm()),
        compiler_params=_params(12),
        cost_estimate=_cost(2),
        name="dx_form",
    )(x, *ps, dres, g)


def _sums_kernel(slot_ref, dx0, dx1, dg0, dg1, out):
    m = dx0.shape[0]
    j = _iota((C2, m), 0)
    ohs = [jnp.where(slot_ref[i:i + 1, :] == j, 1.0, 0.0).astype(BF16) for i in (2, 3)]
    last = lax.broadcasted_iota(jnp.int32, (C2, CB), 0) == C2 - 1
    for c in range(out.shape[1] // CB):
        s = slice(c * CB, (c + 1) * CB)
        tot = jnp.dot(ohs[0], dx0[:, s], preferred_element_type=F32)
        tot = tot + jnp.dot(ohs[1], dx1[:, s], preferred_element_type=F32)
        out[:, s] = jnp.where(last, dg0[:, s] + dg1[:, s], tot)


def _sums(slots, dx0, dx1, dg0, dg1):
    return pl.pallas_call(
        _sums_kernel,
        out_shape=jax.ShapeDtypeStruct((C2, dx0.shape[1]), F32),
        in_specs=[_vm()] * 5,
        out_specs=_vm(),
        compiler_params=_params(6),
        cost_estimate=_cost(1),
        name="dx_sums",
    )(slots, dx0, dx1, dg0, dg1)


def _u_kernel(x_ref, g_ref, w_ref, de_in, u_ref, n_ref, de, z, sems):
    z[...] = jnp.zeros_like(z)
    _fill(z, de, sems, ZP, 0, ZU, False)
    rows = 64
    for b in range(n_ref.shape[0] // rows):
        s = slice(b * rows, (b + 1) * rows)
        xf = x_ref[s].astype(F32)
        rs = lax.rsqrt(jnp.mean(xf * xf, axis=-1, keepdims=True) + EPS)
        n_ref[s] = (xf * rs * g_ref[...].astype(F32)).astype(BF16)
    nk, t, f = u_ref.shape
    for c in range(f // CB):
        s = slice(c * CB, (c + 1) * CB)
        out = jnp.dot(n_ref[...], w_ref[:, s], preferred_element_type=F32).astype(BF16)
        for k in range(nk):
            u_ref[k, :, s] = out[k * t:(k + 1) * t]
    _fill(z, de, sems, ZP, 0, ZU, True)


def _u(x, g, W, nk, de):
    ntok, d = x.shape
    f = W.shape[1]
    return pl.pallas_call(
        _u_kernel,
        out_shape=(
            jax.ShapeDtypeStruct((nk, ntok // nk, f), BF16),
            jax.ShapeDtypeStruct((ntok, d), BF16),
            jax.ShapeDtypeStruct(de.shape, F32),
        ),
        in_specs=[_vm(), _vm(), _vm(), _any()],
        out_specs=(_vm(), _vm(), _any()),
        scratch_shapes=_zscratch(d, ZU),
        input_output_aliases={3: 2},
        compiler_params=_params(20),
        cost_estimate=_cost(10),
        name="u_terms",
    )(x, g, W, de)


def _dw_kernel(lo, n, per, n_ref, du_ref, de_in, dw_ref, de, z, sems):
    i = pl.program_id(0)
    nk, t, f = du_ref.shape

    @pl.when(i == 0)
    def _():
        z[...] = jnp.zeros_like(z)

    _fill(z, de, sems, lo, i * per, jnp.minimum(per, n - i * per), False)
    dw_ref[...] = lax.dot_general(
        n_ref[...], du_ref[...].reshape(nk * t, f), (((0,), (0,)), ((), ())), preferred_element_type=F32
    )

    @pl.when(i == pl.num_programs(0) - 1)
    def _():
        _fill(z, de, sems, lo, 0, n, True)


def _dw(n, du, de, lo, nz):
    nk, t, f = du.shape
    ntok, d = n.shape
    cb = d // 6
    steps = d // cb
    return pl.pallas_call(
        functools.partial(_dw_kernel, lo, nz, -(-nz // steps)),
        out_shape=(jax.ShapeDtypeStruct((d, f), F32), jax.ShapeDtypeStruct(de.shape, F32)),
        grid=(steps,),
        in_specs=[
            pl.BlockSpec((ntok, cb), lambda i: (0, i)),
            pl.BlockSpec((nk, t, f), lambda i: (0, 0, 0)),
            _any(),
        ],
        out_specs=(pl.BlockSpec((cb, f), lambda i: (i, 0)), _any()),
        scratch_shapes=_zscratch(d, nz),
        input_output_aliases={2: 1},
        compiler_params=_params(20),
        cost_estimate=_cost(10),
        name="dw_terms",
    )(n, du, de)


def _scatter_kernel(ts, nk, cnt_ref, list_ref, srow_ref, *refs):
    pieces, (de_in, de, dx, acc, sem) = refs[:-5], refs[-5:]
    ntok = nk * 4 * ts
    for k in range(nk):
        for r in range(4):
            at = pl.multiple_of(k * 4 * ts + (_me() ^ r) * ts, ts)
            dx[pl.ds(at, ts), :] = pieces[r][k * ts:(k + 1) * ts, :]
    cnt = cnt_ref[0, 1]

    def chunk(i, carry):
        base = i * C
        slot = (lax.broadcasted_iota(jnp.int32, (C, ntok), 0) + base).astype(F32)
        oh = jnp.where(slot == srow_ref[...], 1.0, 0.0).astype(BF16)
        for c in range(acc.shape[1] // CB):
            s = slice(c * CB, (c + 1) * CB)
            acc[:, s] = jnp.dot(oh, dx[:, s], preferred_element_type=F32)
        here = jnp.minimum(cnt - base, C)

        def put(j, c2):
            row = list_ref[0, base + j]
            pltpu.make_async_copy(acc.at[pl.ds(j, 1)], de.at[pl.ds(row, 1)], sem).start()
            return c2

        def done(j, c2):
            pltpu.make_async_copy(acc.at[pl.ds(j, 1)], de.at[pl.ds(0, 1)], sem).wait()
            return c2

        lax.fori_loop(0, here, put, 0)
        lax.fori_loop(0, here, done, 0)
        return carry

    lax.fori_loop(0, (cnt + C - 1) // C, chunk, 0)


def _scatter(cnts, rows, srow, pieces, de, ts, nk):
    vs, d = de.shape
    ntok = srow.shape[1]
    return pl.pallas_call(
        functools.partial(_scatter_kernel, ts, nk),
        out_shape=jax.ShapeDtypeStruct((vs, d), F32),
        in_specs=[_sm(), _sm(), _vm()] + [_vm()] * len(pieces) + [_any()],
        out_specs=_any(),
        scratch_shapes=[VMEM((ntok, d), BF16), VMEM((C, d), F32), pltpu.SemaphoreType.DMA],
        input_output_aliases={3 + len(pieces): 0},
        compiler_params=_params(16),
        cost_estimate=_cost(3),
        name="scatter_rows",
    )(cnts, rows, srow, *pieces, de)


def _acc_kernel(lo, n, cnt_ref, oth_ref, slot_ref, dx0, dx1, de_in, de, acc, flag, z, sems):
    z[...] = jnp.zeros_like(z)
    _fill(z, de, sems, lo, 0, n, False)
    for i in (0, 2):
        flag[0, i] = jnp.maximum(cnt_ref[0, i], oth_ref[0, i])
    m = dx0.shape[0]
    j = _iota((C, m), 0)
    ohs = [jnp.where(slot_ref[i:i + 1, :] == j, 1.0, 0.0).astype(BF16) for i in (0, 1)]
    for c in range(acc.shape[1] // CB):
        s = slice(c * CB, (c + 1) * CB)
        tot = jnp.dot(ohs[0], dx0[:, s], preferred_element_type=F32)
        acc[:, s] = tot + jnp.dot(ohs[1], dx1[:, s], preferred_element_type=F32)
    _fill(z, de, sems, lo, 0, n, True)


def _acc(cnts, other, slots, dx0, dx1, de, lo):
    vs, d = de.shape
    n = vs // ZR - lo
    return pl.pallas_call(
        functools.partial(_acc_kernel, lo, n),
        out_shape=(
            jax.ShapeDtypeStruct((vs, d), F32),
            jax.ShapeDtypeStruct((C, d), F32),
            jax.ShapeDtypeStruct((1, 4), jnp.int32),
        ),
        in_specs=[_sm(), _sm()] + [_vm()] * 3 + [_any()],
        out_specs=(_any(), _vm(), _sm()),
        scratch_shapes=_zscratch(d, n),
        input_output_aliases={5: 0},
        compiler_params=_params(8),
        cost_estimate=_cost(n * 0.375),
        name="fill_acc",
    )(cnts, other, slots, dx0, dx1, de)


def _write_kernel(cnt_ref, list_ref, map_ref, acc_in, mine_ref, got_ref, de_in, de, dg_out, acc, sem):
    acc[...] = acc_in[...]

    def add(j, carry):
        at = pl.ds(map_ref[0, j], 1)
        acc[at, :] = acc[at, :] + got_ref[pl.ds(j, 1), :]
        return carry

    lax.fori_loop(0, jnp.minimum(cnt_ref[0, 3], C2 - 1), add, 0)
    here = jnp.minimum(cnt_ref[0, 1], C)

    def put(j, carry):
        pltpu.make_async_copy(acc.at[pl.ds(j, 1)], de.at[pl.ds(list_ref[0, j], 1)], sem).start()
        return carry

    def done(j, carry):
        pltpu.make_async_copy(acc.at[pl.ds(j, 1)], de.at[pl.ds(0, 1)], sem).wait()
        return carry

    lax.fori_loop(0, here, put, 0)
    dg = mine_ref[C2 - 1:C2, :] + got_ref[C2 - 1:C2, :]
    dg_out[...] = dg.reshape(dg_out.shape)
    lax.fori_loop(0, here, done, 0)


def _write(cnts, rows, where, acc, mine, got, de):
    vs, d = de.shape
    return pl.pallas_call(
        _write_kernel,
        out_shape=(jax.ShapeDtypeStruct((vs, d), F32), jax.ShapeDtypeStruct((d,), F32)),
        in_specs=[_sm(), _sm(), _sm()] + [_vm()] * 3 + [_any()],
        out_specs=(_any(), _vm()),
        scratch_shapes=[VMEM((C, d), F32), pltpu.SemaphoreType.DMA],
        input_output_aliases={6: 0},
        compiler_params=_params(6),
        cost_estimate=_cost(3),
        name="write_rows",
    )(cnts, rows, where, acc, mine, got, de)


def solution(mesh):
    ntp = mesh.shape["tp"]
    ndp = mesh.shape["dp"]

    def swap(a, bit):
        return lax.ppermute(a, "tp", [(i, i ^ bit) for i in range(ntp)])

    def share(t):
        t2 = swap(t, 2)
        t1 = swap(t, 1)
        return t, t1, t2, swap(t2, 1)

    def p_terms(du, W, ts, vs):
        q, de = _p_terms(du, W, ts, vs)
        return de, (q[0], swap(q[1], 1), swap(q[2], 2), swap(q[3], 3))

    def fill_rest(de):
        n = ZP + ZU + ZW
        return _zeros(de, n, de.shape[0] // ZR - n)

    def body(ids, E, g, W, du, dres):
        vs, d = E.shape
        nk, t = ids.shape
        ts = t // ntp
        m = nk * ts
        g2 = g.reshape(1, d)

        tab, pos, _, rows, cnts, slots, where = _index_call(None, ids, E, ntp)
        tabs = share(tab)
        de, ps = p_terms(du, W, ts, vs)
        x, xl = _expand(pos, tabs, ts)
        u, n, de = _u(x, g2, W, nk, de)
        dW, de = _dw(n, du, de, ZP + ZU, ZW)
        dx, dg = _dx(xl.reshape(m, d), ps, dres.reshape(m, d), g2)
        dx1, dg1 = swap(dx, 1), swap(dg, 1)
        mine = _sums(slots, dx, dx1, dg, dg1)
        got = swap(mine, 2)
        other = lax.ppermute(cnts, "dp", [(i, (i + 1) % ndp) for i in range(ndp)])
        de, acc, flags = _acc(cnts, other, slots, dx, dx1, de, ZP + ZU + ZW)
        dE, dg = _write(cnts, rows, where, acc, mine, got, de)
        outs = u, xl, dE, dW, dg

        inputs = ids, E, W, du, dres, g2, flags

        def again(c):
            ids, E, W, du, dres, g2, fl, left = lax.optimization_barrier((*inputs, c[0]))
            rounds = fl[0, 0]
            i0 = left - left

            def more(q):
                i, x, _ = q
                tab, pos, *_ = _index_call(i, ids, E, ntp)
                return i + 1, *_expand(pos, share(tab), ts, x)

            zeros = jnp.zeros((nk * t, d), BF16), jnp.zeros((nk, ts, d), BF16)
            _, x, xl = lax.while_loop(lambda q: q[0] < rounds, more, (i0, *zeros))
            _, _, srow, rows, cs, _, _ = _index_call(i0, ids, E, ntp)
            de, ps = p_terms(du, W, ts, vs)
            u, n, de = _u(x, g2, W, nk, de)
            dW, de = _dw(n, du, de, ZP + ZU, ZW)
            dx, dg = _dx(xl.reshape(m, d), ps, dres.reshape(m, d), g2)
            dg2 = dg + swap(dg, 1)
            dg = (dg2 + swap(dg2, 2)).reshape(d)
            dE = _scatter(cs, rows, srow, share(dx), fill_rest(de), ts, nk)
            return i0, (u, xl, dE, dW, dg)

        _, outs = lax.while_loop(lambda c: c[0] > 0, again, (flags[0, 2], outs))
        return outs

    return jax.shard_map(
        body,
        mesh=mesh,
        in_specs=(P("dp", None), P("tp", None), P(None), P(None, "tp"), P("dp", None, "tp"), P("dp", "tp", None)),
        out_specs=(P("dp", None, "tp"), P("dp", "tp", None), P(("dp", "tp"), None), P("dp", "tp"), P("dp")),
        check_vma=False,
    )
```

```python
import functools

import jax
import jax.numpy as jnp
from jax import lax
from jax.experimental import pallas as pl
from jax.experimental.pallas import tpu as pltpu
from jax.sharding import PartitionSpec as P


EPS = 1e-6
C = 64
G = 2
GS = 64
C2 = 32
CB = 256
ZR = 128
ZI, ZP, ZU, ZW, ZD = 6, 9, 15, 18, 3
AT_P, AT_U, AT_W, AT_D, AT_R = ZI, ZI + ZP, ZI + ZP + ZU, ZI + ZP + ZU + ZW, ZI + ZP + ZU + ZW + ZD
TB = 64

F32 = jnp.float32
BF16 = jnp.bfloat16
VMEM = pltpu.VMEM


def _sm():
    return pl.BlockSpec(memory_space=pltpu.SMEM)


def _vm():
    return pl.BlockSpec(memory_space=pltpu.VMEM)


def _any():
    return pl.BlockSpec(memory_space=pl.ANY)


def _params(mb):
    return pltpu.CompilerParams(vmem_limit_bytes=mb << 20)


def _cost(us):
    return pl.CostEstimate(flops=int(us * 4_000_000_000), bytes_accessed=1_000_000, transcendentals=0)


def _iota(shape, dim):
    return lax.broadcasted_iota(jnp.int32, shape, dim).astype(F32)


def _me():
    return lax.axis_index("tp").astype(jnp.int32)


def _fill(z, o, sems, lo, first, n, wait):
    def step(i, carry):
        at = pl.multiple_of((lo + i) * ZR, ZR)
        c = pltpu.make_async_copy(z, o.at[pl.ds(at, ZR)], sems.at[i])
        c.wait() if wait else c.start()
        return carry

    lax.fori_loop(first, first + n, step, 0)


def _zscratch(d, n):
    return [VMEM((ZR, d), F32), pltpu.SemaphoreType.DMA((n,))]


def _index_kernel(vs, ntp, first, *refs):
    if first:
        refs, (de, z, zsems) = refs[:-2], (refs[9], *refs[-2:])
        ids_ref, e_ref, tab_ref, pos_ref, srow_ref, list_ref, cnt_ref, slot_ref, map_ref, _, buf, glv, gls, gsem, sems = refs
        base = 0.0
        z[...] = jnp.zeros_like(z)
        _fill(z, de, zsems, 0, 0, ZI, False)
    else:
        c_ref, ids_ref, e_ref, tab_ref, pos_ref, srow_ref, list_ref, cnt_ref, slot_ref, map_ref, buf, glv, gls, gsem, sems = refs
        base = (c_ref[0] * C).astype(F32)
    mei = _me()
    me = mei.astype(F32)
    lo = me * vs
    nk, t = ids_ref.shape
    ntok = nk * t
    nb = ntok // TB
    idsf = ids_ref[...].astype(F32)
    idr = jnp.concatenate([idsf[k:k + 1] for k in range(nk)], axis=1)

    def column(row, b):
        w = (b * TB) // 128 * 128
        part = jnp.broadcast_to(row[:, w:w + 128], (TB, 128))
        hit = _iota((TB, 128), 1) == _iota((TB, 128), 0) + float(b * TB - w)
        return jnp.sum(jnp.where(hit, part, 0.0), axis=1, keepdims=True)

    def fold(a):
        return sum(a[8 * q:8 * q + 8] for q in range(1, TB // 8)) + a[:8]

    lane = _iota((TB, ntok), 1)
    thr = _iota((TB, 128), 1) * float(vs)
    rank8 = jnp.zeros((8, ntok), F32)
    below8 = jnp.zeros((8, 128), F32)
    idcs = []
    for b in range(nb):
        idc = column(idr, b)
        idcs.append(idc)
        idb = jnp.broadcast_to(idc, (TB, ntok))
        dup = (idb == idr) & (lane < _iota((TB, ntok), 0) + float(b * TB))
        seen = jnp.max(jnp.where(dup, 1.0, 0.0), axis=1, keepdims=True)
        key = jnp.where(seen > 0.5, float(vs * ntp), idc)
        rank8 = rank8 + fold(jnp.where(jnp.broadcast_to(key, (TB, ntok)) < idr, 1.0, 0.0))
        below8 = below8 + fold(jnp.where(jnp.broadcast_to(key, (TB, 128)) < thr, 1.0, 0.0))
    rank = jnp.sum(rank8, axis=0, keepdims=True)
    below = jnp.sum(below8, axis=0, keepdims=True)
    own_r = jnp.floor(idr * (1.0 / vs))
    start = jnp.zeros_like(rank)
    cnt = jnp.zeros((1, 1), F32)
    mx = jnp.zeros((1, 1), F32)
    for d in range(ntp):
        ld = below[:, d:d + 1]
        nd = below[:, d + 1:d + 2] - ld
        start = jnp.where(own_r == float(d), ld, start)
        cnt = jnp.where(me == float(d), nd, cnt)
        mx = jnp.maximum(mx, nd)
    slot_r = rank - start
    my_r = jnp.where(own_r == me, slot_r, -1.0)

    slot_l = _iota((TB, 128), 1) + base
    acc = jnp.zeros((TB, 128), F32)
    mys = []
    for b in range(nb):
        my_c = column(my_r, b)
        mys.append(my_c)
        acc = jnp.maximum(acc, jnp.where(my_c == slot_l, idcs[b] - lo, 0.0))
    glv[...] = jnp.broadcast_to(jnp.max(acc, axis=0, keepdims=True), (8, 128)).astype(jnp.int32)
    cp = pltpu.make_async_copy(glv, gls, gsem)
    cp.start()
    cp.wait()

    def fetch(q, j, carry):
        j = q * GS + j
        g = pl.multiple_of((gls[0, j] >> 1) << 1, G)
        at = pl.multiple_of(j * G, G)
        pltpu.make_async_copy(e_ref.at[pl.ds(g, G)], buf.at[pl.ds(at, G)], sems.at[q]).start()
        return carry

    for q in range(C // GS):
        lax.fori_loop(0, GS, functools.partial(fetch, q), 0, unroll=8)

    ts = t // ntp
    part = lax.broadcasted_iota(jnp.int32, (1, ntok), 1) // ts % ntp
    chips = [jnp.where(part // 2 == c, 1.0, 0.0) for c in range(ntp // 2)]
    rank28 = jnp.zeros((8, ntok), F32)
    below28 = [jnp.zeros((8, 128), F32) for _ in chips]
    for b in range(nb):
        idc = idcs[b]
        dup = (jnp.broadcast_to(idc, (TB, ntok)) == idr) & (lane < _iota((TB, ntok), 0) + float(b * TB))
        c = b * TB // ts % ntp // 2
        seen = jnp.max(jnp.where(dup, chips[c], 0.0), axis=1, keepdims=True)
        key = jnp.where(seen > 0.5, float(vs * ntp), idc)
        rank28 = rank28 + fold(jnp.where(jnp.broadcast_to(key, (TB, ntok)) < idr, chips[c], 0.0))
        below28[c] = below28[c] + fold(jnp.where(jnp.broadcast_to(key, (TB, 128)) < thr, 1.0, 0.0))
    rank2 = jnp.sum(rank28, axis=0, keepdims=True)
    below2 = [jnp.sum(b8, axis=0, keepdims=True) for b8 in below28]
    start2 = jnp.zeros_like(rank)
    cnt2 = jnp.zeros((1, 1), F32)
    mx2 = jnp.zeros((1, 1), F32)
    for c, chip in enumerate(chips):
        for d in range(ntp):
            ld = below2[c][:, d:d + 1]
            nd = below2[c][:, d + 1:d + 2] - ld
            start2 = jnp.where((own_r == float(d)) & (chip > 0.5), ld, start2)
            if d // 2 != c:
                cnt2 = jnp.where(me == float(d), nd, cnt2)
                mx2 = jnp.maximum(mx2, nd)
    slot2_r = rank2 - start2
    srow_ref[...] = my_r
    full = jnp.zeros((8, ntok), F32)
    lane8 = _iota((8, ntok), 1)
    for b in range(nb):
        for q in range(TB // 8):
            s = slice(8 * q, 8 * q + 8)
            full = jnp.maximum(full, jnp.where(mys[b][s] == lane8, idcs[b][s] - lo, 0.0))
    list_ref[...] = jnp.max(full, axis=0, keepdims=True).astype(jnp.int32)
    rel = (own_r.astype(jnp.int32) ^ mei).astype(F32)
    pos = jnp.where((slot_r >= base) & (slot_r < base + C), rel * C + slot_r - base, -1.0)
    for b in range(nb):
        pos_ref[b * TB:(b + 1) * TB, :] = column(pos, b)
    lane1 = lax.broadcasted_iota(jnp.int32, (1, 128), 1)
    over = jnp.where((mx > C) | (mx2 > C2 - 1), 1.0, 0.0)
    rounds = jnp.floor((mx + C - 1.0) * (1.0 / C))
    cnts = jnp.where(lane1 == 0, rounds, jnp.where(lane1 == 1, cnt, jnp.where(lane1 == 2, over, cnt2)))
    cnt_ref[...] = cnts.astype(jnp.int32)
    facing = (mei ^ 2).astype(F32)
    sums_r = jnp.where(own_r == facing, slot2_r, -1.0)
    rows = [jnp.zeros((1, nk * ts), F32)] * 4
    for q in range(ntp):
        at = [slice(k * t + q * ts, k * t + (q + 1) * ts) for k in range(nk)]
        mine = jnp.concatenate([my_r[:, w] for w in at], axis=1)
        sums = jnp.concatenate([sums_r[:, w] for w in at], axis=1)
        own, sib = me == float(q), me == float(q ^ 1)
        rows = [
            jnp.where(own, mine, rows[0]), jnp.where(sib, mine, rows[1]),
            jnp.where(own, sums, rows[2]), jnp.where(sib, sums, rows[3]),
        ]
    for j, r in enumerate(rows):
        slot_ref[j:j + 1, :] = r
    far = (part // 2).astype(F32) != jnp.floor(me * 0.5)
    got_r = jnp.where(far & (own_r == me), slot2_r, -1.0)
    acc2 = jnp.zeros((TB, 128), F32)
    slot_j = _iota((TB, 128), 1)
    for b in range(nb):
        acc2 = jnp.maximum(acc2, jnp.where(column(got_r, b) == slot_j, mys[b], 0.0))
    map_ref[...] = jnp.minimum(jnp.max(acc2, axis=0, keepdims=True), C - 1.0).astype(jnp.int32)
    hit = jnp.where(my_r == _iota((C, ntok), 0) + base, idr - lo, 0.0)
    want = jnp.max(hit, axis=1, keepdims=True)
    want = want - jnp.floor(want * (1.0 / G)) * G
    for q in range(C // GS):
        r = slice(q * GS * G, (q + 1) * GS * G)
        mine = want[q * GS:(q + 1) * GS] + _iota((GS, 1), 0) * G
        sel = jnp.where(_iota((GS, GS * G), 1) == mine, 1.0, 0.0).astype(BF16)
        pltpu.make_async_copy(e_ref.at[pl.ds(0, GS * G)], buf.at[r], sems.at[q]).wait()
        tab_ref[q * GS:(q + 1) * GS, :] = jnp.dot(sel, buf[r, :], preferred_element_type=F32).astype(BF16)
    if first:
        _fill(z, de, zsems, 0, 0, ZI, True)


def _index_call(chunk, ids, E, ntp):
    vs, d = E.shape
    ntok = ids.shape[0] * ids.shape[1]
    first = chunk is None
    return pl.pallas_call(
        functools.partial(_index_kernel, vs, ntp, first),
        out_shape=(
            jax.ShapeDtypeStruct((C, d), BF16),
            jax.ShapeDtypeStruct((ntok, 1), F32),
            jax.ShapeDtypeStruct((1, ntok), F32),
            jax.ShapeDtypeStruct((1, ntok), jnp.int32),
            jax.ShapeDtypeStruct((1, 128), jnp.int32),
            jax.ShapeDtypeStruct((4, ntok // ntp), F32),
            jax.ShapeDtypeStruct((1, 128), jnp.int32),
        ) + ((jax.ShapeDtypeStruct((vs, d), F32),) if first else ()),
        in_specs=([] if first else [_sm()]) + [_vm(), pl.BlockSpec(memory_space=pltpu.HBM)],
        out_specs=(_vm(),) * 7 + ((_any(),) if first else ()),
        scratch_shapes=[
            VMEM((C * G, d), BF16),
            VMEM((8, 128), jnp.int32),
            pltpu.SMEM((8, 128), jnp.int32),
            pltpu.SemaphoreType.DMA,
            pltpu.SemaphoreType.DMA((C // GS,)),
        ] + (_zscratch(d, ZI) if first else []),
        compiler_params=_params(8),
        cost_estimate=_cost(5),
        name="index_gather",
    )(*([] if first else [chunk.reshape(1)]), ids, E)


def _expand_kernel(ts, acc, *refs):
    if acc:
        x_in, pos, t0, t1, t2, t3, x_out, xl_out = refs
    else:
        pos, t0, t1, t2, t3, x_out, xl_out = refs
    oh = jnp.where(pos[...] == _iota((pos.shape[0], 4 * C), 1), 1.0, 0.0).astype(BF16)
    for c in range(x_out.shape[1] // CB):
        s = slice(c * CB, (c + 1) * CB)
        tab = jnp.concatenate([t[:, s] for t in (t0, t1, t2, t3)], axis=0)
        tot = jnp.dot(oh, tab, preferred_element_type=F32)
        if acc:
            tot = tot + x_in[:, s].astype(F32)
        x_out[:, s] = tot.astype(BF16)
    t = 4 * ts
    for k in range(x_out.shape[0] // t):
        at = pl.multiple_of(k * t + _me() * ts, ts)
        xl_out[k] = x_out[pl.ds(at, ts), :]


def _expand(pos, tabs, ts, x=None):
    ntok, d = pos.shape[0], tabs[0].shape[1]
    ins = ([x] if x is not None else []) + [pos, *tabs]
    return pl.pallas_call(
        functools.partial(_expand_kernel, ts, x is not None),
        out_shape=(jax.ShapeDtypeStruct((ntok, d), BF16), jax.ShapeDtypeStruct((ntok // (4 * ts), ts, d), BF16)),
        in_specs=[_vm()] * len(ins),
        out_specs=(_vm(), _vm()),
        compiler_params=_params(12),
        cost_estimate=_cost(3),
        name="expand",
    )(*ins)


def _p_kernel(ts, du_ref, w_ref, de_in, *refs):
    outs, (de, dur, z, sems) = refs[:-4], refs[-4:]
    nk = du_ref.shape[0]

    @pl.when(pl.program_id(0) == 0)
    def _():
        z[...] = jnp.zeros_like(z)
        for k in range(nk):
            for r in range(4):
                at = pl.multiple_of((_me() ^ r) * ts, ts)
                dur[pl.ds((r * nk + k) * ts, ts), :] = du_ref[k, pl.ds(at, ts), :]
        _fill(z, de, sems, AT_P, 0, ZP, False)

    out = lax.dot_general(dur[...], w_ref[...], (((1,), (1,)), ((), ())), preferred_element_type=F32)
    for i, o in enumerate(outs):
        o[...] = out[i * nk * ts:(i + 1) * nk * ts].astype(BF16)

    @pl.when(pl.program_id(0) == pl.num_programs(0) - 1)
    def _():
        _fill(z, de, sems, AT_P, 0, ZP, True)


def _p_terms(du, W, ts, de):
    nk, t, f = du.shape
    d = W.shape[0]
    cb = 3 * CB
    out = pl.pallas_call(
        functools.partial(_p_kernel, ts),
        out_shape=(jax.ShapeDtypeStruct((nk * ts, d), BF16),) * 4 + (jax.ShapeDtypeStruct(de.shape, F32),),
        grid=(d // cb,),
        in_specs=[pl.BlockSpec((nk, t, f), lambda i: (0, 0, 0)), pl.BlockSpec((cb, f), lambda i: (i, 0)), _any()],
        out_specs=(pl.BlockSpec((nk * ts, cb), lambda i: (0, i)),) * 4 + (_any(),),
        scratch_shapes=[VMEM((nk * t, f), BF16)] + _zscratch(d, ZP),
        input_output_aliases={2: 4},
        compiler_params=_params(20),
        cost_estimate=_cost(5),
        name="p_terms",
    )(du, W, de)
    return out[:4], out[4]


def _zero_kernel(lo, n, de_in, o, z, sems):
    z[...] = jnp.zeros_like(z)
    _fill(z, o, sems, lo, 0, n, False)
    _fill(z, o, sems, lo, 0, n, True)


def _zeros(de, lo, n):
    vs, d = de.shape
    return pl.pallas_call(
        functools.partial(_zero_kernel, lo, n),
        out_shape=jax.ShapeDtypeStruct((vs, d), F32),
        in_specs=[_any()],
        out_specs=_any(),
        scratch_shapes=_zscratch(d, n),
        input_output_aliases={0: 0},
        compiler_params=_params(4),
        cost_estimate=_cost(n * 0.375),
        name="zero_fill",
    )(de)


def _dx_kernel(x, p0, p1, p2, p3, dres, g, de_in, dx, dg, de, z, sems):
    z[...] = jnp.zeros_like(z)
    _fill(z, de, sems, AT_D, 0, ZD, False)
    rows = 32
    tot = None
    for b in range(dx.shape[0] // rows):
        s = slice(b * rows, (b + 1) * rows)
        xf = x[s].astype(F32)
        rs = lax.rsqrt(jnp.mean(xf * xf, axis=-1, keepdims=True) + EPS)
        nh = xf * rs
        dn = (p0[s].astype(F32) + p1[s].astype(F32)) + (p2[s].astype(F32) + p3[s].astype(F32))
        gdn = g[...].astype(F32) * dn
        out = dres[s].astype(F32) + rs * (gdn - nh * jnp.mean(nh * gdn, axis=-1, keepdims=True))
        dx[s] = out.astype(BF16)
        part = jnp.sum(dn * nh, axis=0, keepdims=True)
        tot = part if tot is None else tot + part
    dg[...] = tot
    _fill(z, de, sems, AT_D, 0, ZD, True)


def _dx(x, ps, dres, g, de):
    m, d = x.shape
    return pl.pallas_call(
        _dx_kernel,
        out_shape=(
            jax.ShapeDtypeStruct((m, d), BF16),
            jax.ShapeDtypeStruct((1, d), F32),
            jax.ShapeDtypeStruct(de.shape, F32),
        ),
        in_specs=[_vm()] * 7 + [_any()],
        out_specs=(_vm(), _vm(), _any()),
        scratch_shapes=_zscratch(d, ZD),
        input_output_aliases={7: 2},
        compiler_params=_params(12),
        cost_estimate=_cost(2),
        name="dx_form",
    )(x, *ps, dres, g, de)


def _sums_kernel(slot_ref, dx0, dx1, dg0, dg1, out):
    m = dx0.shape[0]
    j = _iota((C2, m), 0)
    ohs = [jnp.where(slot_ref[i:i + 1, :] == j, 1.0, 0.0).astype(BF16) for i in (2, 3)]
    last = lax.broadcasted_iota(jnp.int32, (C2, CB), 0) == C2 - 1
    for c in range(out.shape[1] // CB):
        s = slice(c * CB, (c + 1) * CB)
        tot = jnp.dot(ohs[0], dx0[:, s], preferred_element_type=F32)
        tot = tot + jnp.dot(ohs[1], dx1[:, s], preferred_element_type=F32)
        out[:, s] = jnp.where(last, dg0[:, s] + dg1[:, s], tot)


def _sums(slots, dx0, dx1, dg0, dg1):
    return pl.pallas_call(
        _sums_kernel,
        out_shape=jax.ShapeDtypeStruct((C2, dx0.shape[1]), F32),
        in_specs=[_vm()] * 5,
        out_specs=_vm(),
        compiler_params=_params(6),
        cost_estimate=_cost(1),
        name="dx_sums",
    )(slots, dx0, dx1, dg0, dg1)


def _u_kernel(x_ref, g_ref, w_ref, de_in, u_ref, n_ref, de, z, sems):
    z[...] = jnp.zeros_like(z)
    _fill(z, de, sems, AT_U, 0, ZU, False)
    rows = 64
    for b in range(n_ref.shape[0] // rows):
        s = slice(b * rows, (b + 1) * rows)
        xf = x_ref[s].astype(F32)
        rs = lax.rsqrt(jnp.mean(xf * xf, axis=-1, keepdims=True) + EPS)
        n_ref[s] = (xf * rs * g_ref[...].astype(F32)).astype(BF16)
    nk, t, f = u_ref.shape
    for c in range(f // CB):
        s = slice(c * CB, (c + 1) * CB)
        out = jnp.dot(n_ref[...], w_ref[:, s], preferred_element_type=F32).astype(BF16)
        for k in range(nk):
            u_ref[k, :, s] = out[k * t:(k + 1) * t]
    _fill(z, de, sems, AT_U, 0, ZU, True)


def _u(x, g, W, nk, de):
    ntok, d = x.shape
    f = W.shape[1]
    return pl.pallas_call(
        _u_kernel,
        out_shape=(
            jax.ShapeDtypeStruct((nk, ntok // nk, f), BF16),
            jax.ShapeDtypeStruct((ntok, d), BF16),
            jax.ShapeDtypeStruct(de.shape, F32),
        ),
        in_specs=[_vm(), _vm(), _vm(), _any()],
        out_specs=(_vm(), _vm(), _any()),
        scratch_shapes=_zscratch(d, ZU),
        input_output_aliases={3: 2},
        compiler_params=_params(20),
        cost_estimate=_cost(10),
        name="u_terms",
    )(x, g, W, de)


def _dw_kernel(lo, n, per, n_ref, du_ref, de_in, dw_ref, de, z, sems):
    i = pl.program_id(0)
    nk, t, f = du_ref.shape

    @pl.when(i == 0)
    def _():
        z[...] = jnp.zeros_like(z)

    _fill(z, de, sems, lo, i * per, jnp.minimum(per, n - i * per), False)
    dw_ref[...] = lax.dot_general(
        n_ref[...], du_ref[...].reshape(nk * t, f), (((0,), (0,)), ((), ())), preferred_element_type=F32
    )

    @pl.when(i == pl.num_programs(0) - 1)
    def _():
        _fill(z, de, sems, lo, 0, n, True)


def _dw(n, du, de, lo, nz):
    nk, t, f = du.shape
    ntok, d = n.shape
    cb = d // 6
    steps = d // cb
    return pl.pallas_call(
        functools.partial(_dw_kernel, lo, nz, -(-nz // steps)),
        out_shape=(jax.ShapeDtypeStruct((d, f), F32), jax.ShapeDtypeStruct(de.shape, F32)),
        grid=(steps,),
        in_specs=[
            pl.BlockSpec((ntok, cb), lambda i: (0, i)),
            pl.BlockSpec((nk, t, f), lambda i: (0, 0, 0)),
            _any(),
        ],
        out_specs=(pl.BlockSpec((cb, f), lambda i: (i, 0)), _any()),
        scratch_shapes=_zscratch(d, nz),
        input_output_aliases={2: 1},
        compiler_params=_params(20),
        cost_estimate=_cost(10),
        name="dw_terms",
    )(n, du, de)


def _scatter_kernel(ts, nk, cnt_ref, list_ref, srow_ref, *refs):
    pieces, (de_in, de, dx, acc, sem) = refs[:-5], refs[-5:]
    ntok = nk * 4 * ts
    for k in range(nk):
        for r in range(4):
            at = pl.multiple_of(k * 4 * ts + (_me() ^ r) * ts, ts)
            dx[pl.ds(at, ts), :] = pieces[r][k * ts:(k + 1) * ts, :]
    cnt = cnt_ref[0, 1]

    def chunk(i, carry):
        base = i * C
        slot = (lax.broadcasted_iota(jnp.int32, (C, ntok), 0) + base).astype(F32)
        oh = jnp.where(slot == srow_ref[...], 1.0, 0.0).astype(BF16)
        for c in range(acc.shape[1] // CB):
            s = slice(c * CB, (c + 1) * CB)
            acc[:, s] = jnp.dot(oh, dx[:, s], preferred_element_type=F32)
        here = jnp.minimum(cnt - base, C)

        def put(j, c2):
            row = list_ref[0, base + j]
            pltpu.make_async_copy(acc.at[pl.ds(j, 1)], de.at[pl.ds(row, 1)], sem).start()
            return c2

        def done(j, c2):
            pltpu.make_async_copy(acc.at[pl.ds(j, 1)], de.at[pl.ds(0, 1)], sem).wait()
            return c2

        lax.fori_loop(0, here, put, 0)
        lax.fori_loop(0, here, done, 0)
        return carry

    lax.fori_loop(0, (cnt + C - 1) // C, chunk, 0)


def _scatter(cnts, rows, srow, pieces, de, ts, nk):
    vs, d = de.shape
    ntok = srow.shape[1]
    return pl.pallas_call(
        functools.partial(_scatter_kernel, ts, nk),
        out_shape=jax.ShapeDtypeStruct((vs, d), F32),
        in_specs=[_sm(), _sm(), _vm()] + [_vm()] * len(pieces) + [_any()],
        out_specs=_any(),
        scratch_shapes=[VMEM((ntok, d), BF16), VMEM((C, d), F32), pltpu.SemaphoreType.DMA],
        input_output_aliases={3 + len(pieces): 0},
        compiler_params=_params(16),
        cost_estimate=_cost(3),
        name="scatter_rows",
    )(cnts, rows, srow, *pieces, de)


def _acc_kernel(lo, n, cnt_ref, oth_ref, slot_ref, dx0, dx1, de_in, de, acc, flag, z, sems):
    z[...] = jnp.zeros_like(z)
    _fill(z, de, sems, lo, 0, n, False)
    for i in (0, 2):
        flag[0, i] = jnp.maximum(cnt_ref[0, i], oth_ref[0, i])
    m = dx0.shape[0]
    j = _iota((C, m), 0)
    ohs = [jnp.where(slot_ref[i:i + 1, :] == j, 1.0, 0.0).astype(BF16) for i in (0, 1)]
    for c in range(acc.shape[1] // CB):
        s = slice(c * CB, (c + 1) * CB)
        tot = jnp.dot(ohs[0], dx0[:, s], preferred_element_type=F32)
        acc[:, s] = tot + jnp.dot(ohs[1], dx1[:, s], preferred_element_type=F32)
    _fill(z, de, sems, lo, 0, n, True)


def _acc(cnts, other, slots, dx0, dx1, de, lo):
    vs, d = de.shape
    n = vs // ZR - lo
    return pl.pallas_call(
        functools.partial(_acc_kernel, lo, n),
        out_shape=(
            jax.ShapeDtypeStruct((vs, d), F32),
            jax.ShapeDtypeStruct((C, d), F32),
            jax.ShapeDtypeStruct((1, 4), jnp.int32),
        ),
        in_specs=[_sm(), _sm()] + [_vm()] * 3 + [_any()],
        out_specs=(_any(), _vm(), _sm()),
        scratch_shapes=_zscratch(d, n),
        input_output_aliases={5: 0},
        compiler_params=_params(8),
        cost_estimate=_cost(n * 0.375),
        name="fill_acc",
    )(cnts, other, slots, dx0, dx1, de)


def _write_kernel(cnt_ref, list_ref, map_ref, acc_in, mine_ref, got_ref, de_in, de, dg_out, acc, sem):
    acc[...] = acc_in[...]

    def add(j, carry):
        at = pl.ds(map_ref[0, j], 1)
        acc[at, :] = acc[at, :] + got_ref[pl.ds(j, 1), :]
        return carry

    lax.fori_loop(0, jnp.minimum(cnt_ref[0, 3], C2 - 1), add, 0)
    here = jnp.minimum(cnt_ref[0, 1], C)

    def put(j, carry):
        pltpu.make_async_copy(acc.at[pl.ds(j, 1)], de.at[pl.ds(list_ref[0, j], 1)], sem).start()
        return carry

    def done(j, carry):
        pltpu.make_async_copy(acc.at[pl.ds(j, 1)], de.at[pl.ds(0, 1)], sem).wait()
        return carry

    lax.fori_loop(0, here, put, 0)
    dg = mine_ref[C2 - 1:C2, :] + got_ref[C2 - 1:C2, :]
    dg_out[...] = dg.reshape(dg_out.shape)
    lax.fori_loop(0, here, done, 0)


def _write(cnts, rows, where, acc, mine, got, de):
    vs, d = de.shape
    return pl.pallas_call(
        _write_kernel,
        out_shape=(jax.ShapeDtypeStruct((vs, d), F32), jax.ShapeDtypeStruct((d,), F32)),
        in_specs=[_sm(), _sm(), _sm()] + [_vm()] * 3 + [_any()],
        out_specs=(_any(), _vm()),
        scratch_shapes=[VMEM((C, d), F32), pltpu.SemaphoreType.DMA],
        input_output_aliases={6: 0},
        compiler_params=_params(6),
        cost_estimate=_cost(3),
        name="write_rows",
    )(cnts, rows, where, acc, mine, got, de)


def solution(mesh):
    ntp = mesh.shape["tp"]
    ndp = mesh.shape["dp"]

    def swap(a, bit):
        return lax.ppermute(a, "tp", [(i, i ^ bit) for i in range(ntp)])

    def share(t):
        t2 = swap(t, 2)
        t1 = swap(t, 1)
        return t, t1, t2, swap(t2, 1)

    def p_terms(du, W, ts, de):
        q, de = _p_terms(du, W, ts, de)
        return de, (q[0], swap(q[1], 1), swap(q[2], 2), swap(q[3], 3))

    def body(ids, E, g, W, du, dres):
        vs, d = E.shape
        nk, t = ids.shape
        ts = t // ntp
        m = nk * ts
        g2 = g.reshape(1, d)

        tab, pos, _, rows, cnts, slots, where, de = _index_call(None, ids, E, ntp)
        tabs = share(tab)
        de, ps = p_terms(du, W, ts, de)
        x, xl = _expand(pos, tabs, ts)
        u, n, de = _u(x, g2, W, nk, de)
        dW, de = _dw(n, du, de, AT_W, ZW)
        dx, dg, de = _dx(xl.reshape(m, d), ps, dres.reshape(m, d), g2, de)
        dx1, dg1 = swap(dx, 1), swap(dg, 1)
        mine = _sums(slots, dx, dx1, dg, dg1)
        got = swap(mine, 2)
        other = lax.ppermute(cnts, "dp", [(i, (i + 1) % ndp) for i in range(ndp)])
        de, acc, flags = _acc(cnts, other, slots, dx, dx1, de, AT_R)
        dE, dg = _write(cnts, rows, where, acc, mine, got, de)
        outs = u, xl, dE, dW, dg

        inputs = ids, E, W, du, dres, g2, flags

        def again(c):
            ids, E, W, du, dres, g2, fl, left = lax.optimization_barrier((*inputs, c[0]))
            rounds = fl[0, 0]
            i0 = left - left

            def more(q):
                i, x, _ = q
                tab, pos, *_ = _index_call(i, ids, E, ntp)
                return i + 1, *_expand(pos, share(tab), ts, x)

            zeros = jnp.zeros((nk * t, d), BF16), jnp.zeros((nk, ts, d), BF16)
            _, x, xl = lax.while_loop(lambda q: q[0] < rounds, more, (i0, *zeros))
            _, _, srow, rows, cs, _, _ = _index_call(i0, ids, E, ntp)
            de, ps = p_terms(du, W, ts, _zeros(c[1][2], 0, ZI))
            u, n, de = _u(x, g2, W, nk, de)
            dW, de = _dw(n, du, de, AT_W, ZW)
            dx, dg, de = _dx(xl.reshape(m, d), ps, dres.reshape(m, d), g2, de)
            dg2 = dg + swap(dg, 1)
            dg = (dg2 + swap(dg2, 2)).reshape(d)
            dE = _scatter(cs, rows, srow, share(dx), _zeros(de, AT_R, vs // ZR - AT_R), ts, nk)
            return i0, (u, xl, dE, dW, dg)

        _, outs = lax.while_loop(lambda c: c[0] > 0, again, (jnp.minimum(flags[0, 2], 1), outs))
        return outs

    return jax.shard_map(
        body,
        mesh=mesh,
        in_specs=(P("dp", None), P("tp", None), P(None), P(None, "tp"), P("dp", None, "tp"), P("dp", "tp", None)),
        out_specs=(P("dp", None, "tp"), P("dp", "tp", None), P(("dp", "tp"), None), P("dp", "tp"), P("dp")),
        check_vma=False,
    )
```

```python
import functools

import jax
import jax.numpy as jnp
from jax import lax
from jax.experimental import pallas as pl
from jax.experimental.pallas import tpu as pltpu
from jax.sharding import PartitionSpec as P


EPS = 1e-6
C = 64
G = 2
GS = 64
C2 = 32
CB = 256
ZR = 128
ZP, ZU, ZW = 8, 15, 24
AT_U, AT_W, AT_R = ZP, ZP + ZU, ZP + ZU + ZW
TB = 64

F32 = jnp.float32
BF16 = jnp.bfloat16
VMEM = pltpu.VMEM


def _sm():
    return pl.BlockSpec(memory_space=pltpu.SMEM)


def _vm():
    return pl.BlockSpec(memory_space=pltpu.VMEM)


def _any():
    return pl.BlockSpec(memory_space=pl.ANY)


def _params(mb):
    return pltpu.CompilerParams(vmem_limit_bytes=mb << 20)


def _cost(us):
    return pl.CostEstimate(flops=int(us * 4_000_000_000), bytes_accessed=1_000_000, transcendentals=0)


def _iota(shape, dim):
    return lax.broadcasted_iota(jnp.int32, shape, dim).astype(F32)


def _me():
    return lax.axis_index("tp").astype(jnp.int32)


def _fill(z, o, sems, lo, first, n, wait):
    def step(i, carry):
        at = pl.multiple_of((lo + i) * ZR, ZR)
        c = pltpu.make_async_copy(z, o.at[pl.ds(at, ZR)], sems.at[i])
        c.wait() if wait else c.start()
        return carry

    lax.fori_loop(first, first + n, step, 0)


def _zscratch(d, n):
    return [VMEM((ZR, d), F32), pltpu.SemaphoreType.DMA((n,))]


def _index_kernel(vs, ntp, first, *refs):
    if first:
        ids_ref, e_ref, tab_ref, pos_ref, srow_ref, list_ref, cnt_ref, slot_ref, map_ref, buf, glv, gls, gsem, sems = refs
        base = 0.0
    else:
        c_ref, ids_ref, e_ref, tab_ref, pos_ref, srow_ref, list_ref, cnt_ref, slot_ref, map_ref, buf, glv, gls, gsem, sems = refs
        base = (c_ref[0] * C).astype(F32)
    mei = _me()
    me = mei.astype(F32)
    lo = me * vs
    nk, t = ids_ref.shape
    ntok = nk * t
    nb = ntok // TB
    idsf = ids_ref[...].astype(F32)
    idr = jnp.concatenate([idsf[k:k + 1] for k in range(nk)], axis=1)

    def column(row, b):
        w = (b * TB) // 128 * 128
        part = jnp.broadcast_to(row[:, w:w + 128], (TB, 128))
        hit = _iota((TB, 128), 1) == _iota((TB, 128), 0) + float(b * TB - w)
        return jnp.sum(jnp.where(hit, part, 0.0), axis=1, keepdims=True)

    def fold(a):
        return sum(a[8 * q:8 * q + 8] for q in range(1, TB // 8)) + a[:8]

    lane = _iota((TB, ntok), 1)
    thr = _iota((TB, 128), 1) * float(vs)
    rank8 = jnp.zeros((8, ntok), F32)
    below8 = jnp.zeros((8, 128), F32)
    idcs = []
    for b in range(nb):
        idc = column(idr, b)
        idcs.append(idc)
        idb = jnp.broadcast_to(idc, (TB, ntok))
        dup = (idb == idr) & (lane < _iota((TB, ntok), 0) + float(b * TB))
        seen = jnp.max(jnp.where(dup, 1.0, 0.0), axis=1, keepdims=True)
        key = jnp.where(seen > 0.5, float(vs * ntp), idc)
        rank8 = rank8 + fold(jnp.where(jnp.broadcast_to(key, (TB, ntok)) < idr, 1.0, 0.0))
        below8 = below8 + fold(jnp.where(jnp.broadcast_to(key, (TB, 128)) < thr, 1.0, 0.0))
    rank = jnp.sum(rank8, axis=0, keepdims=True)
    below = jnp.sum(below8, axis=0, keepdims=True)
    own_r = jnp.floor(idr * (1.0 / vs))
    start = jnp.zeros_like(rank)
    cnt = jnp.zeros((1, 1), F32)
    mx = jnp.zeros((1, 1), F32)
    for d in range(ntp):
        ld = below[:, d:d + 1]
        nd = below[:, d + 1:d + 2] - ld
        start = jnp.where(own_r == float(d), ld, start)
        cnt = jnp.where(me == float(d), nd, cnt)
        mx = jnp.maximum(mx, nd)
    slot_r = rank - start
    my_r = jnp.where(own_r == me, slot_r, -1.0)

    slot_l = _iota((TB, 128), 1) + base
    acc = jnp.zeros((TB, 128), F32)
    mys = []
    for b in range(nb):
        my_c = column(my_r, b)
        mys.append(my_c)
        acc = jnp.maximum(acc, jnp.where(my_c == slot_l, idcs[b] - lo, 0.0))
    glv[...] = jnp.broadcast_to(jnp.max(acc, axis=0, keepdims=True), (8, 128)).astype(jnp.int32)
    cp = pltpu.make_async_copy(glv, gls, gsem)
    cp.start()
    cp.wait()

    def fetch(q, j, carry):
        j = q * GS + j
        g = pl.multiple_of((gls[0, j] >> 1) << 1, G)
        at = pl.multiple_of(j * G, G)
        pltpu.make_async_copy(e_ref.at[pl.ds(g, G)], buf.at[pl.ds(at, G)], sems.at[q]).start()
        return carry

    for q in range(C // GS):
        lax.fori_loop(0, GS, functools.partial(fetch, q), 0, unroll=8)

    ts = t // ntp
    part = lax.broadcasted_iota(jnp.int32, (1, ntok), 1) // ts % ntp
    chips = [jnp.where(part // 2 == c, 1.0, 0.0) for c in range(ntp // 2)]
    rank28 = jnp.zeros((8, ntok), F32)
    below28 = [jnp.zeros((8, 128), F32) for _ in chips]
    for b in range(nb):
        idc = idcs[b]
        dup = (jnp.broadcast_to(idc, (TB, ntok)) == idr) & (lane < _iota((TB, ntok), 0) + float(b * TB))
        c = b * TB // ts % ntp // 2
        seen = jnp.max(jnp.where(dup, chips[c], 0.0), axis=1, keepdims=True)
        key = jnp.where(seen > 0.5, float(vs * ntp), idc)
        rank28 = rank28 + fold(jnp.where(jnp.broadcast_to(key, (TB, ntok)) < idr, chips[c], 0.0))
        below28[c] = below28[c] + fold(jnp.where(jnp.broadcast_to(key, (TB, 128)) < thr, 1.0, 0.0))
    rank2 = jnp.sum(rank28, axis=0, keepdims=True)
    below2 = [jnp.sum(b8, axis=0, keepdims=True) for b8 in below28]
    start2 = jnp.zeros_like(rank)
    cnt2 = jnp.zeros((1, 1), F32)
    mx2 = jnp.zeros((1, 1), F32)
    for c, chip in enumerate(chips):
        for d in range(ntp):
            ld = below2[c][:, d:d + 1]
            nd = below2[c][:, d + 1:d + 2] - ld
            start2 = jnp.where((own_r == float(d)) & (chip > 0.5), ld, start2)
            if d // 2 != c:
                cnt2 = jnp.where(me == float(d), nd, cnt2)
                mx2 = jnp.maximum(mx2, nd)
    slot2_r = rank2 - start2
    srow_ref[...] = my_r
    full = jnp.zeros((8, ntok), F32)
    lane8 = _iota((8, ntok), 1)
    for b in range(nb):
        for q in range(TB // 8):
            s = slice(8 * q, 8 * q + 8)
            full = jnp.maximum(full, jnp.where(mys[b][s] == lane8, idcs[b][s] - lo, 0.0))
    list_ref[...] = jnp.max(full, axis=0, keepdims=True).astype(jnp.int32)
    rel = (own_r.astype(jnp.int32) ^ mei).astype(F32)
    pos = jnp.where((slot_r >= base) & (slot_r < base + C), rel * C + slot_r - base, -1.0)
    for b in range(nb):
        pos_ref[b * TB:(b + 1) * TB, :] = column(pos, b)
    lane1 = lax.broadcasted_iota(jnp.int32, (1, 128), 1)
    over = jnp.where((mx > C) | (mx2 > C2 - 1), 1.0, 0.0)
    rounds = jnp.floor((mx + C - 1.0) * (1.0 / C))
    cnts = jnp.where(lane1 == 0, rounds, jnp.where(lane1 == 1, cnt, jnp.where(lane1 == 2, over, cnt2)))
    cnt_ref[...] = cnts.astype(jnp.int32)
    facing = (mei ^ 2).astype(F32)
    sums_r = jnp.where(own_r == facing, slot2_r, -1.0)
    rows = [jnp.zeros((1, nk * ts), F32)] * 4
    for q in range(ntp):
        at = [slice(k * t + q * ts, k * t + (q + 1) * ts) for k in range(nk)]
        mine = jnp.concatenate([my_r[:, w] for w in at], axis=1)
        sums = jnp.concatenate([sums_r[:, w] for w in at], axis=1)
        own, sib = me == float(q), me == float(q ^ 1)
        rows = [
            jnp.where(own, mine, rows[0]), jnp.where(sib, mine, rows[1]),
            jnp.where(own, sums, rows[2]), jnp.where(sib, sums, rows[3]),
        ]
    for j, r in enumerate(rows):
        slot_ref[j:j + 1, :] = r
    far = (part // 2).astype(F32) != jnp.floor(me * 0.5)
    got_r = jnp.where(far & (own_r == me), slot2_r, -1.0)
    acc2 = jnp.zeros((TB, 128), F32)
    acc3 = jnp.zeros((TB, 128), F32)
    slot_j = _iota((TB, 128), 1)
    for b in range(nb):
        hit = column(got_r, b) == slot_j
        acc2 = jnp.maximum(acc2, jnp.where(hit, mys[b], 0.0))
        acc3 = jnp.maximum(acc3, jnp.where(hit, idcs[b] - lo, 0.0))
    slots = jnp.minimum(jnp.max(acc2, axis=0, keepdims=True), C - 1.0)
    local = jnp.max(acc3, axis=0, keepdims=True)
    many = jnp.where(lane1 == 127, cnt2, slots)
    map_ref[...] = jnp.concatenate([many, local], axis=1).astype(jnp.int32)
    hit = jnp.where(my_r == _iota((C, ntok), 0) + base, idr - lo, 0.0)
    want = jnp.max(hit, axis=1, keepdims=True)
    want = want - jnp.floor(want * (1.0 / G)) * G
    for q in range(C // GS):
        r = slice(q * GS * G, (q + 1) * GS * G)
        mine = want[q * GS:(q + 1) * GS] + _iota((GS, 1), 0) * G
        sel = jnp.where(_iota((GS, GS * G), 1) == mine, 1.0, 0.0).astype(BF16)
        pltpu.make_async_copy(e_ref.at[pl.ds(0, GS * G)], buf.at[r], sems.at[q]).wait()
        tab_ref[q * GS:(q + 1) * GS, :] = jnp.dot(sel, buf[r, :], preferred_element_type=F32).astype(BF16)


def _index_call(chunk, ids, E, ntp):
    vs, d = E.shape
    ntok = ids.shape[0] * ids.shape[1]
    first = chunk is None
    return pl.pallas_call(
        functools.partial(_index_kernel, vs, ntp, first),
        out_shape=(
            jax.ShapeDtypeStruct((C, d), BF16),
            jax.ShapeDtypeStruct((ntok, 1), F32),
            jax.ShapeDtypeStruct((1, ntok), F32),
            jax.ShapeDtypeStruct((1, ntok), jnp.int32),
            jax.ShapeDtypeStruct((1, 128), jnp.int32),
            jax.ShapeDtypeStruct((4, ntok // ntp), F32),
            jax.ShapeDtypeStruct((1, 256), jnp.int32),
        ),
        in_specs=([] if first else [_sm()]) + [_vm(), pl.BlockSpec(memory_space=pltpu.HBM)],
        out_specs=(_vm(),) * 7,
        scratch_shapes=[
            VMEM((C * G, d), BF16),
            VMEM((8, 128), jnp.int32),
            pltpu.SMEM((8, 128), jnp.int32),
            pltpu.SemaphoreType.DMA,
            pltpu.SemaphoreType.DMA((C // GS,)),
        ],
        compiler_params=_params(8),
        cost_estimate=_cost(12),
        name="index_gather",
    )(*([] if first else [chunk.reshape(1)]), ids, E)


def _expand_kernel(ts, acc, *refs):
    if acc:
        x_in, pos, t0, t1, t2, t3, x_out, xl_out = refs
    else:
        pos, t0, t1, t2, t3, x_out, xl_out = refs
    oh = jnp.where(pos[...] == _iota((pos.shape[0], 4 * C), 1), 1.0, 0.0).astype(BF16)
    for c in range(x_out.shape[1] // CB):
        s = slice(c * CB, (c + 1) * CB)
        tab = jnp.concatenate([t[:, s] for t in (t0, t1, t2, t3)], axis=0)
        tot = jnp.dot(oh, tab, preferred_element_type=F32)
        if acc:
            tot = tot + x_in[:, s].astype(F32)
        x_out[:, s] = tot.astype(BF16)
    t = 4 * ts
    for k in range(x_out.shape[0] // t):
        at = pl.multiple_of(k * t + _me() * ts, ts)
        xl_out[k] = x_out[pl.ds(at, ts), :]


def _expand(pos, tabs, ts, x=None):
    ntok, d = pos.shape[0], tabs[0].shape[1]
    ins = ([x] if x is not None else []) + [pos, *tabs]
    return pl.pallas_call(
        functools.partial(_expand_kernel, ts, x is not None),
        out_shape=(jax.ShapeDtypeStruct((ntok, d), BF16), jax.ShapeDtypeStruct((ntok // (4 * ts), ts, d), BF16)),
        in_specs=[_vm()] * len(ins),
        out_specs=(_vm(), _vm()),
        compiler_params=_params(12),
        cost_estimate=_cost(3),
        name="expand",
    )(*ins)


def _p_kernel(ts, du_ref, w_ref, *refs):
    outs, (de, dur, z, sems) = refs[:-4], refs[-4:]
    nk = du_ref.shape[0]

    @pl.when(pl.program_id(0) == 0)
    def _():
        z[...] = jnp.zeros_like(z)
        for k in range(nk):
            for r in range(4):
                at = pl.multiple_of((_me() ^ r) * ts, ts)
                dur[pl.ds((r * nk + k) * ts, ts), :] = du_ref[k, pl.ds(at, ts), :]
        _fill(z, de, sems, 0, 0, ZP, False)

    out = lax.dot_general(dur[...], w_ref[...], (((1,), (1,)), ((), ())), preferred_element_type=F32)
    for i, o in enumerate(outs):
        o[...] = out[i * nk * ts:(i + 1) * nk * ts].astype(BF16)

    @pl.when(pl.program_id(0) == pl.num_programs(0) - 1)
    def _():
        _fill(z, de, sems, 0, 0, ZP, True)


def _p_terms(du, W, ts, vs):
    nk, t, f = du.shape
    d = W.shape[0]
    cb = 3 * CB
    out = pl.pallas_call(
        functools.partial(_p_kernel, ts),
        out_shape=(jax.ShapeDtypeStruct((nk * ts, d), BF16),) * 4 + (jax.ShapeDtypeStruct((vs, d), F32),),
        grid=(d // cb,),
        in_specs=[pl.BlockSpec((nk, t, f), lambda i: (0, 0, 0)), pl.BlockSpec((cb, f), lambda i: (i, 0))],
        out_specs=(pl.BlockSpec((nk * ts, cb), lambda i: (0, i)),) * 4 + (_any(),),
        scratch_shapes=[VMEM((nk * t, f), BF16)] + _zscratch(d, ZP),
        compiler_params=_params(20),
        cost_estimate=_cost(5),
        name="p_terms",
    )(du, W)
    return out[:4], out[4]


def _zero_kernel(lo, n, de_in, o, z, sems):
    z[...] = jnp.zeros_like(z)
    _fill(z, o, sems, lo, 0, n, False)
    _fill(z, o, sems, lo, 0, n, True)


def _zeros(de, lo, n):
    vs, d = de.shape
    return pl.pallas_call(
        functools.partial(_zero_kernel, lo, n),
        out_shape=jax.ShapeDtypeStruct((vs, d), F32),
        in_specs=[_any()],
        out_specs=_any(),
        scratch_shapes=_zscratch(d, n),
        input_output_aliases={0: 0},
        compiler_params=_params(4),
        cost_estimate=_cost(n * 0.375),
        name="zero_fill",
    )(de)


def _dx_kernel(x, p0, p1, p2, p3, dres, g, dx, dg):
    rows = 32
    tot = None
    for b in range(dx.shape[0] // rows):
        s = slice(b * rows, (b + 1) * rows)
        xf = x[s].astype(F32)
        rs = lax.rsqrt(jnp.mean(xf * xf, axis=-1, keepdims=True) + EPS)
        nh = xf * rs
        dn = (p0[s].astype(F32) + p1[s].astype(F32)) + (p2[s].astype(F32) + p3[s].astype(F32))
        gdn = g[...].astype(F32) * dn
        out = dres[s].astype(F32) + rs * (gdn - nh * jnp.mean(nh * gdn, axis=-1, keepdims=True))
        dx[s] = out.astype(BF16)
        part = jnp.sum(dn * nh, axis=0, keepdims=True)
        tot = part if tot is None else tot + part
    dg[...] = tot


def _dx(x, ps, dres, g):
    m, d = x.shape
    return pl.pallas_call(
        _dx_kernel,
        out_shape=(
            jax.ShapeDtypeStruct((m, d), BF16),
            jax.ShapeDtypeStruct((1, d), F32),
        ),
        in_specs=[_vm()] * 7,
        out_specs=(_vm(), _vm()),
        compiler_params=_params(12),
        cost_estimate=_cost(2),
        name="dx_form",
    )(x, *ps, dres, g)


def _sums_kernel(slot_ref, dx0, dx1, dg0, dg1, out):
    m = dx0.shape[0]
    j = _iota((C2, m), 0)
    ohs = [jnp.where(slot_ref[i:i + 1, :] == j, 1.0, 0.0).astype(BF16) for i in (2, 3)]
    last = lax.broadcasted_iota(jnp.int32, (C2, CB), 0) == C2 - 1
    for c in range(out.shape[1] // CB):
        s = slice(c * CB, (c + 1) * CB)
        tot = jnp.dot(ohs[0], dx0[:, s], preferred_element_type=F32)
        tot = tot + jnp.dot(ohs[1], dx1[:, s], preferred_element_type=F32)
        out[:, s] = jnp.where(last, dg0[:, s] + dg1[:, s], tot)


def _sums(slots, dx0, dx1, dg0, dg1):
    return pl.pallas_call(
        _sums_kernel,
        out_shape=jax.ShapeDtypeStruct((C2, dx0.shape[1]), F32),
        in_specs=[_vm()] * 5,
        out_specs=_vm(),
        compiler_params=_params(6),
        cost_estimate=_cost(1),
        name="dx_sums",
    )(slots, dx0, dx1, dg0, dg1)


def _u_kernel(x_ref, g_ref, w_ref, de_in, u_ref, n_ref, de, z, sems):
    z[...] = jnp.zeros_like(z)
    _fill(z, de, sems, AT_U, 0, ZU, False)
    rows = 64
    for b in range(n_ref.shape[0] // rows):
        s = slice(b * rows, (b + 1) * rows)
        xf = x_ref[s].astype(F32)
        rs = lax.rsqrt(jnp.mean(xf * xf, axis=-1, keepdims=True) + EPS)
        n_ref[s] = (xf * rs * g_ref[...].astype(F32)).astype(BF16)
    nk, t, f = u_ref.shape
    for c in range(f // CB):
        s = slice(c * CB, (c + 1) * CB)
        out = jnp.dot(n_ref[...], w_ref[:, s], preferred_element_type=F32).astype(BF16)
        for k in range(nk):
            u_ref[k, :, s] = out[k * t:(k + 1) * t]
    _fill(z, de, sems, AT_U, 0, ZU, True)


def _u(x, g, W, nk, de):
    ntok, d = x.shape
    f = W.shape[1]
    return pl.pallas_call(
        _u_kernel,
        out_shape=(
            jax.ShapeDtypeStruct((nk, ntok // nk, f), BF16),
            jax.ShapeDtypeStruct((ntok, d), BF16),
            jax.ShapeDtypeStruct(de.shape, F32),
        ),
        in_specs=[_vm(), _vm(), _vm(), _any()],
        out_specs=(_vm(), _vm(), _any()),
        scratch_shapes=_zscratch(d, ZU),
        input_output_aliases={3: 2},
        compiler_params=_params(20),
        cost_estimate=_cost(10),
        name="u_terms",
    )(x, g, W, de)


def _dw_kernel(lo, n, per, n_ref, du_ref, de_in, dw_ref, de, z, sems):
    i = pl.program_id(0)
    nk, t, f = du_ref.shape

    @pl.when(i == 0)
    def _():
        z[...] = jnp.zeros_like(z)

    _fill(z, de, sems, lo, i * per, jnp.minimum(per, n - i * per), False)
    dw_ref[...] = lax.dot_general(
        n_ref[...], du_ref[...].reshape(nk * t, f), (((0,), (0,)), ((), ())), preferred_element_type=F32
    )

    @pl.when(i == pl.num_programs(0) - 1)
    def _():
        _fill(z, de, sems, lo, 0, n, True)


def _dw(n, du, de, lo, nz):
    nk, t, f = du.shape
    ntok, d = n.shape
    cb = d // 6
    steps = d // cb
    return pl.pallas_call(
        functools.partial(_dw_kernel, lo, nz, -(-nz // steps)),
        out_shape=(jax.ShapeDtypeStruct((d, f), F32), jax.ShapeDtypeStruct(de.shape, F32)),
        grid=(steps,),
        in_specs=[
            pl.BlockSpec((ntok, cb), lambda i: (0, i)),
            pl.BlockSpec((nk, t, f), lambda i: (0, 0, 0)),
            _any(),
        ],
        out_specs=(pl.BlockSpec((cb, f), lambda i: (i, 0)), _any()),
        scratch_shapes=_zscratch(d, nz),
        input_output_aliases={2: 1},
        compiler_params=_params(20),
        cost_estimate=_cost(10),
        name="dw_terms",
    )(n, du, de)


def _scatter_kernel(ts, nk, cnt_ref, list_ref, srow_ref, *refs):
    pieces, (de_in, de, dx, acc, sem) = refs[:-5], refs[-5:]
    ntok = nk * 4 * ts
    for k in range(nk):
        for r in range(4):
            at = pl.multiple_of(k * 4 * ts + (_me() ^ r) * ts, ts)
            dx[pl.ds(at, ts), :] = pieces[r][k * ts:(k + 1) * ts, :]
    cnt = cnt_ref[0, 1]

    def chunk(i, carry):
        base = i * C
        slot = (lax.broadcasted_iota(jnp.int32, (C, ntok), 0) + base).astype(F32)
        oh = jnp.where(slot == srow_ref[...], 1.0, 0.0).astype(BF16)
        for c in range(acc.shape[1] // CB):
            s = slice(c * CB, (c + 1) * CB)
            acc[:, s] = jnp.dot(oh, dx[:, s], preferred_element_type=F32)
        here = jnp.minimum(cnt - base, C)

        def put(j, c2):
            row = list_ref[0, base + j]
            pltpu.make_async_copy(acc.at[pl.ds(j, 1)], de.at[pl.ds(row, 1)], sem).start()
            return c2

        def done(j, c2):
            pltpu.make_async_copy(acc.at[pl.ds(j, 1)], de.at[pl.ds(0, 1)], sem).wait()
            return c2

        lax.fori_loop(0, here, put, 0)
        lax.fori_loop(0, here, done, 0)
        return carry

    lax.fori_loop(0, (cnt + C - 1) // C, chunk, 0)


def _scatter(cnts, rows, srow, pieces, de, ts, nk):
    vs, d = de.shape
    ntok = srow.shape[1]
    return pl.pallas_call(
        functools.partial(_scatter_kernel, ts, nk),
        out_shape=jax.ShapeDtypeStruct((vs, d), F32),
        in_specs=[_sm(), _sm(), _vm()] + [_vm()] * len(pieces) + [_any()],
        out_specs=_any(),
        scratch_shapes=[VMEM((ntok, d), BF16), VMEM((C, d), F32), pltpu.SemaphoreType.DMA],
        input_output_aliases={3 + len(pieces): 0},
        compiler_params=_params(16),
        cost_estimate=_cost(3),
        name="scatter_rows",
    )(cnts, rows, srow, *pieces, de)


def _acc_kernel(lo, n, cnt_ref, oth_ref, list_ref, slot_ref, dx0, dx1, de_in, de, acc, flag, z, sems, sem):
    z[...] = jnp.zeros_like(z)
    _fill(z, de, sems, lo, 0, n, False)
    for i in (0, 2):
        flag[0, i] = jnp.maximum(cnt_ref[0, i], oth_ref[0, i])
    m = dx0.shape[0]
    j = _iota((C, m), 0)
    ohs = [jnp.where(slot_ref[i:i + 1, :] == j, 1.0, 0.0).astype(BF16) for i in (0, 1)]
    for c in range(acc.shape[1] // CB):
        s = slice(c * CB, (c + 1) * CB)
        tot = jnp.dot(ohs[0], dx0[:, s], preferred_element_type=F32)
        acc[:, s] = tot + jnp.dot(ohs[1], dx1[:, s], preferred_element_type=F32)
    _fill(z, de, sems, lo, 0, n, True)
    here = jnp.minimum(cnt_ref[0, 1], C)

    def put(j, carry):
        pltpu.make_async_copy(acc.at[pl.ds(j, 1)], de.at[pl.ds(list_ref[0, j], 1)], sem).start()
        return carry

    def done(j, carry):
        pltpu.make_async_copy(acc.at[pl.ds(j, 1)], de.at[pl.ds(0, 1)], sem).wait()
        return carry

    lax.fori_loop(0, here, put, 0)
    lax.fori_loop(0, here, done, 0)


def _acc(cnts, other, rows, slots, dx0, dx1, de, lo):
    vs, d = de.shape
    n = vs // ZR - lo
    return pl.pallas_call(
        functools.partial(_acc_kernel, lo, n),
        out_shape=(
            jax.ShapeDtypeStruct((vs, d), F32),
            jax.ShapeDtypeStruct((C, d), F32),
            jax.ShapeDtypeStruct((1, 4), jnp.int32),
        ),
        in_specs=[_sm(), _sm(), _sm()] + [_vm()] * 3 + [_any()],
        out_specs=(_any(), _vm(), _sm()),
        scratch_shapes=_zscratch(d, n) + [pltpu.SemaphoreType.DMA],
        input_output_aliases={6: 0},
        compiler_params=_params(8),
        cost_estimate=_cost(n * 0.375),
        name="fill_acc",
    )(cnts, other, rows, slots, dx0, dx1, de)


def _write_kernel(map_ref, acc, mine_ref, got_ref, de_in, de, dg_out, out, sem):
    n = jnp.minimum(map_ref[0, 127], C2 - 1)

    def put(j, carry):
        out[pl.ds(j, 1), :] = acc[pl.ds(map_ref[0, j], 1), :] + got_ref[pl.ds(j, 1), :]
        pltpu.make_async_copy(out.at[pl.ds(j, 1)], de.at[pl.ds(map_ref[0, 128 + j], 1)], sem).start()
        return carry

    def done(j, carry):
        pltpu.make_async_copy(out.at[pl.ds(j, 1)], de.at[pl.ds(0, 1)], sem).wait()
        return carry

    lax.fori_loop(0, n, put, 0)
    dg = mine_ref[C2 - 1:C2, :] + got_ref[C2 - 1:C2, :]
    dg_out[...] = dg.reshape(dg_out.shape)
    lax.fori_loop(0, n, done, 0)


def _write(where, acc, mine, got, de):
    vs, d = de.shape
    return pl.pallas_call(
        _write_kernel,
        out_shape=(jax.ShapeDtypeStruct((vs, d), F32), jax.ShapeDtypeStruct((d,), F32)),
        in_specs=[_sm()] + [_vm()] * 3 + [_any()],
        out_specs=(_any(), _vm()),
        scratch_shapes=[VMEM((C2, d), F32), pltpu.SemaphoreType.DMA],
        input_output_aliases={4: 0},
        compiler_params=_params(6),
        cost_estimate=_cost(3),
        name="write_rows",
    )(where, acc, mine, got, de)


def solution(mesh):
    ntp = mesh.shape["tp"]
    ndp = mesh.shape["dp"]

    def swap(a, bit):
        return lax.ppermute(a, "tp", [(i, i ^ bit) for i in range(ntp)])

    def share(t):
        t2 = swap(t, 2)
        t1 = swap(t, 1)
        return t, t1, t2, swap(t2, 1)

    def p_terms(du, W, ts, vs):
        q, de = _p_terms(du, W, ts, vs)
        return de, (q[0], swap(q[1], 1), swap(q[2], 2), swap(q[3], 3))

    def body(ids, E, g, W, du, dres):
        vs, d = E.shape
        nk, t = ids.shape
        ts = t // ntp
        m = nk * ts
        g2 = g.reshape(1, d)

        tab, pos, _, rows, cnts, slots, where = _index_call(None, ids, E, ntp)
        tabs = share(tab)
        de, ps = p_terms(du, W, ts, vs)
        x, xl = _expand(pos, tabs, ts)
        u, n, de = _u(x, g2, W, nk, de)
        dW, de = _dw(n, du, de, AT_W, ZW)
        dx, dg = _dx(xl.reshape(m, d), ps, dres.reshape(m, d), g2)
        dx1, dg1 = swap(dx, 1), swap(dg, 1)
        mine = _sums(slots, dx, dx1, dg, dg1)
        got = swap(mine, 2)
        other = lax.ppermute(cnts, "dp", [(i, (i + 1) % ndp) for i in range(ndp)])
        de, acc, flags = _acc(cnts, other, rows, slots, dx, dx1, de, AT_R)
        dE, dg = _write(where, acc, mine, got, de)
        outs = u, xl, dE, dW, dg

        inputs = ids, E, W, du, dres, g2, flags

        def again(c):
            ids, E, W, du, dres, g2, fl, left = lax.optimization_barrier((*inputs, c[0]))
            rounds = fl[0, 0]
            i0 = left - left

            def more(q):
                i, x, _ = q
                tab, pos, *_ = _index_call(i, ids, E, ntp)
                return i + 1, *_expand(pos, share(tab), ts, x)

            zeros = jnp.zeros((nk * t, d), BF16), jnp.zeros((nk, ts, d), BF16)
            _, x, xl = lax.while_loop(lambda q: q[0] < rounds, more, (i0, *zeros))
            _, _, srow, rows, cs, _, _ = _index_call(i0, ids, E, ntp)
            de, ps = p_terms(du, W, ts, vs)
            u, n, de = _u(x, g2, W, nk, de)
            dW, de = _dw(n, du, de, AT_W, ZW)
            dx, dg = _dx(xl.reshape(m, d), ps, dres.reshape(m, d), g2)
            dg2 = dg + swap(dg, 1)
            dg = (dg2 + swap(dg2, 2)).reshape(d)
            dE = _scatter(cs, rows, srow, share(dx), _zeros(de, AT_R, vs // ZR - AT_R), ts, nk)
            return i0, (u, xl, dE, dW, dg)

        _, outs = lax.while_loop(lambda c: c[0] > 0, again, (jnp.minimum(flags[0, 2], 1), outs))
        return outs

    return jax.shard_map(
        body,
        mesh=mesh,
        in_specs=(P("dp", None), P("tp", None), P(None), P(None, "tp"), P("dp", None, "tp"), P("dp", "tp", None)),
        out_specs=(P("dp", None, "tp"), P("dp", "tp", None), P(("dp", "tp"), None), P("dp", "tp"), P("dp")),
        check_vma=False,
    )
```

```python
import functools

import jax
import jax.numpy as jnp
from jax import lax
from jax.experimental import pallas as pl
from jax.experimental.pallas import tpu as pltpu
from jax.sharding import PartitionSpec as P


EPS = 1e-6
C = 64
G = 2
GS = 64
C2 = 32
CB = 256
ZR = 128
ZP, ZA, ZU, ZW, ZB = 8, 4, 15, 21, 3
AT_A, AT_U, AT_W, AT_B, AT_R = ZP, ZP + ZA, ZP + ZA + ZU, ZP + ZA + ZU + ZW, ZP + ZA + ZU + ZW + ZB
TB = 64

F32 = jnp.float32
BF16 = jnp.bfloat16
VMEM = pltpu.VMEM


def _sm():
    return pl.BlockSpec(memory_space=pltpu.SMEM)


def _vm():
    return pl.BlockSpec(memory_space=pltpu.VMEM)


def _any():
    return pl.BlockSpec(memory_space=pl.ANY)


def _params(mb):
    return pltpu.CompilerParams(vmem_limit_bytes=mb << 20)


def _cost(us):
    return pl.CostEstimate(flops=int(us * 4_000_000_000), bytes_accessed=1_000_000, transcendentals=0)


def _iota(shape, dim):
    return lax.broadcasted_iota(jnp.int32, shape, dim).astype(F32)


def _me():
    return lax.axis_index("tp").astype(jnp.int32)


def _fill(z, o, sems, lo, first, n, wait):
    def step(i, carry):
        at = pl.multiple_of((lo + i) * ZR, ZR)
        c = pltpu.make_async_copy(z, o.at[pl.ds(at, ZR)], sems.at[i])
        c.wait() if wait else c.start()
        return carry

    lax.fori_loop(first, first + n, step, 0)


def _zscratch(d, n):
    return [VMEM((ZR, d), F32), pltpu.SemaphoreType.DMA((n,))]


def _index_kernel(vs, ntp, first, *refs):
    if first:
        ids_ref, e_ref, tab_ref, pos_ref, srow_ref, list_ref, cnt_ref, slot_ref, map_ref, buf, glv, gls, gsem, sems = refs
        base = 0.0
    else:
        c_ref, ids_ref, e_ref, tab_ref, pos_ref, srow_ref, list_ref, cnt_ref, slot_ref, map_ref, buf, glv, gls, gsem, sems = refs
        base = (c_ref[0] * C).astype(F32)
    mei = _me()
    me = mei.astype(F32)
    lo = me * vs
    nk, t = ids_ref.shape
    ntok = nk * t
    nb = ntok // TB
    idsf = ids_ref[...].astype(F32)
    idr = jnp.concatenate([idsf[k:k + 1] for k in range(nk)], axis=1)

    def column(row, b):
        w = (b * TB) // 128 * 128
        part = jnp.broadcast_to(row[:, w:w + 128], (TB, 128))
        hit = _iota((TB, 128), 1) == _iota((TB, 128), 0) + float(b * TB - w)
        return jnp.sum(jnp.where(hit, part, 0.0), axis=1, keepdims=True)

    def fold(a):
        return sum(a[8 * q:8 * q + 8] for q in range(1, TB // 8)) + a[:8]

    lane = _iota((TB, ntok), 1)
    thr = _iota((TB, 128), 1) * float(vs)
    rank8 = jnp.zeros((8, ntok), F32)
    below8 = jnp.zeros((8, 128), F32)
    idcs = []
    for b in range(nb):
        idc = column(idr, b)
        idcs.append(idc)
        idb = jnp.broadcast_to(idc, (TB, ntok))
        dup = (idb == idr) & (lane < _iota((TB, ntok), 0) + float(b * TB))
        seen = jnp.max(jnp.where(dup, 1.0, 0.0), axis=1, keepdims=True)
        key = jnp.where(seen > 0.5, float(vs * ntp), idc)
        rank8 = rank8 + fold(jnp.where(jnp.broadcast_to(key, (TB, ntok)) < idr, 1.0, 0.0))
        below8 = below8 + fold(jnp.where(jnp.broadcast_to(key, (TB, 128)) < thr, 1.0, 0.0))
    rank = jnp.sum(rank8, axis=0, keepdims=True)
    below = jnp.sum(below8, axis=0, keepdims=True)
    own_r = jnp.floor(idr * (1.0 / vs))
    start = jnp.zeros_like(rank)
    cnt = jnp.zeros((1, 1), F32)
    mx = jnp.zeros((1, 1), F32)
    for d in range(ntp):
        ld = below[:, d:d + 1]
        nd = below[:, d + 1:d + 2] - ld
        start = jnp.where(own_r == float(d), ld, start)
        cnt = jnp.where(me == float(d), nd, cnt)
        mx = jnp.maximum(mx, nd)
    slot_r = rank - start
    my_r = jnp.where(own_r == me, slot_r, -1.0)

    slot_l = _iota((TB, 128), 1) + base
    acc = jnp.zeros((TB, 128), F32)
    mys = []
    for b in range(nb):
        my_c = column(my_r, b)
        mys.append(my_c)
        acc = jnp.maximum(acc, jnp.where(my_c == slot_l, idcs[b] - lo, 0.0))
    glv[...] = jnp.broadcast_to(jnp.max(acc, axis=0, keepdims=True), (8, 128)).astype(jnp.int32)
    cp = pltpu.make_async_copy(glv, gls, gsem)
    cp.start()
    cp.wait()

    def fetch(q, j, carry):
        j = q * GS + j
        g = pl.multiple_of((gls[0, j] >> 1) << 1, G)
        at = pl.multiple_of(j * G, G)
        pltpu.make_async_copy(e_ref.at[pl.ds(g, G)], buf.at[pl.ds(at, G)], sems.at[q]).start()
        return carry

    for q in range(C // GS):
        lax.fori_loop(0, GS, functools.partial(fetch, q), 0, unroll=8)

    ts = t // ntp
    part = lax.broadcasted_iota(jnp.int32, (1, ntok), 1) // ts % ntp
    chips = [jnp.where(part // 2 == c, 1.0, 0.0) for c in range(ntp // 2)]
    rank28 = jnp.zeros((8, ntok), F32)
    below28 = [jnp.zeros((8, 128), F32) for _ in chips]
    for b in range(nb):
        idc = idcs[b]
        dup = (jnp.broadcast_to(idc, (TB, ntok)) == idr) & (lane < _iota((TB, ntok), 0) + float(b * TB))
        c = b * TB // ts % ntp // 2
        seen = jnp.max(jnp.where(dup, chips[c], 0.0), axis=1, keepdims=True)
        key = jnp.where(seen > 0.5, float(vs * ntp), idc)
        rank28 = rank28 + fold(jnp.where(jnp.broadcast_to(key, (TB, ntok)) < idr, chips[c], 0.0))
        below28[c] = below28[c] + fold(jnp.where(jnp.broadcast_to(key, (TB, 128)) < thr, 1.0, 0.0))
    rank2 = jnp.sum(rank28, axis=0, keepdims=True)
    below2 = [jnp.sum(b8, axis=0, keepdims=True) for b8 in below28]
    start2 = jnp.zeros_like(rank)
    cnt2 = jnp.zeros((1, 1), F32)
    mx2 = jnp.zeros((1, 1), F32)
    for c, chip in enumerate(chips):
        for d in range(ntp):
            ld = below2[c][:, d:d + 1]
            nd = below2[c][:, d + 1:d + 2] - ld
            start2 = jnp.where((own_r == float(d)) & (chip > 0.5), ld, start2)
            if d // 2 != c:
                cnt2 = jnp.where(me == float(d), nd, cnt2)
                mx2 = jnp.maximum(mx2, nd)
    slot2_r = rank2 - start2
    srow_ref[...] = my_r
    full = jnp.zeros((8, ntok), F32)
    lane8 = _iota((8, ntok), 1)
    for b in range(nb):
        for q in range(TB // 8):
            s = slice(8 * q, 8 * q + 8)
            full = jnp.maximum(full, jnp.where(mys[b][s] == lane8, idcs[b][s] - lo, 0.0))
    list_ref[...] = jnp.max(full, axis=0, keepdims=True).astype(jnp.int32)
    rel = (own_r.astype(jnp.int32) ^ mei).astype(F32)
    pos = jnp.where((slot_r >= base) & (slot_r < base + C), rel * C + slot_r - base, -1.0)
    for b in range(nb):
        pos_ref[b * TB:(b + 1) * TB, :] = column(pos, b)
    lane1 = lax.broadcasted_iota(jnp.int32, (1, 128), 1)
    over = jnp.where((mx > C) | (mx2 > C2 - 1), 1.0, 0.0)
    rounds = jnp.floor((mx + C - 1.0) * (1.0 / C))
    cnts = jnp.where(lane1 == 0, rounds, jnp.where(lane1 == 1, cnt, jnp.where(lane1 == 2, over, cnt2)))
    cnt_ref[...] = cnts.astype(jnp.int32)
    facing = (mei ^ 2).astype(F32)
    sums_r = jnp.where(own_r == facing, slot2_r, -1.0)
    rows = [jnp.zeros((1, nk * ts), F32)] * 4
    for q in range(ntp):
        at = [slice(k * t + q * ts, k * t + (q + 1) * ts) for k in range(nk)]
        mine = jnp.concatenate([my_r[:, w] for w in at], axis=1)
        sums = jnp.concatenate([sums_r[:, w] for w in at], axis=1)
        own, sib = me == float(q), me == float(q ^ 1)
        rows = [
            jnp.where(own, mine, rows[0]), jnp.where(sib, mine, rows[1]),
            jnp.where(own, sums, rows[2]), jnp.where(sib, sums, rows[3]),
        ]
    for j, r in enumerate(rows):
        slot_ref[j:j + 1, :] = r
    far = (part // 2).astype(F32) != jnp.floor(me * 0.5)
    got_r = jnp.where(far & (own_r == me), slot2_r, -1.0)
    acc2 = jnp.zeros((TB, 128), F32)
    slot_j = _iota((TB, 128), 1)
    for b in range(nb):
        acc2 = jnp.maximum(acc2, jnp.where(column(got_r, b) == slot_j, mys[b], 0.0))
    slots = jnp.minimum(jnp.max(acc2, axis=0, keepdims=True), C - 1.0)
    many = jnp.where(lane1 == 127, cnt2, slots)
    mine = jnp.where(lane1 == 127, cnt, jnp.max(full, axis=0, keepdims=True)[:, :128])
    map_ref[...] = jnp.concatenate([many, mine], axis=1).astype(jnp.int32)
    hit = jnp.where(my_r == _iota((C, ntok), 0) + base, idr - lo, 0.0)
    want = jnp.max(hit, axis=1, keepdims=True)
    want = want - jnp.floor(want * (1.0 / G)) * G
    for q in range(C // GS):
        r = slice(q * GS * G, (q + 1) * GS * G)
        mine = want[q * GS:(q + 1) * GS] + _iota((GS, 1), 0) * G
        sel = jnp.where(_iota((GS, GS * G), 1) == mine, 1.0, 0.0).astype(BF16)
        pltpu.make_async_copy(e_ref.at[pl.ds(0, GS * G)], buf.at[r], sems.at[q]).wait()
        tab_ref[q * GS:(q + 1) * GS, :] = jnp.dot(sel, buf[r, :], preferred_element_type=F32).astype(BF16)


def _index_call(chunk, ids, E, ntp):
    vs, d = E.shape
    ntok = ids.shape[0] * ids.shape[1]
    first = chunk is None
    return pl.pallas_call(
        functools.partial(_index_kernel, vs, ntp, first),
        out_shape=(
            jax.ShapeDtypeStruct((C, d), BF16),
            jax.ShapeDtypeStruct((ntok, 1), F32),
            jax.ShapeDtypeStruct((1, ntok), F32),
            jax.ShapeDtypeStruct((1, ntok), jnp.int32),
            jax.ShapeDtypeStruct((1, 128), jnp.int32),
            jax.ShapeDtypeStruct((4, ntok // ntp), F32),
            jax.ShapeDtypeStruct((1, 256), jnp.int32),
        ),
        in_specs=([] if first else [_sm()]) + [_vm(), pl.BlockSpec(memory_space=pltpu.HBM)],
        out_specs=(_vm(),) * 7,
        scratch_shapes=[
            VMEM((C * G, d), BF16),
            VMEM((8, 128), jnp.int32),
            pltpu.SMEM((8, 128), jnp.int32),
            pltpu.SemaphoreType.DMA,
            pltpu.SemaphoreType.DMA((C // GS,)),
        ],
        compiler_params=_params(8),
        cost_estimate=_cost(12),
        name="index_gather",
    )(*([] if first else [chunk.reshape(1)]), ids, E)


def _expand_kernel(ts, acc, *refs):
    if acc:
        x_in, pos, t0, t1, t2, t3, x_out, xl_out = refs
    else:
        pos, t0, t1, t2, t3, x_out, xl_out = refs
    oh = jnp.where(pos[...] == _iota((pos.shape[0], 4 * C), 1), 1.0, 0.0).astype(BF16)
    for c in range(x_out.shape[1] // CB):
        s = slice(c * CB, (c + 1) * CB)
        tab = jnp.concatenate([t[:, s] for t in (t0, t1, t2, t3)], axis=0)
        tot = jnp.dot(oh, tab, preferred_element_type=F32)
        if acc:
            tot = tot + x_in[:, s].astype(F32)
        x_out[:, s] = tot.astype(BF16)
    t = 4 * ts
    for k in range(x_out.shape[0] // t):
        at = pl.multiple_of(k * t + _me() * ts, ts)
        xl_out[k] = x_out[pl.ds(at, ts), :]


def _expand(pos, tabs, ts, x=None):
    ntok, d = pos.shape[0], tabs[0].shape[1]
    ins = ([x] if x is not None else []) + [pos, *tabs]
    return pl.pallas_call(
        functools.partial(_expand_kernel, ts, x is not None),
        out_shape=(jax.ShapeDtypeStruct((ntok, d), BF16), jax.ShapeDtypeStruct((ntok // (4 * ts), ts, d), BF16)),
        in_specs=[_vm()] * len(ins),
        out_specs=(_vm(), _vm()),
        compiler_params=_params(12),
        cost_estimate=_cost(3),
        name="expand",
    )(*ins)


def _p_kernel(ts, du_ref, w_ref, *refs):
    outs, (de, dur, z, sems) = refs[:-4], refs[-4:]
    nk = du_ref.shape[0]

    @pl.when(pl.program_id(0) == 0)
    def _():
        z[...] = jnp.zeros_like(z)
        for k in range(nk):
            for r in range(4):
                at = pl.multiple_of((_me() ^ r) * ts, ts)
                dur[pl.ds((r * nk + k) * ts, ts), :] = du_ref[k, pl.ds(at, ts), :]
        _fill(z, de, sems, 0, 0, ZP, False)

    out = lax.dot_general(dur[...], w_ref[...], (((1,), (1,)), ((), ())), preferred_element_type=F32)
    for i, o in enumerate(outs):
        o[...] = out[i * nk * ts:(i + 1) * nk * ts].astype(BF16)

    @pl.when(pl.program_id(0) == pl.num_programs(0) - 1)
    def _():
        _fill(z, de, sems, 0, 0, ZP, True)


def _p_terms(du, W, ts, vs):
    nk, t, f = du.shape
    d = W.shape[0]
    cb = 3 * CB
    out = pl.pallas_call(
        functools.partial(_p_kernel, ts),
        out_shape=(jax.ShapeDtypeStruct((nk * ts, d), BF16),) * 4 + (jax.ShapeDtypeStruct((vs, d), F32),),
        grid=(d // cb,),
        in_specs=[pl.BlockSpec((nk, t, f), lambda i: (0, 0, 0)), pl.BlockSpec((cb, f), lambda i: (i, 0))],
        out_specs=(pl.BlockSpec((nk * ts, cb), lambda i: (0, i)),) * 4 + (_any(),),
        scratch_shapes=[VMEM((nk * t, f), BF16)] + _zscratch(d, ZP),
        compiler_params=_params(20),
        cost_estimate=_cost(5),
        name="p_terms",
    )(du, W)
    return out[:4], out[4]


def _zero_kernel(lo, n, de_in, o, z, sems):
    z[...] = jnp.zeros_like(z)
    _fill(z, o, sems, lo, 0, n, False)
    _fill(z, o, sems, lo, 0, n, True)


def _zeros(de, lo, n):
    vs, d = de.shape
    return pl.pallas_call(
        functools.partial(_zero_kernel, lo, n),
        out_shape=jax.ShapeDtypeStruct((vs, d), F32),
        in_specs=[_any()],
        out_specs=_any(),
        scratch_shapes=_zscratch(d, n),
        input_output_aliases={0: 0},
        compiler_params=_params(4),
        cost_estimate=_cost(n * 0.375),
    )(de)


def _dx_kernel(x, p0, p1, p2, p3, dres, g, dx, dg):
    rows = 32
    tot = None
    for b in range(dx.shape[0] // rows):
        s = slice(b * rows, (b + 1) * rows)
        xf = x[s].astype(F32)
        rs = lax.rsqrt(jnp.mean(xf * xf, axis=-1, keepdims=True) + EPS)
        nh = xf * rs
        dn = (p0[s].astype(F32) + p1[s].astype(F32)) + (p2[s].astype(F32) + p3[s].astype(F32))
        gdn = g[...].astype(F32) * dn
        out = dres[s].astype(F32) + rs * (gdn - nh * jnp.mean(nh * gdn, axis=-1, keepdims=True))
        dx[s] = out.astype(BF16)
        part = jnp.sum(dn * nh, axis=0, keepdims=True)
        tot = part if tot is None else tot + part
    dg[...] = tot


def _dx(x, ps, dres, g):
    m, d = x.shape
    return pl.pallas_call(
        _dx_kernel,
        out_shape=(
            jax.ShapeDtypeStruct((m, d), BF16),
            jax.ShapeDtypeStruct((1, d), F32),
        ),
        in_specs=[_vm()] * 7,
        out_specs=(_vm(), _vm()),
        compiler_params=_params(12),
        cost_estimate=_cost(2),
        name="dx_form",
    )(x, *ps, dres, g)


def _sums_kernel(slot_ref, dx0, dx1, dg0, dg1, out):
    m = dx0.shape[0]
    j = _iota((C2, m), 0)
    ohs = [jnp.where(slot_ref[i:i + 1, :] == j, 1.0, 0.0).astype(BF16) for i in (2, 3)]
    last = lax.broadcasted_iota(jnp.int32, (C2, CB), 0) == C2 - 1
    for c in range(out.shape[1] // CB):
        s = slice(c * CB, (c + 1) * CB)
        tot = jnp.dot(ohs[0], dx0[:, s], preferred_element_type=F32)
        tot = tot + jnp.dot(ohs[1], dx1[:, s], preferred_element_type=F32)
        out[:, s] = jnp.where(last, dg0[:, s] + dg1[:, s], tot)


def _sums(slots, dx0, dx1, dg0, dg1):
    return pl.pallas_call(
        _sums_kernel,
        out_shape=jax.ShapeDtypeStruct((C2, dx0.shape[1]), F32),
        in_specs=[_vm()] * 5,
        out_specs=_vm(),
        compiler_params=_params(6),
        cost_estimate=_cost(1),
        name="dx_sums",
    )(slots, dx0, dx1, dg0, dg1)


def _u_kernel(x_ref, g_ref, w_ref, de_in, u_ref, n_ref, de, z, sems):
    z[...] = jnp.zeros_like(z)
    _fill(z, de, sems, AT_U, 0, ZU, False)
    rows = 64
    for b in range(n_ref.shape[0] // rows):
        s = slice(b * rows, (b + 1) * rows)
        xf = x_ref[s].astype(F32)
        rs = lax.rsqrt(jnp.mean(xf * xf, axis=-1, keepdims=True) + EPS)
        n_ref[s] = (xf * rs * g_ref[...].astype(F32)).astype(BF16)
    nk, t, f = u_ref.shape
    for c in range(f // CB):
        s = slice(c * CB, (c + 1) * CB)
        out = jnp.dot(n_ref[...], w_ref[:, s], preferred_element_type=F32).astype(BF16)
        for k in range(nk):
            u_ref[k, :, s] = out[k * t:(k + 1) * t]
    _fill(z, de, sems, AT_U, 0, ZU, True)


def _u(x, g, W, nk, de):
    ntok, d = x.shape
    f = W.shape[1]
    return pl.pallas_call(
        _u_kernel,
        out_shape=(
            jax.ShapeDtypeStruct((nk, ntok // nk, f), BF16),
            jax.ShapeDtypeStruct((ntok, d), BF16),
            jax.ShapeDtypeStruct(de.shape, F32),
        ),
        in_specs=[_vm(), _vm(), _vm(), _any()],
        out_specs=(_vm(), _vm(), _any()),
        scratch_shapes=_zscratch(d, ZU),
        input_output_aliases={3: 2},
        compiler_params=_params(20),
        cost_estimate=_cost(10),
        name="u_terms",
    )(x, g, W, de)


def _dw_kernel(lo, n, per, n_ref, du_ref, de_in, dw_ref, de, z, sems):
    i = pl.program_id(0)
    nk, t, f = du_ref.shape

    @pl.when(i == 0)
    def _():
        z[...] = jnp.zeros_like(z)

    _fill(z, de, sems, lo, i * per, jnp.minimum(per, n - i * per), False)
    dw_ref[...] = lax.dot_general(
        n_ref[...], du_ref[...].reshape(nk * t, f), (((0,), (0,)), ((), ())), preferred_element_type=F32
    )

    @pl.when(i == pl.num_programs(0) - 1)
    def _():
        _fill(z, de, sems, lo, 0, n, True)


def _dw(n, du, de, lo, nz):
    nk, t, f = du.shape
    ntok, d = n.shape
    cb = d // 6
    steps = d // cb
    return pl.pallas_call(
        functools.partial(_dw_kernel, lo, nz, -(-nz // steps)),
        out_shape=(jax.ShapeDtypeStruct((d, f), F32), jax.ShapeDtypeStruct(de.shape, F32)),
        grid=(steps,),
        in_specs=[
            pl.BlockSpec((ntok, cb), lambda i: (0, i)),
            pl.BlockSpec((nk, t, f), lambda i: (0, 0, 0)),
            _any(),
        ],
        out_specs=(pl.BlockSpec((cb, f), lambda i: (i, 0)), _any()),
        scratch_shapes=_zscratch(d, nz),
        input_output_aliases={2: 1},
        compiler_params=_params(20),
        cost_estimate=_cost(10),
        name="dw_terms",
    )(n, du, de)


def _scatter_kernel(ts, nk, cnt_ref, list_ref, srow_ref, *refs):
    pieces, (de_in, de, dx, acc, sem) = refs[:-5], refs[-5:]
    ntok = nk * 4 * ts
    for k in range(nk):
        for r in range(4):
            at = pl.multiple_of(k * 4 * ts + (_me() ^ r) * ts, ts)
            dx[pl.ds(at, ts), :] = pieces[r][k * ts:(k + 1) * ts, :]
    cnt = cnt_ref[0, 1]

    def chunk(i, carry):
        base = i * C
        slot = (lax.broadcasted_iota(jnp.int32, (C, ntok), 0) + base).astype(F32)
        oh = jnp.where(slot == srow_ref[...], 1.0, 0.0).astype(BF16)
        for c in range(acc.shape[1] // CB):
            s = slice(c * CB, (c + 1) * CB)
            acc[:, s] = jnp.dot(oh, dx[:, s], preferred_element_type=F32)
        here = jnp.minimum(cnt - base, C)

        def put(j, c2):
            row = list_ref[0, base + j]
            pltpu.make_async_copy(acc.at[pl.ds(j, 1)], de.at[pl.ds(row, 1)], sem).start()
            return c2

        def done(j, c2):
            pltpu.make_async_copy(acc.at[pl.ds(j, 1)], de.at[pl.ds(0, 1)], sem).wait()
            return c2

        lax.fori_loop(0, here, put, 0)
        lax.fori_loop(0, here, done, 0)
        return carry

    lax.fori_loop(0, (cnt + C - 1) // C, chunk, 0)


def _scatter(cnts, rows, srow, pieces, de, ts, nk):
    vs, d = de.shape
    ntok = srow.shape[1]
    return pl.pallas_call(
        functools.partial(_scatter_kernel, ts, nk),
        out_shape=jax.ShapeDtypeStruct((vs, d), F32),
        in_specs=[_sm(), _sm(), _vm()] + [_vm()] * len(pieces) + [_any()],
        out_specs=_any(),
        scratch_shapes=[VMEM((ntok, d), BF16), VMEM((C, d), F32), pltpu.SemaphoreType.DMA],
        input_output_aliases={3 + len(pieces): 0},
        compiler_params=_params(16),
        cost_estimate=_cost(3),
        name="scatter_rows",
    )(cnts, rows, srow, *pieces, de)


def _acc_kernel(lo, n, cnt_ref, oth_ref, slot_ref, dx0, dx1, de_in, de, acc, flag, z, sems):
    z[...] = jnp.zeros_like(z)
    _fill(z, de, sems, lo, 0, n, False)
    for i in (0, 2):
        flag[0, i] = jnp.maximum(cnt_ref[0, i], oth_ref[0, i])
    m = dx0.shape[0]
    j = _iota((C, m), 0)
    ohs = [jnp.where(slot_ref[i:i + 1, :] == j, 1.0, 0.0).astype(BF16) for i in (0, 1)]
    for c in range(acc.shape[1] // CB):
        s = slice(c * CB, (c + 1) * CB)
        tot = jnp.dot(ohs[0], dx0[:, s], preferred_element_type=F32)
        acc[:, s] = tot + jnp.dot(ohs[1], dx1[:, s], preferred_element_type=F32)
    _fill(z, de, sems, lo, 0, n, True)


def _acc(cnts, other, slots, dx0, dx1, de, lo):
    vs, d = de.shape
    n = vs // ZR - lo
    return pl.pallas_call(
        functools.partial(_acc_kernel, lo, n),
        out_shape=(
            jax.ShapeDtypeStruct((vs, d), F32),
            jax.ShapeDtypeStruct((C, d), F32),
            jax.ShapeDtypeStruct((1, 4), jnp.int32),
        ),
        in_specs=[_sm(), _sm()] + [_vm()] * 3 + [_any()],
        out_specs=(_any(), _vm(), _sm()),
        scratch_shapes=_zscratch(d, n),
        input_output_aliases={5: 0},
        compiler_params=_params(8),
        cost_estimate=_cost(n * 0.375),
        name="fill_acc",
    )(cnts, other, slots, dx0, dx1, de)


def _write_kernel(map_ref, acc_in, mine_ref, got_ref, de_in, de, dg_out, acc, sem):
    acc[...] = acc_in[...]

    def add(j, carry):
        at = pl.ds(map_ref[0, j], 1)
        acc[at, :] = acc[at, :] + got_ref[pl.ds(j, 1), :]
        return carry

    lax.fori_loop(0, jnp.minimum(map_ref[0, 127], C2 - 1), add, 0)
    n = jnp.minimum(map_ref[0, 255], C)

    def put(j, carry):
        pltpu.make_async_copy(acc.at[pl.ds(j, 1)], de.at[pl.ds(map_ref[0, 128 + j], 1)], sem).start()
        return carry

    def done(j, carry):
        pltpu.make_async_copy(acc.at[pl.ds(j, 1)], de.at[pl.ds(0, 1)], sem).wait()
        return carry

    lax.fori_loop(0, n, put, 0)
    dg = mine_ref[C2 - 1:C2, :] + got_ref[C2 - 1:C2, :]
    dg_out[...] = dg.reshape(dg_out.shape)
    lax.fori_loop(0, n, done, 0)


def _write(where, acc, mine, got, de):
    vs, d = de.shape
    return pl.pallas_call(
        _write_kernel,
        out_shape=(jax.ShapeDtypeStruct((vs, d), F32), jax.ShapeDtypeStruct((d,), F32)),
        in_specs=[_sm()] + [_vm()] * 3 + [_any()],
        out_specs=(_any(), _vm()),
        scratch_shapes=[VMEM((C, d), F32), pltpu.SemaphoreType.DMA],
        input_output_aliases={4: 0},
        compiler_params=_params(6),
        cost_estimate=_cost(3),
        name="write_rows",
    )(where, acc, mine, got, de)


def solution(mesh):
    ntp = mesh.shape["tp"]
    ndp = mesh.shape["dp"]

    def swap(a, bit):
        return lax.ppermute(a, "tp", [(i, i ^ bit) for i in range(ntp)])

    def share(t):
        t2 = swap(t, 2)
        t1 = swap(t, 1)
        return t, t1, t2, swap(t2, 1)

    def p_terms(du, W, ts, vs):
        q, de = _p_terms(du, W, ts, vs)
        return de, (q[0], swap(q[1], 1), swap(q[2], 2), swap(q[3], 3))

    def body(ids, E, g, W, du, dres):
        vs, d = E.shape
        nk, t = ids.shape
        ts = t // ntp
        m = nk * ts
        g2 = g.reshape(1, d)

        tab, pos, _, _, cnts, slots, where = _index_call(None, ids, E, ntp)
        tabs = share(tab)
        de, ps = p_terms(du, W, ts, vs)
        de = _zeros(de, AT_A, ZA)
        x, xl = _expand(pos, tabs, ts)
        u, n, de = _u(x, g2, W, nk, de)
        dW, de = _dw(n, du, de, AT_W, ZW)
        dx, dg = _dx(xl.reshape(m, d), ps, dres.reshape(m, d), g2)
        dx1, dg1 = swap(dx, 1), swap(dg, 1)
        de = _zeros(de, AT_B, ZB)
        mine = _sums(slots, dx, dx1, dg, dg1)
        got = swap(mine, 2)
        other = lax.ppermute(cnts, "dp", [(i, (i + 1) % ndp) for i in range(ndp)])
        de, acc, flags = _acc(cnts, other, slots, dx, dx1, de, AT_R)
        dE, dg = _write(where, acc, mine, got, de)
        outs = u, xl, dE, dW, dg

        inputs = ids, E, W, du, dres, g2, flags

        def again(c):
            ids, E, W, du, dres, g2, fl, left = lax.optimization_barrier((*inputs, c[0]))
            rounds = fl[0, 0]
            i0 = left - left

            def more(q):
                i, x, _ = q
                tab, pos, *_ = _index_call(i, ids, E, ntp)
                return i + 1, *_expand(pos, share(tab), ts, x)

            zeros = jnp.zeros((nk * t, d), BF16), jnp.zeros((nk, ts, d), BF16)
            _, x, xl = lax.while_loop(lambda q: q[0] < rounds, more, (i0, *zeros))
            _, _, srow, rows, cs, _, _ = _index_call(i0, ids, E, ntp)
            de, ps = p_terms(du, W, ts, vs)
            u, n, de = _u(x, g2, W, nk, _zeros(de, AT_A, ZA))
            dW, de = _dw(n, du, de, AT_W, ZW)
            dx, dg = _dx(xl.reshape(m, d), ps, dres.reshape(m, d), g2)
            dg2 = dg + swap(dg, 1)
            dg = (dg2 + swap(dg2, 2)).reshape(d)
            dE = _scatter(cs, rows, srow, share(dx), _zeros(de, AT_B, vs // ZR - AT_B), ts, nk)
            return i0, (u, xl, dE, dW, dg)

        _, outs = lax.while_loop(lambda c: c[0] > 0, again, (jnp.minimum(flags[0, 2], 1), outs))
        return outs

    return jax.shard_map(
        body,
        mesh=mesh,
        in_specs=(P("dp", None), P("tp", None), P(None), P(None, "tp"), P("dp", None, "tp"), P("dp", "tp", None)),
        out_specs=(P("dp", None, "tp"), P("dp", "tp", None), P(("dp", "tp"), None), P("dp", "tp"), P("dp")),
        check_vma=False,
    )
```

```python
import functools

import jax
import jax.numpy as jnp
from jax import lax
from jax.experimental import pallas as pl
from jax.experimental.pallas import tpu as pltpu
from jax.sharding import PartitionSpec as P


EPS = 1e-6
C = 64
G = 2
C2 = 32
CB = 256
ZR = 128
ZP, ZA, ZU, ZW, ZB = 8, 6, 14, 20, 3
AT_A, AT_U, AT_B, AT_R = ZP, ZP + ZA, ZP + ZA + ZU + ZW, ZP + ZA + ZU + ZW + ZB
TB = 64

F32 = jnp.float32
BF16 = jnp.bfloat16
VMEM = pltpu.VMEM


def _sm():
    return pl.BlockSpec(memory_space=pltpu.SMEM)


def _vm():
    return pl.BlockSpec(memory_space=pltpu.VMEM)


def _any():
    return pl.BlockSpec(memory_space=pl.ANY)


def _params(mb):
    return pltpu.CompilerParams(vmem_limit_bytes=mb << 20)


def _cost(us):
    return pl.CostEstimate(flops=int(us * 4_000_000_000), bytes_accessed=1_000_000, transcendentals=0)


def _iota(shape, dim):
    return lax.broadcasted_iota(jnp.int32, shape, dim).astype(F32)


def _me():
    return lax.axis_index("tp").astype(jnp.int32)


def _fill(z, o, sems, lo, first, n, wait):
    def step(i, carry):
        at = pl.multiple_of((lo + i) * ZR, ZR)
        c = pltpu.make_async_copy(z, o.at[pl.ds(at, ZR)], sems.at[i])
        c.wait() if wait else c.start()
        return carry

    lax.fori_loop(first, first + n, step, 0)


def _zscratch(d, n):
    return [VMEM((ZR, d), F32), pltpu.SemaphoreType.DMA((n,))]


def _column(row, b):
    w = (b * TB) // 128 * 128
    part = jnp.broadcast_to(row[:, w:w + 128], (TB, 128))
    hit = _iota((TB, 128), 1) == _iota((TB, 128), 0) + float(b * TB - w)
    return jnp.sum(jnp.where(hit, part, 0.0), axis=1, keepdims=True)


def _fold(a):
    return sum(a[8 * q:8 * q + 8] for q in range(1, TB // 8)) + a[:8]


def _ids_row(ids_ref):
    idsf = ids_ref[...].astype(F32)
    return jnp.concatenate([idsf[k:k + 1] for k in range(ids_ref.shape[0])], axis=1)


def _ranks(idr, idcs, vs, ntp, masks):
    ntok = idr.shape[1]
    lane = _iota((TB, ntok), 1)
    thr = _iota((TB, 128), 1) * float(vs)
    rank8 = jnp.zeros((8, ntok), F32)
    below8 = [jnp.zeros((8, 128), F32) for _ in masks]
    for b, idc in enumerate(idcs):
        i = [i for i, (_, blocks) in enumerate(masks) if blocks[b]][0]
        mask = masks[i][0]
        dup = (jnp.broadcast_to(idc, (TB, ntok)) == idr) & (lane < _iota((TB, ntok), 0) + float(b * TB))
        seen = jnp.max(jnp.where(dup, mask, 0.0), axis=1, keepdims=True)
        key = jnp.where(seen > 0.5, float(vs * ntp), idc)
        rank8 = rank8 + _fold(jnp.where(jnp.broadcast_to(key, (TB, ntok)) < idr, mask, 0.0))
        below8[i] = below8[i] + _fold(jnp.where(jnp.broadcast_to(key, (TB, 128)) < thr, 1.0, 0.0))
    return jnp.sum(rank8, axis=0, keepdims=True), [jnp.sum(b8, axis=0, keepdims=True) for b8 in below8]


def _table_slots(idr, idcs, vs, ntp):
    rank, (below,) = _ranks(idr, idcs, vs, ntp, [(jnp.ones_like(idr), [True] * len(idcs))])
    own_r = jnp.floor(idr * (1.0 / vs))
    start = jnp.zeros_like(rank)
    for d in range(ntp):
        start = jnp.where(own_r == float(d), below[:, d:d + 1], start)
    return own_r, rank - start, below


def _index_kernel(vs, ntp, first, *refs):
    if first:
        ids_ref, e_ref, tab_ref, buf, glv, gls, gsem, sem = refs
        base = 0.0
    else:
        c_ref, ids_ref, e_ref, tab_ref, buf, glv, gls, gsem, sem = refs
        base = (c_ref[0] * C).astype(F32)
    me = _me().astype(F32)
    lo = me * vs
    idr = _ids_row(ids_ref)
    ntok = idr.shape[1]
    idcs = [_column(idr, b) for b in range(ntok // TB)]
    own_r, slot_r, _ = _table_slots(idr, idcs, vs, ntp)
    my_r = jnp.where(own_r == me, slot_r, -1.0)
    slot_l = _iota((TB, 128), 1) + base
    acc = jnp.zeros((TB, 128), F32)
    for b, idc in enumerate(idcs):
        acc = jnp.maximum(acc, jnp.where(_column(my_r, b) == slot_l, idc - lo, 0.0))
    glv[...] = jnp.broadcast_to(jnp.max(acc, axis=0, keepdims=True), (8, 128)).astype(jnp.int32)
    cp = pltpu.make_async_copy(glv, gls, gsem)
    cp.start()
    cp.wait()

    def fetch(j, carry):
        g = pl.multiple_of((gls[0, j] >> 1) << 1, G)
        at = pl.multiple_of(j * G, G)
        pltpu.make_async_copy(e_ref.at[pl.ds(g, G)], buf.at[pl.ds(at, G)], sem).start()
        return carry

    lax.fori_loop(0, C, fetch, 0, unroll=8)
    hit = jnp.where(my_r == _iota((C, ntok), 0) + base, idr - lo, 0.0)
    want = jnp.max(hit, axis=1, keepdims=True)
    want = want - jnp.floor(want * (1.0 / G)) * G + _iota((C, 1), 0) * G
    sel = jnp.where(_iota((C, C * G), 1) == want, 1.0, 0.0).astype(BF16)
    pltpu.make_async_copy(e_ref.at[pl.ds(0, C * G)], buf, sem).wait()
    tab_ref[...] = jnp.dot(sel, buf[...], preferred_element_type=F32).astype(BF16)


def _index_call(chunk, ids, E, ntp):
    vs, d = E.shape
    first = chunk is None
    return pl.pallas_call(
        functools.partial(_index_kernel, vs, ntp, first),
        out_shape=jax.ShapeDtypeStruct((C, d), BF16),
        in_specs=([] if first else [_sm()]) + [_vm(), pl.BlockSpec(memory_space=pltpu.HBM)],
        out_specs=_vm(),
        scratch_shapes=[
            VMEM((C * G, d), BF16),
            VMEM((8, 128), jnp.int32),
            pltpu.SMEM((8, 128), jnp.int32),
            pltpu.SemaphoreType.DMA,
            pltpu.SemaphoreType.DMA,
        ],
        compiler_params=_params(8),
        cost_estimate=_cost(12),
        name="index_gather",
    )(*([] if first else [chunk.reshape(1)]), ids, E)


def _slots_kernel(vs, ntp, c_ref, ids_ref, de_in, pos_ref, srow_ref, list_ref, cnt_ref, slot_ref, map_ref, de, z, sems):
    z[...] = jnp.zeros_like(z)
    _fill(z, de, sems, AT_A, 0, ZA, False)
    base = (c_ref[0] * C).astype(F32)
    mei = _me()
    me = mei.astype(F32)
    lo = me * vs
    nk, t = ids_ref.shape
    ntok = nk * t
    nb = ntok // TB
    ts = t // ntp
    idr = _ids_row(ids_ref)
    idcs = [_column(idr, b) for b in range(nb)]
    own_r, slot_r, below = _table_slots(idr, idcs, vs, ntp)
    my_r = jnp.where(own_r == me, slot_r, -1.0)
    cnt = jnp.zeros((1, 1), F32)
    mx = jnp.zeros((1, 1), F32)
    for d in range(ntp):
        nd = below[:, d + 1:d + 2] - below[:, d:d + 1]
        cnt = jnp.where(me == float(d), nd, cnt)
        mx = jnp.maximum(mx, nd)
    srow_ref[...] = my_r
    rel = (own_r.astype(jnp.int32) ^ mei).astype(F32)
    pos = jnp.where((slot_r >= base) & (slot_r < base + C), rel * C + slot_r - base, -1.0)
    for b in range(nb):
        pos_ref[b * TB:(b + 1) * TB, :] = _column(pos, b)

    part = lax.broadcasted_iota(jnp.int32, (1, ntok), 1) // ts % ntp
    chips = [
        (jnp.where(part // 2 == c, 1.0, 0.0), [b * TB // ts % ntp // 2 == c for b in range(nb)])
        for c in range(ntp // 2)
    ]
    rank2, below2 = _ranks(idr, idcs, vs, ntp, chips)
    start2 = jnp.zeros_like(rank2)
    cnt2 = jnp.zeros((1, 1), F32)
    mx2 = jnp.zeros((1, 1), F32)
    for c, (chip, _) in enumerate(chips):
        for d in range(ntp):
            ld = below2[c][:, d:d + 1]
            nd = below2[c][:, d + 1:d + 2] - ld
            start2 = jnp.where((own_r == float(d)) & (chip > 0.5), ld, start2)
            if d // 2 != c:
                cnt2 = jnp.where(me == float(d), nd, cnt2)
                mx2 = jnp.maximum(mx2, nd)
    slot2_r = rank2 - start2
    lane1 = lax.broadcasted_iota(jnp.int32, (1, 128), 1)
    over = jnp.where((mx > C) | (mx2 > C2 - 1), 1.0, 0.0)
    rounds = jnp.floor((mx + C - 1.0) * (1.0 / C))
    cnts = jnp.where(lane1 == 0, rounds, jnp.where(lane1 == 1, cnt, jnp.where(lane1 == 2, over, cnt2)))
    cnt_ref[...] = cnts.astype(jnp.int32)
    facing = (mei ^ 2).astype(F32)
    sums_r = jnp.where(own_r == facing, slot2_r, -1.0)
    rows = [jnp.zeros((1, nk * ts), F32)] * 4
    for q in range(ntp):
        at = [slice(k * t + q * ts, k * t + (q + 1) * ts) for k in range(nk)]
        mine = jnp.concatenate([my_r[:, w] for w in at], axis=1)
        sums = jnp.concatenate([sums_r[:, w] for w in at], axis=1)
        own, sib = me == float(q), me == float(q ^ 1)
        rows = [
            jnp.where(own, mine, rows[0]), jnp.where(sib, mine, rows[1]),
            jnp.where(own, sums, rows[2]), jnp.where(sib, sums, rows[3]),
        ]
    for j, r in enumerate(rows):
        slot_ref[j:j + 1, :] = r
    far = (part // 2).astype(F32) != jnp.floor(me * 0.5)
    got_r = jnp.where(far & (own_r == me), slot2_r, -1.0)
    acc2 = jnp.zeros((TB, 128), F32)
    slot_j = _iota((TB, 128), 1)
    full = jnp.zeros((8, ntok), F32)
    lane8 = _iota((8, ntok), 1)
    for b in range(nb):
        my_c = _column(my_r, b)
        acc2 = jnp.maximum(acc2, jnp.where(_column(got_r, b) == slot_j, my_c, 0.0))
        for q in range(TB // 8):
            s = slice(8 * q, 8 * q + 8)
            full = jnp.maximum(full, jnp.where(my_c[s] == lane8, idcs[b][s] - lo, 0.0))
    full = jnp.max(full, axis=0, keepdims=True)
    list_ref[...] = full.astype(jnp.int32)
    slots = jnp.minimum(jnp.max(acc2, axis=0, keepdims=True), C - 1.0)
    many = jnp.where(lane1 == 127, cnt2, slots)
    mine = jnp.where(lane1 == 127, cnt, full[:, :128])
    map_ref[...] = jnp.concatenate([many, mine], axis=1).astype(jnp.int32)
    _fill(z, de, sems, AT_A, 0, ZA, True)


def _slots(chunk, ids, ntp, de):
    vs, d = de.shape
    ntok = ids.shape[0] * ids.shape[1]
    return pl.pallas_call(
        functools.partial(_slots_kernel, vs, ntp),
        out_shape=(
            jax.ShapeDtypeStruct((ntok, 1), F32),
            jax.ShapeDtypeStruct((1, ntok), F32),
            jax.ShapeDtypeStruct((1, ntok), jnp.int32),
            jax.ShapeDtypeStruct((1, 128), jnp.int32),
            jax.ShapeDtypeStruct((4, ntok // ntp), F32),
            jax.ShapeDtypeStruct((1, 256), jnp.int32),
            jax.ShapeDtypeStruct(de.shape, F32),
        ),
        in_specs=[_sm(), _vm(), _any()],
        out_specs=(_vm(),) * 6 + (_any(),),
        scratch_shapes=_zscratch(d, ZA),
        input_output_aliases={2: 6},
        compiler_params=_params(6),
        cost_estimate=_cost(3),
        name="slots",
    )(chunk.reshape(1), ids, de)


def _expand_kernel(ts, acc, *refs):
    if acc:
        x_in, pos, t0, t1, t2, t3, x_out, xl_out = refs
    else:
        pos, t0, t1, t2, t3, x_out, xl_out = refs
    oh = jnp.where(pos[...] == _iota((pos.shape[0], 4 * C), 1), 1.0, 0.0).astype(BF16)
    for c in range(x_out.shape[1] // CB):
        s = slice(c * CB, (c + 1) * CB)
        tab = jnp.concatenate([t[:, s] for t in (t0, t1, t2, t3)], axis=0)
        tot = jnp.dot(oh, tab, preferred_element_type=F32)
        if acc:
            tot = tot + x_in[:, s].astype(F32)
        x_out[:, s] = tot.astype(BF16)
    t = 4 * ts
    for k in range(x_out.shape[0] // t):
        at = pl.multiple_of(k * t + _me() * ts, ts)
        xl_out[k] = x_out[pl.ds(at, ts), :]


def _expand(pos, tabs, ts, x=None):
    ntok, d = pos.shape[0], tabs[0].shape[1]
    ins = ([x] if x is not None else []) + [pos, *tabs]
    return pl.pallas_call(
        functools.partial(_expand_kernel, ts, x is not None),
        out_shape=(jax.ShapeDtypeStruct((ntok, d), BF16), jax.ShapeDtypeStruct((ntok // (4 * ts), ts, d), BF16)),
        in_specs=[_vm()] * len(ins),
        out_specs=(_vm(), _vm()),
        compiler_params=_params(12),
        cost_estimate=_cost(3),
        name="expand",
    )(*ins)


def _p_kernel(ts, du_ref, w_ref, *refs):
    outs, (de, dur, z, sems) = refs[:-4], refs[-4:]
    nk = du_ref.shape[0]

    @pl.when(pl.program_id(0) == 0)
    def _():
        z[...] = jnp.zeros_like(z)
        for k in range(nk):
            for r in range(4):
                at = pl.multiple_of((_me() ^ r) * ts, ts)
                dur[pl.ds((r * nk + k) * ts, ts), :] = du_ref[k, pl.ds(at, ts), :]
        _fill(z, de, sems, 0, 0, ZP, False)

    out = lax.dot_general(dur[...], w_ref[...], (((1,), (1,)), ((), ())), preferred_element_type=F32)
    for i, o in enumerate(outs):
        o[...] = out[i * nk * ts:(i + 1) * nk * ts].astype(BF16)

    @pl.when(pl.program_id(0) == pl.num_programs(0) - 1)
    def _():
        _fill(z, de, sems, 0, 0, ZP, True)


def _p_terms(du, W, ts, vs):
    nk, t, f = du.shape
    d = W.shape[0]
    cb = 3 * CB
    out = pl.pallas_call(
        functools.partial(_p_kernel, ts),
        out_shape=(jax.ShapeDtypeStruct((nk * ts, d), BF16),) * 4 + (jax.ShapeDtypeStruct((vs, d), F32),),
        grid=(d // cb,),
        in_specs=[pl.BlockSpec((nk, t, f), lambda i: (0, 0, 0)), pl.BlockSpec((cb, f), lambda i: (i, 0))],
        out_specs=(pl.BlockSpec((nk * ts, cb), lambda i: (0, i)),) * 4 + (_any(),),
        scratch_shapes=[VMEM((nk * t, f), BF16)] + _zscratch(d, ZP),
        compiler_params=_params(20),
        cost_estimate=_cost(5),
        name="p_terms",
    )(du, W)
    return out[:4], out[4]


def _zero_kernel(lo, n, de_in, o, z, sems):
    z[...] = jnp.zeros_like(z)
    _fill(z, o, sems, lo, 0, n, False)
    _fill(z, o, sems, lo, 0, n, True)


def _zeros(de, lo, n):
    vs, d = de.shape
    return pl.pallas_call(
        functools.partial(_zero_kernel, lo, n),
        out_shape=jax.ShapeDtypeStruct((vs, d), F32),
        in_specs=[_any()],
        out_specs=_any(),
        scratch_shapes=_zscratch(d, n),
        input_output_aliases={0: 0},
        compiler_params=_params(4),
        cost_estimate=_cost(n * 0.375),
    )(de)


def _dx_kernel(x, p0, p1, p2, p3, dres, g, dx, dg):
    rows = 32
    tot = None
    for b in range(dx.shape[0] // rows):
        s = slice(b * rows, (b + 1) * rows)
        xf = x[s].astype(F32)
        rs = lax.rsqrt(jnp.mean(xf * xf, axis=-1, keepdims=True) + EPS)
        nh = xf * rs
        dn = (p0[s].astype(F32) + p1[s].astype(F32)) + (p2[s].astype(F32) + p3[s].astype(F32))
        gdn = g[...].astype(F32) * dn
        out = dres[s].astype(F32) + rs * (gdn - nh * jnp.mean(nh * gdn, axis=-1, keepdims=True))
        dx[s] = out.astype(BF16)
        part = jnp.sum(dn * nh, axis=0, keepdims=True)
        tot = part if tot is None else tot + part
    dg[...] = tot


def _dx(x, ps, dres, g):
    m, d = x.shape
    return pl.pallas_call(
        _dx_kernel,
        out_shape=(
            jax.ShapeDtypeStruct((m, d), BF16),
            jax.ShapeDtypeStruct((1, d), F32),
        ),
        in_specs=[_vm()] * 7,
        out_specs=(_vm(), _vm()),
        compiler_params=_params(12),
        cost_estimate=_cost(2),
        name="dx_form",
    )(x, *ps, dres, g)


def _sums_kernel(slot_ref, dx0, dx1, dg0, dg1, out):
    m = dx0.shape[0]
    j = _iota((C2, m), 0)
    ohs = [jnp.where(slot_ref[i:i + 1, :] == j, 1.0, 0.0).astype(BF16) for i in (2, 3)]
    last = lax.broadcasted_iota(jnp.int32, (C2, CB), 0) == C2 - 1
    for c in range(out.shape[1] // CB):
        s = slice(c * CB, (c + 1) * CB)
        tot = jnp.dot(ohs[0], dx0[:, s], preferred_element_type=F32)
        tot = tot + jnp.dot(ohs[1], dx1[:, s], preferred_element_type=F32)
        out[:, s] = jnp.where(last, dg0[:, s] + dg1[:, s], tot)


def _sums(slots, dx0, dx1, dg0, dg1):
    return pl.pallas_call(
        _sums_kernel,
        out_shape=jax.ShapeDtypeStruct((C2, dx0.shape[1]), F32),
        in_specs=[_vm()] * 5,
        out_specs=_vm(),
        compiler_params=_params(6),
        cost_estimate=_cost(1),
        name="dx_sums",
    )(slots, dx0, dx1, dg0, dg1)


def _udw_kernel(per, x_ref, g_ref, w_ref, du_ref, de_in, u_ref, dw_ref, de, n, z, sems):
    i = pl.program_id(0)
    nk, t, f = du_ref.shape
    cb = dw_ref.shape[0]

    @pl.when(i == 0)
    def _():
        z[...] = jnp.zeros_like(z)
        _fill(z, de, sems, AT_U, 0, ZU, False)
        rows = 64
        for b in range(n.shape[0] // rows):
            s = slice(b * rows, (b + 1) * rows)
            xf = x_ref[s].astype(F32)
            rs = lax.rsqrt(jnp.mean(xf * xf, axis=-1, keepdims=True) + EPS)
            n[s] = (xf * rs * g_ref[...].astype(F32)).astype(BF16)
        for c in range(f // CB):
            s = slice(c * CB, (c + 1) * CB)
            out = jnp.dot(n[...], w_ref[:, s], preferred_element_type=F32).astype(BF16)
            for k in range(nk):
                u_ref[k, :, s] = out[k * t:(k + 1) * t]

    _fill(z, de, sems, AT_U, ZU + i * per, jnp.minimum(per, ZW - i * per), False)
    blk = n[:, pl.ds(pl.multiple_of(i * cb, 128), cb)]
    dw_ref[...] = lax.dot_general(
        blk, du_ref[...].reshape(nk * t, f), (((0,), (0,)), ((), ())), preferred_element_type=F32
    )

    @pl.when(i == pl.num_programs(0) - 1)
    def _():
        _fill(z, de, sems, AT_U, 0, ZU + ZW, True)


def _udw(x, g, W, du, de):
    nk, t, f = du.shape
    ntok, d = x.shape
    cb = d // 6
    steps = d // cb
    return pl.pallas_call(
        functools.partial(_udw_kernel, -(-ZW // steps)),
        out_shape=(
            jax.ShapeDtypeStruct((nk, t, f), BF16),
            jax.ShapeDtypeStruct((d, f), F32),
            jax.ShapeDtypeStruct(de.shape, F32),
        ),
        grid=(steps,),
        in_specs=[_vm(), _vm(), _vm(), _vm(), _any()],
        out_specs=(pl.BlockSpec((nk, t, f), lambda i: (0, 0, 0)), pl.BlockSpec((cb, f), lambda i: (i, 0)), _any()),
        scratch_shapes=[VMEM((ntok, d), BF16)] + _zscratch(d, ZU + ZW),
        input_output_aliases={4: 2},
        compiler_params=_params(20),
        cost_estimate=_cost(20),
        name="u_dw",
    )(x, g, W, du, de)


def _scatter_kernel(ts, nk, cnt_ref, list_ref, srow_ref, *refs):
    pieces, (de_in, de, dx, acc, sem) = refs[:-5], refs[-5:]
    ntok = nk * 4 * ts
    for k in range(nk):
        for r in range(4):
            at = pl.multiple_of(k * 4 * ts + (_me() ^ r) * ts, ts)
            dx[pl.ds(at, ts), :] = pieces[r][k * ts:(k + 1) * ts, :]
    cnt = cnt_ref[0, 1]

    def chunk(i, carry):
        base = i * C
        slot = (lax.broadcasted_iota(jnp.int32, (C, ntok), 0) + base).astype(F32)
        oh = jnp.where(slot == srow_ref[...], 1.0, 0.0).astype(BF16)
        for c in range(acc.shape[1] // CB):
            s = slice(c * CB, (c + 1) * CB)
            acc[:, s] = jnp.dot(oh, dx[:, s], preferred_element_type=F32)
        here = jnp.minimum(cnt - base, C)

        def put(j, c2):
            row = list_ref[0, base + j]
            pltpu.make_async_copy(acc.at[pl.ds(j, 1)], de.at[pl.ds(row, 1)], sem).start()
            return c2

        def done(j, c2):
            pltpu.make_async_copy(acc.at[pl.ds(j, 1)], de.at[pl.ds(0, 1)], sem).wait()
            return c2

        lax.fori_loop(0, here, put, 0)
        lax.fori_loop(0, here, done, 0)
        return carry

    lax.fori_loop(0, (cnt + C - 1) // C, chunk, 0)


def _scatter(cnts, rows, srow, pieces, de, ts, nk):
    vs, d = de.shape
    ntok = srow.shape[1]
    return pl.pallas_call(
        functools.partial(_scatter_kernel, ts, nk),
        out_shape=jax.ShapeDtypeStruct((vs, d), F32),
        in_specs=[_sm(), _sm(), _vm()] + [_vm()] * len(pieces) + [_any()],
        out_specs=_any(),
        scratch_shapes=[VMEM((ntok, d), BF16), VMEM((C, d), F32), pltpu.SemaphoreType.DMA],
        input_output_aliases={3 + len(pieces): 0},
        compiler_params=_params(16),
        cost_estimate=_cost(3),
        name="scatter_rows",
    )(cnts, rows, srow, *pieces, de)


def _acc_kernel(lo, n, cnt_ref, oth_ref, slot_ref, dx0, dx1, de_in, de, acc, flag, z, sems):
    z[...] = jnp.zeros_like(z)
    _fill(z, de, sems, lo, 0, n, False)
    for i in (0, 2):
        flag[0, i] = jnp.maximum(cnt_ref[0, i], oth_ref[0, i])
    m = dx0.shape[0]
    j = _iota((C, m), 0)
    ohs = [jnp.where(slot_ref[i:i + 1, :] == j, 1.0, 0.0).astype(BF16) for i in (0, 1)]
    for c in range(acc.shape[1] // CB):
        s = slice(c * CB, (c + 1) * CB)
        tot = jnp.dot(ohs[0], dx0[:, s], preferred_element_type=F32)
        acc[:, s] = tot + jnp.dot(ohs[1], dx1[:, s], preferred_element_type=F32)
    _fill(z, de, sems, lo, 0, n, True)


def _acc(cnts, other, slots, dx0, dx1, de, lo):
    vs, d = de.shape
    n = vs // ZR - lo
    return pl.pallas_call(
        functools.partial(_acc_kernel, lo, n),
        out_shape=(
            jax.ShapeDtypeStruct((vs, d), F32),
            jax.ShapeDtypeStruct((C, d), F32),
            jax.ShapeDtypeStruct((1, 4), jnp.int32),
        ),
        in_specs=[_sm(), _sm()] + [_vm()] * 3 + [_any()],
        out_specs=(_any(), _vm(), _sm()),
        scratch_shapes=_zscratch(d, n),
        input_output_aliases={5: 0},
        compiler_params=_params(8),
        cost_estimate=_cost(n * 0.375),
        name="fill_acc",
    )(cnts, other, slots, dx0, dx1, de)


def _write_kernel(map_ref, acc_in, mine_ref, got_ref, de_in, de, dg_out, acc, sem):
    acc[...] = acc_in[...]

    def add(j, carry):
        at = pl.ds(map_ref[0, j], 1)
        acc[at, :] = acc[at, :] + got_ref[pl.ds(j, 1), :]
        return carry

    lax.fori_loop(0, jnp.minimum(map_ref[0, 127], C2 - 1), add, 0)
    n = jnp.minimum(map_ref[0, 255], C)

    def put(j, carry):
        pltpu.make_async_copy(acc.at[pl.ds(j, 1)], de.at[pl.ds(map_ref[0, 128 + j], 1)], sem).start()
        return carry

    def done(j, carry):
        pltpu.make_async_copy(acc.at[pl.ds(j, 1)], de.at[pl.ds(0, 1)], sem).wait()
        return carry

    lax.fori_loop(0, n, put, 0)
    dg = mine_ref[C2 - 1:C2, :] + got_ref[C2 - 1:C2, :]
    dg_out[...] = dg.reshape(dg_out.shape)
    lax.fori_loop(0, n, done, 0)


def _write(where, acc, mine, got, de):
    vs, d = de.shape
    return pl.pallas_call(
        _write_kernel,
        out_shape=(jax.ShapeDtypeStruct((vs, d), F32), jax.ShapeDtypeStruct((d,), F32)),
        in_specs=[_sm()] + [_vm()] * 3 + [_any()],
        out_specs=(_any(), _vm()),
        scratch_shapes=[VMEM((C, d), F32), pltpu.SemaphoreType.DMA],
        input_output_aliases={4: 0},
        compiler_params=_params(6),
        cost_estimate=_cost(3),
        name="write_rows",
    )(where, acc, mine, got, de)


def solution(mesh):
    ntp = mesh.shape["tp"]
    ndp = mesh.shape["dp"]

    def swap(a, bit):
        return lax.ppermute(a, "tp", [(i, i ^ bit) for i in range(ntp)])

    def share(t):
        t2 = swap(t, 2)
        t1 = swap(t, 1)
        return t, t1, t2, swap(t2, 1)

    def p_terms(du, W, ts, vs):
        q, de = _p_terms(du, W, ts, vs)
        return de, (q[0], swap(q[1], 1), swap(q[2], 2), swap(q[3], 3))

    def body(ids, E, g, W, du, dres):
        vs, d = E.shape
        nk, t = ids.shape
        ts = t // ntp
        m = nk * ts
        g2 = g.reshape(1, d)

        tabs = share(_index_call(None, ids, E, ntp))
        de, ps = p_terms(du, W, ts, vs)
        pos, _, _, cnts, slots, where, de = _slots(jnp.int32(0), ids, ntp, de)
        x, xl = _expand(pos, tabs, ts)
        u, dW, de = _udw(x, g2, W, du, de)
        dx, dg = _dx(xl.reshape(m, d), ps, dres.reshape(m, d), g2)
        dx1, dg1 = swap(dx, 1), swap(dg, 1)
        de = _zeros(de, AT_B, ZB)
        mine = _sums(slots, dx, dx1, dg, dg1)
        got = swap(mine, 2)
        other = lax.ppermute(cnts, "dp", [(i, (i + 1) % ndp) for i in range(ndp)])
        de, acc, flags = _acc(cnts, other, slots, dx, dx1, de, AT_R)
        dE, dg = _write(where, acc, mine, got, de)
        outs = u, xl, dE, dW, dg

        inputs = ids, E, W, du, dres, g2, flags

        def again(c):
            ids, E, W, du, dres, g2, fl, left = lax.optimization_barrier((*inputs, c[0]))
            rounds = fl[0, 0]
            i0 = left - left

            def more(q):
                i, x, _, de = q
                pos, *_, de = _slots(i, ids, ntp, de)
                return i + 1, *_expand(pos, share(_index_call(i, ids, E, ntp)), ts, x), de

            zeros = jnp.zeros((nk * t, d), BF16), jnp.zeros((nk, ts, d), BF16)
            de, ps = p_terms(du, W, ts, vs)
            _, x, xl, de = lax.while_loop(lambda q: q[0] < rounds, more, (i0, *zeros, de))
            _, srow, rows, cs, _, _, de = _slots(i0, ids, ntp, de)
            u, dW, de = _udw(x, g2, W, du, de)
            dx, dg = _dx(xl.reshape(m, d), ps, dres.reshape(m, d), g2)
            dg2 = dg + swap(dg, 1)
            dg = (dg2 + swap(dg2, 2)).reshape(d)
            dE = _scatter(cs, rows, srow, share(dx), _zeros(de, AT_B, vs // ZR - AT_B), ts, nk)
            return i0, (u, xl, dE, dW, dg)

        _, outs = lax.while_loop(lambda c: c[0] > 0, again, (jnp.minimum(flags[0, 2], 1), outs))
        return outs

    return jax.shard_map(
        body,
        mesh=mesh,
        in_specs=(P("dp", None), P("tp", None), P(None), P(None, "tp"), P("dp", None, "tp"), P("dp", "tp", None)),
        out_specs=(P("dp", None, "tp"), P("dp", "tp", None), P(("dp", "tp"), None), P("dp", "tp"), P("dp")),
        check_vma=False,
    )
```

```python
import functools

import jax
import jax.numpy as jnp
from jax import lax
from jax.experimental import pallas as pl
from jax.experimental.pallas import tpu as pltpu
from jax.sharding import PartitionSpec as P


EPS = 1e-6
C = 56
G = 2
C2 = 32
CB = 256
ZR = 128
ZP, ZA, ZU, ZW = 8, 6, 15, 22
AT_A, AT_U, AT_R = ZP, ZP + ZA, ZP + ZA + ZU + ZW
TB = 64

F32 = jnp.float32
BF16 = jnp.bfloat16
VMEM = pltpu.VMEM


def _sm():
    return pl.BlockSpec(memory_space=pltpu.SMEM)


def _vm():
    return pl.BlockSpec(memory_space=pltpu.VMEM)


def _any():
    return pl.BlockSpec(memory_space=pl.ANY)


def _params(mb):
    return pltpu.CompilerParams(vmem_limit_bytes=mb << 20)


def _cost(us):
    return pl.CostEstimate(flops=int(us * 4_000_000_000), bytes_accessed=1_000_000, transcendentals=0)


def _iota(shape, dim):
    return lax.broadcasted_iota(jnp.int32, shape, dim).astype(F32)


def _me():
    return lax.axis_index("tp").astype(jnp.int32)


def _fill(z, o, sems, lo, first, n, wait):
    def step(i, carry):
        at = pl.multiple_of((lo + i) * ZR, ZR)
        c = pltpu.make_async_copy(z, o.at[pl.ds(at, ZR)], sems.at[i])
        c.wait() if wait else c.start()
        return carry

    lax.fori_loop(first, first + n, step, 0)


def _zscratch(d, n):
    return [VMEM((ZR, d), F32), pltpu.SemaphoreType.DMA((n,))]


def _column(row, b):
    w = (b * TB) // 128 * 128
    part = jnp.broadcast_to(row[:, w:w + 128], (TB, 128))
    hit = _iota((TB, 128), 1) == _iota((TB, 128), 0) + float(b * TB - w)
    return jnp.sum(jnp.where(hit, part, 0.0), axis=1, keepdims=True)


def _fold(a):
    return sum(a[8 * q:8 * q + 8] for q in range(1, TB // 8)) + a[:8]


def _ids_row(ids_ref):
    idsf = ids_ref[...].astype(F32)
    return jnp.concatenate([idsf[k:k + 1] for k in range(ids_ref.shape[0])], axis=1)


def _ranks(idr, idcs, vs, ntp, masks):
    ntok = idr.shape[1]
    lane = _iota((TB, ntok), 1)
    thr = _iota((TB, 128), 1) * float(vs)
    rank8 = jnp.zeros((8, ntok), F32)
    below8 = [jnp.zeros((8, 128), F32) for _ in masks]
    for b, idc in enumerate(idcs):
        i = [i for i, (_, blocks) in enumerate(masks) if blocks[b]][0]
        mask = masks[i][0]
        dup = (jnp.broadcast_to(idc, (TB, ntok)) == idr) & (lane < _iota((TB, ntok), 0) + float(b * TB))
        seen = jnp.max(jnp.where(dup, mask, 0.0), axis=1, keepdims=True)
        key = jnp.where(seen > 0.5, float(vs * ntp), idc)
        rank8 = rank8 + _fold(jnp.where(jnp.broadcast_to(key, (TB, ntok)) < idr, mask, 0.0))
        below8[i] = below8[i] + _fold(jnp.where(jnp.broadcast_to(key, (TB, 128)) < thr, 1.0, 0.0))
    return jnp.sum(rank8, axis=0, keepdims=True), [jnp.sum(b8, axis=0, keepdims=True) for b8 in below8]


def _table_slots(idr, idcs, vs, ntp):
    rank, (below,) = _ranks(idr, idcs, vs, ntp, [(jnp.ones_like(idr), [True] * len(idcs))])
    own_r = jnp.floor(idr * (1.0 / vs))
    start = jnp.zeros_like(rank)
    for d in range(ntp):
        start = jnp.where(own_r == float(d), below[:, d:d + 1], start)
    return own_r, rank - start, below


def _index_kernel(vs, ntp, first, *refs):
    if first:
        ids_ref, e_ref, tab_ref, buf, glv, gls, gsem, sem = refs
        base = 0.0
    else:
        c_ref, ids_ref, e_ref, tab_ref, buf, glv, gls, gsem, sem = refs
        base = (c_ref[0] * C).astype(F32)
    me = _me().astype(F32)
    lo = me * vs
    idr = _ids_row(ids_ref)
    ntok = idr.shape[1]
    idcs = [_column(idr, b) for b in range(ntok // TB)]
    own_r, slot_r, _ = _table_slots(idr, idcs, vs, ntp)
    my_r = jnp.where(own_r == me, slot_r, -1.0)
    slot_l = _iota((TB, 128), 1) + base
    acc = jnp.zeros((TB, 128), F32)
    for b, idc in enumerate(idcs):
        acc = jnp.maximum(acc, jnp.where(_column(my_r, b) == slot_l, idc - lo, 0.0))
    glv[...] = jnp.broadcast_to(jnp.max(acc, axis=0, keepdims=True), (8, 128)).astype(jnp.int32)
    cp = pltpu.make_async_copy(glv, gls, gsem)
    cp.start()
    cp.wait()

    def fetch(j, carry):
        g = pl.multiple_of((gls[0, j] >> 1) << 1, G)
        at = pl.multiple_of(j * G, G)
        pltpu.make_async_copy(e_ref.at[pl.ds(g, G)], buf.at[pl.ds(at, G)], sem).start()
        return carry

    lax.fori_loop(0, C, fetch, 0, unroll=8)
    hit = jnp.where(my_r == _iota((C, ntok), 0) + base, idr - lo, 0.0)
    want = jnp.max(hit, axis=1, keepdims=True)
    want = want - jnp.floor(want * (1.0 / G)) * G + _iota((C, 1), 0) * G
    sel = jnp.where(_iota((C, C * G), 1) == want, 1.0, 0.0).astype(BF16)
    pltpu.make_async_copy(e_ref.at[pl.ds(0, C * G)], buf, sem).wait()
    tab_ref[...] = jnp.dot(sel, buf[...], preferred_element_type=F32).astype(BF16)


def _index_call(chunk, ids, E, ntp):
    vs, d = E.shape
    first = chunk is None
    return pl.pallas_call(
        functools.partial(_index_kernel, vs, ntp, first),
        out_shape=jax.ShapeDtypeStruct((C, d), BF16),
        in_specs=([] if first else [_sm()]) + [_vm(), pl.BlockSpec(memory_space=pltpu.HBM)],
        out_specs=_vm(),
        scratch_shapes=[
            VMEM((C * G, d), BF16),
            VMEM((8, 128), jnp.int32),
            pltpu.SMEM((8, 128), jnp.int32),
            pltpu.SemaphoreType.DMA,
            pltpu.SemaphoreType.DMA,
        ],
        compiler_params=_params(8),
        cost_estimate=_cost(12),
        name="index_gather",
    )(*([] if first else [chunk.reshape(1)]), ids, E)


def _slots_kernel(vs, ntp, c_ref, ids_ref, de_in, pos_ref, srow_ref, list_ref, cnt_ref, slot_ref, map_ref, de, z, sems):
    z[...] = jnp.zeros_like(z)
    _fill(z, de, sems, AT_A, 0, ZA, False)
    base = (c_ref[0] * C).astype(F32)
    mei = _me()
    me = mei.astype(F32)
    lo = me * vs
    nk, t = ids_ref.shape
    ntok = nk * t
    nb = ntok // TB
    ts = t // ntp
    idr = _ids_row(ids_ref)
    idcs = [_column(idr, b) for b in range(nb)]
    own_r, slot_r, below = _table_slots(idr, idcs, vs, ntp)
    my_r = jnp.where(own_r == me, slot_r, -1.0)
    cnt = jnp.zeros((1, 1), F32)
    mx = jnp.zeros((1, 1), F32)
    for d in range(ntp):
        nd = below[:, d + 1:d + 2] - below[:, d:d + 1]
        cnt = jnp.where(me == float(d), nd, cnt)
        mx = jnp.maximum(mx, nd)
    srow_ref[...] = my_r
    rel = (own_r.astype(jnp.int32) ^ mei).astype(F32)
    pos = jnp.where((slot_r >= base) & (slot_r < base + C), rel * C + slot_r - base, -1.0)
    for b in range(nb):
        pos_ref[b * TB:(b + 1) * TB, :] = _column(pos, b)

    part = lax.broadcasted_iota(jnp.int32, (1, ntok), 1) // ts % ntp
    chips = [
        (jnp.where(part // 2 == c, 1.0, 0.0), [b * TB // ts % ntp // 2 == c for b in range(nb)])
        for c in range(ntp // 2)
    ]
    rank2, below2 = _ranks(idr, idcs, vs, ntp, chips)
    start2 = jnp.zeros_like(rank2)
    cnt2 = jnp.zeros((1, 1), F32)
    mx2 = jnp.zeros((1, 1), F32)
    for c, (chip, _) in enumerate(chips):
        for d in range(ntp):
            ld = below2[c][:, d:d + 1]
            nd = below2[c][:, d + 1:d + 2] - ld
            start2 = jnp.where((own_r == float(d)) & (chip > 0.5), ld, start2)
            if d // 2 != c:
                cnt2 = jnp.where(me == float(d), nd, cnt2)
                mx2 = jnp.maximum(mx2, nd)
    slot2_r = rank2 - start2
    lane1 = lax.broadcasted_iota(jnp.int32, (1, 128), 1)
    over = jnp.where((mx > C) | (mx2 > C2 - 1), 1.0, 0.0)
    rounds = jnp.floor((mx + C - 1.0) * (1.0 / C))
    cnts = jnp.where(lane1 == 0, rounds, jnp.where(lane1 == 1, cnt, jnp.where(lane1 == 2, over, cnt2)))
    cnt_ref[...] = cnts.astype(jnp.int32)
    facing = (mei ^ 2).astype(F32)
    sums_r = jnp.where(own_r == facing, slot2_r, -1.0)
    rows = [jnp.zeros((1, nk * ts), F32)] * 4
    for q in range(ntp):
        at = [slice(k * t + q * ts, k * t + (q + 1) * ts) for k in range(nk)]
        mine = jnp.concatenate([my_r[:, w] for w in at], axis=1)
        sums = jnp.concatenate([sums_r[:, w] for w in at], axis=1)
        own, sib = me == float(q), me == float(q ^ 1)
        rows = [
            jnp.where(own, mine, rows[0]), jnp.where(sib, mine, rows[1]),
            jnp.where(own, sums, rows[2]), jnp.where(sib, sums, rows[3]),
        ]
    for j, r in enumerate(rows):
        slot_ref[j:j + 1, :] = r
    far = (part // 2).astype(F32) != jnp.floor(me * 0.5)
    got_r = jnp.where(far & (own_r == me), slot2_r, -1.0)
    acc2 = jnp.zeros((TB, 128), F32)
    slot_j = _iota((TB, 128), 1)
    full = jnp.zeros((8, ntok), F32)
    lane8 = _iota((8, ntok), 1)
    for b in range(nb):
        my_c = _column(my_r, b)
        acc2 = jnp.maximum(acc2, jnp.where(_column(got_r, b) == slot_j, my_c, 0.0))
        for q in range(TB // 8):
            s = slice(8 * q, 8 * q + 8)
            full = jnp.maximum(full, jnp.where(my_c[s] == lane8, idcs[b][s] - lo, 0.0))
    full = jnp.max(full, axis=0, keepdims=True)
    list_ref[...] = full.astype(jnp.int32)
    slots = jnp.minimum(jnp.max(acc2, axis=0, keepdims=True), C - 1.0)
    many = jnp.where(lane1 == 127, cnt2, slots)
    mine = jnp.where(lane1 == 127, cnt, full[:, :128])
    map_ref[...] = jnp.concatenate([many, mine], axis=1).astype(jnp.int32)
    _fill(z, de, sems, AT_A, 0, ZA, True)


def _slots(chunk, ids, ntp, de):
    vs, d = de.shape
    ntok = ids.shape[0] * ids.shape[1]
    return pl.pallas_call(
        functools.partial(_slots_kernel, vs, ntp),
        out_shape=(
            jax.ShapeDtypeStruct((ntok, 1), F32),
            jax.ShapeDtypeStruct((1, ntok), F32),
            jax.ShapeDtypeStruct((1, ntok), jnp.int32),
            jax.ShapeDtypeStruct((1, 128), jnp.int32),
            jax.ShapeDtypeStruct((4, ntok // ntp), F32),
            jax.ShapeDtypeStruct((1, 256), jnp.int32),
            jax.ShapeDtypeStruct(de.shape, F32),
        ),
        in_specs=[_sm(), _vm(), _any()],
        out_specs=(_vm(),) * 6 + (_any(),),
        scratch_shapes=_zscratch(d, ZA),
        input_output_aliases={2: 6},
        compiler_params=_params(6),
        cost_estimate=_cost(3),
        name="slots",
    )(chunk.reshape(1), ids, de)


def _expand_kernel(ts, acc, *refs):
    if acc:
        x_in, pos, t0, t1, t2, t3, x_out, xl_out = refs
    else:
        pos, t0, t1, t2, t3, x_out, xl_out = refs
    oh = jnp.where(pos[...] == _iota((pos.shape[0], 4 * C), 1), 1.0, 0.0).astype(BF16)
    for c in range(x_out.shape[1] // CB):
        s = slice(c * CB, (c + 1) * CB)
        tab = jnp.concatenate([t[:, s] for t in (t0, t1, t2, t3)], axis=0)
        tot = jnp.dot(oh, tab, preferred_element_type=F32)
        if acc:
            tot = tot + x_in[:, s].astype(F32)
        x_out[:, s] = tot.astype(BF16)
    t = 4 * ts
    for k in range(x_out.shape[0] // t):
        at = pl.multiple_of(k * t + _me() * ts, ts)
        xl_out[k] = x_out[pl.ds(at, ts), :]


def _expand(pos, tabs, ts, x=None):
    ntok, d = pos.shape[0], tabs[0].shape[1]
    ins = ([x] if x is not None else []) + [pos, *tabs]
    return pl.pallas_call(
        functools.partial(_expand_kernel, ts, x is not None),
        out_shape=(jax.ShapeDtypeStruct((ntok, d), BF16), jax.ShapeDtypeStruct((ntok // (4 * ts), ts, d), BF16)),
        in_specs=[_vm()] * len(ins),
        out_specs=(_vm(), _vm()),
        compiler_params=_params(12),
        cost_estimate=_cost(3),
        name="expand",
    )(*ins)


def _p_kernel(ts, du_ref, w_ref, *refs):
    outs, (de, dur, z, sems) = refs[:-4], refs[-4:]
    nk = du_ref.shape[0]

    @pl.when(pl.program_id(0) == 0)
    def _():
        z[...] = jnp.zeros_like(z)
        for k in range(nk):
            for r in range(4):
                at = pl.multiple_of((_me() ^ r) * ts, ts)
                dur[pl.ds((r * nk + k) * ts, ts), :] = du_ref[k, pl.ds(at, ts), :]
        _fill(z, de, sems, 0, 0, ZP, False)

    out = lax.dot_general(dur[...], w_ref[...], (((1,), (1,)), ((), ())), preferred_element_type=F32)
    for i, o in enumerate(outs):
        o[...] = out[i * nk * ts:(i + 1) * nk * ts].astype(BF16)

    @pl.when(pl.program_id(0) == pl.num_programs(0) - 1)
    def _():
        _fill(z, de, sems, 0, 0, ZP, True)


def _p_terms(du, W, ts, vs):
    nk, t, f = du.shape
    d = W.shape[0]
    cb = 3 * CB
    out = pl.pallas_call(
        functools.partial(_p_kernel, ts),
        out_shape=(jax.ShapeDtypeStruct((nk * ts, d), BF16),) * 4 + (jax.ShapeDtypeStruct((vs, d), F32),),
        grid=(d // cb,),
        in_specs=[pl.BlockSpec((nk, t, f), lambda i: (0, 0, 0)), pl.BlockSpec((cb, f), lambda i: (i, 0))],
        out_specs=(pl.BlockSpec((nk * ts, cb), lambda i: (0, i)),) * 4 + (_any(),),
        scratch_shapes=[VMEM((nk * t, f), BF16)] + _zscratch(d, ZP),
        compiler_params=_params(20),
        cost_estimate=_cost(5),
        name="p_terms",
    )(du, W)
    return out[:4], out[4]


def _zero_kernel(lo, n, de_in, o, z, sems):
    z[...] = jnp.zeros_like(z)
    _fill(z, o, sems, lo, 0, n, False)
    _fill(z, o, sems, lo, 0, n, True)


def _zeros(de, lo, n):
    vs, d = de.shape
    return pl.pallas_call(
        functools.partial(_zero_kernel, lo, n),
        out_shape=jax.ShapeDtypeStruct((vs, d), F32),
        in_specs=[_any()],
        out_specs=_any(),
        scratch_shapes=_zscratch(d, n),
        input_output_aliases={0: 0},
        compiler_params=_params(4),
        cost_estimate=_cost(n * 0.375),
    )(de)


def _dx_kernel(x, p0, p1, p2, p3, dres, g, dx, dg):
    rows = 32
    tot = None
    for b in range(dx.shape[0] // rows):
        s = slice(b * rows, (b + 1) * rows)
        xf = x[s].astype(F32)
        rs = lax.rsqrt(jnp.mean(xf * xf, axis=-1, keepdims=True) + EPS)
        nh = xf * rs
        dn = (p0[s].astype(F32) + p1[s].astype(F32)) + (p2[s].astype(F32) + p3[s].astype(F32))
        gdn = g[...].astype(F32) * dn
        out = dres[s].astype(F32) + rs * (gdn - nh * jnp.mean(nh * gdn, axis=-1, keepdims=True))
        dx[s] = out.astype(BF16)
        part = jnp.sum(dn * nh, axis=0, keepdims=True)
        tot = part if tot is None else tot + part
    dg[...] = tot


def _dx(x, ps, dres, g):
    m, d = x.shape
    return pl.pallas_call(
        _dx_kernel,
        out_shape=(
            jax.ShapeDtypeStruct((m, d), BF16),
            jax.ShapeDtypeStruct((1, d), F32),
        ),
        in_specs=[_vm()] * 7,
        out_specs=(_vm(), _vm()),
        compiler_params=_params(12),
        cost_estimate=_cost(2),
        name="dx_form",
    )(x, *ps, dres, g)


def _sums_kernel(slot_ref, dx0, dx1, dg0, dg1, out):
    m = dx0.shape[0]
    j = _iota((C2, m), 0)
    ohs = [jnp.where(slot_ref[i:i + 1, :] == j, 1.0, 0.0).astype(BF16) for i in (2, 3)]
    last = lax.broadcasted_iota(jnp.int32, (C2, CB), 0) == C2 - 1
    for c in range(out.shape[1] // CB):
        s = slice(c * CB, (c + 1) * CB)
        tot = jnp.dot(ohs[0], dx0[:, s], preferred_element_type=F32)
        tot = tot + jnp.dot(ohs[1], dx1[:, s], preferred_element_type=F32)
        out[:, s] = jnp.where(last, dg0[:, s] + dg1[:, s], tot)


def _sums(slots, dx0, dx1, dg0, dg1):
    return pl.pallas_call(
        _sums_kernel,
        out_shape=jax.ShapeDtypeStruct((C2, dx0.shape[1]), F32),
        in_specs=[_vm()] * 5,
        out_specs=_vm(),
        compiler_params=_params(6),
        cost_estimate=_cost(1),
        name="dx_sums",
    )(slots, dx0, dx1, dg0, dg1)


def _udw_kernel(per, x_ref, g_ref, w_ref, du_ref, de_in, u_ref, dw_ref, de, n, z, sems):
    i = pl.program_id(0)
    nk, t, f = du_ref.shape
    cb = dw_ref.shape[0]

    @pl.when(i == 0)
    def _():
        z[...] = jnp.zeros_like(z)
        _fill(z, de, sems, AT_U, 0, ZU, False)
        rows = 64
        for b in range(n.shape[0] // rows):
            s = slice(b * rows, (b + 1) * rows)
            xf = x_ref[s].astype(F32)
            rs = lax.rsqrt(jnp.mean(xf * xf, axis=-1, keepdims=True) + EPS)
            n[s] = (xf * rs * g_ref[...].astype(F32)).astype(BF16)
        for c in range(f // CB):
            s = slice(c * CB, (c + 1) * CB)
            out = jnp.dot(n[...], w_ref[:, s], preferred_element_type=F32).astype(BF16)
            for k in range(nk):
                u_ref[k, :, s] = out[k * t:(k + 1) * t]

    _fill(z, de, sems, AT_U, ZU + i * per, jnp.minimum(per, ZW - i * per), False)
    blk = n[:, pl.ds(pl.multiple_of(i * cb, 128), cb)]
    dw_ref[...] = lax.dot_general(
        blk, du_ref[...].reshape(nk * t, f), (((0,), (0,)), ((), ())), preferred_element_type=F32
    )

    @pl.when(i == pl.num_programs(0) - 1)
    def _():
        _fill(z, de, sems, AT_U, 0, ZU + ZW, True)


def _udw(x, g, W, du, de):
    nk, t, f = du.shape
    ntok, d = x.shape
    cb = d // 6
    steps = d // cb
    return pl.pallas_call(
        functools.partial(_udw_kernel, -(-ZW // steps)),
        out_shape=(
            jax.ShapeDtypeStruct((nk, t, f), BF16),
            jax.ShapeDtypeStruct((d, f), F32),
            jax.ShapeDtypeStruct(de.shape, F32),
        ),
        grid=(steps,),
        in_specs=[_vm(), _vm(), _vm(), _vm(), _any()],
        out_specs=(pl.BlockSpec((nk, t, f), lambda i: (0, 0, 0)), pl.BlockSpec((cb, f), lambda i: (i, 0)), _any()),
        scratch_shapes=[VMEM((ntok, d), BF16)] + _zscratch(d, ZU + ZW),
        input_output_aliases={4: 2},
        compiler_params=_params(20),
        cost_estimate=_cost(20),
        name="u_dw",
    )(x, g, W, du, de)


def _scatter_kernel(ts, nk, cnt_ref, list_ref, srow_ref, *refs):
    pieces, (de_in, de, dx, acc, sem) = refs[:-5], refs[-5:]
    ntok = nk * 4 * ts
    for k in range(nk):
        for r in range(4):
            at = pl.multiple_of(k * 4 * ts + (_me() ^ r) * ts, ts)
            dx[pl.ds(at, ts), :] = pieces[r][k * ts:(k + 1) * ts, :]
    cnt = cnt_ref[0, 1]

    def chunk(i, carry):
        base = i * C
        slot = (lax.broadcasted_iota(jnp.int32, (C, ntok), 0) + base).astype(F32)
        oh = jnp.where(slot == srow_ref[...], 1.0, 0.0).astype(BF16)
        for c in range(acc.shape[1] // CB):
            s = slice(c * CB, (c + 1) * CB)
            acc[:, s] = jnp.dot(oh, dx[:, s], preferred_element_type=F32)
        here = jnp.minimum(cnt - base, C)

        def put(j, c2):
            row = list_ref[0, base + j]
            pltpu.make_async_copy(acc.at[pl.ds(j, 1)], de.at[pl.ds(row, 1)], sem).start()
            return c2

        def done(j, c2):
            pltpu.make_async_copy(acc.at[pl.ds(j, 1)], de.at[pl.ds(0, 1)], sem).wait()
            return c2

        lax.fori_loop(0, here, put, 0)
        lax.fori_loop(0, here, done, 0)
        return carry

    lax.fori_loop(0, (cnt + C - 1) // C, chunk, 0)


def _scatter(cnts, rows, srow, pieces, de, ts, nk):
    vs, d = de.shape
    ntok = srow.shape[1]
    return pl.pallas_call(
        functools.partial(_scatter_kernel, ts, nk),
        out_shape=jax.ShapeDtypeStruct((vs, d), F32),
        in_specs=[_sm(), _sm(), _vm()] + [_vm()] * len(pieces) + [_any()],
        out_specs=_any(),
        scratch_shapes=[VMEM((ntok, d), BF16), VMEM((C, d), F32), pltpu.SemaphoreType.DMA],
        input_output_aliases={3 + len(pieces): 0},
        compiler_params=_params(16),
        cost_estimate=_cost(3),
        name="scatter_rows",
    )(cnts, rows, srow, *pieces, de)


def _acc_kernel(lo, n, cnt_ref, oth_ref, slot_ref, dx0, dx1, de_in, de, acc, flag, z, sems):
    z[...] = jnp.zeros_like(z)
    _fill(z, de, sems, lo, 0, n, False)
    for i in (0, 2):
        flag[0, i] = jnp.maximum(cnt_ref[0, i], oth_ref[0, i])
    m = dx0.shape[0]
    j = _iota((C, m), 0)
    ohs = [jnp.where(slot_ref[i:i + 1, :] == j, 1.0, 0.0).astype(BF16) for i in (0, 1)]
    for c in range(acc.shape[1] // CB):
        s = slice(c * CB, (c + 1) * CB)
        tot = jnp.dot(ohs[0], dx0[:, s], preferred_element_type=F32)
        acc[:, s] = tot + jnp.dot(ohs[1], dx1[:, s], preferred_element_type=F32)
    _fill(z, de, sems, lo, 0, n, True)


def _acc(cnts, other, slots, dx0, dx1, de, lo):
    vs, d = de.shape
    n = vs // ZR - lo
    return pl.pallas_call(
        functools.partial(_acc_kernel, lo, n),
        out_shape=(
            jax.ShapeDtypeStruct((vs, d), F32),
            jax.ShapeDtypeStruct((C, d), F32),
            jax.ShapeDtypeStruct((1, 4), jnp.int32),
        ),
        in_specs=[_sm(), _sm()] + [_vm()] * 3 + [_any()],
        out_specs=(_any(), _vm(), _sm()),
        scratch_shapes=_zscratch(d, n),
        input_output_aliases={5: 0},
        compiler_params=_params(8),
        cost_estimate=_cost(n * 0.375),
        name="fill_acc",
    )(cnts, other, slots, dx0, dx1, de)


def _write_kernel(map_ref, acc_in, mine_ref, got_ref, de_in, de, dg_out, acc, sem):
    acc[...] = acc_in[...]

    def add(j, carry):
        at = pl.ds(map_ref[0, j], 1)
        acc[at, :] = acc[at, :] + got_ref[pl.ds(j, 1), :]
        return carry

    lax.fori_loop(0, jnp.minimum(map_ref[0, 127], C2 - 1), add, 0)
    n = jnp.minimum(map_ref[0, 255], C)

    def put(j, carry):
        pltpu.make_async_copy(acc.at[pl.ds(j, 1)], de.at[pl.ds(map_ref[0, 128 + j], 1)], sem).start()
        return carry

    def done(j, carry):
        pltpu.make_async_copy(acc.at[pl.ds(j, 1)], de.at[pl.ds(0, 1)], sem).wait()
        return carry

    lax.fori_loop(0, n, put, 0)
    dg = mine_ref[C2 - 1:C2, :] + got_ref[C2 - 1:C2, :]
    dg_out[...] = dg.reshape(dg_out.shape)
    lax.fori_loop(0, n, done, 0)


def _write(where, acc, mine, got, de):
    vs, d = de.shape
    return pl.pallas_call(
        _write_kernel,
        out_shape=(jax.ShapeDtypeStruct((vs, d), F32), jax.ShapeDtypeStruct((d,), F32)),
        in_specs=[_sm()] + [_vm()] * 3 + [_any()],
        out_specs=(_any(), _vm()),
        scratch_shapes=[VMEM((C, d), F32), pltpu.SemaphoreType.DMA],
        input_output_aliases={4: 0},
        compiler_params=_params(6),
        cost_estimate=_cost(3),
        name="write_rows",
    )(where, acc, mine, got, de)


def solution(mesh):
    ntp = mesh.shape["tp"]
    ndp = mesh.shape["dp"]

    def swap(a, bit):
        return lax.ppermute(a, "tp", [(i, i ^ bit) for i in range(ntp)])

    def share(t):
        t2 = swap(t, 2)
        t1 = swap(t, 1)
        return t, t1, t2, swap(t2, 1)

    def p_terms(du, W, ts, vs):
        q, de = _p_terms(du, W, ts, vs)
        return de, (q[0], swap(q[1], 1), swap(q[2], 2), swap(q[3], 3))

    def body(ids, E, g, W, du, dres):
        vs, d = E.shape
        nk, t = ids.shape
        ts = t // ntp
        m = nk * ts
        g2 = g.reshape(1, d)

        tabs = share(_index_call(None, ids, E, ntp))
        de, ps = p_terms(du, W, ts, vs)
        pos, _, _, cnts, slots, where, de = _slots(jnp.int32(0), ids, ntp, de)
        x, xl = _expand(pos, tabs, ts)
        u, dW, de = _udw(x, g2, W, du, de)
        dx, dg = _dx(xl.reshape(m, d), ps, dres.reshape(m, d), g2)
        dx1, dg1 = swap(dx, 1), swap(dg, 1)
        mine = _sums(slots, dx, dx1, dg, dg1)
        got = swap(mine, 2)
        other = lax.ppermute(cnts, "dp", [(i, (i + 1) % ndp) for i in range(ndp)])
        de, acc, flags = _acc(cnts, other, slots, dx, dx1, de, AT_R)
        dE, dg = _write(where, acc, mine, got, de)
        outs = u, xl, dE, dW, dg

        inputs = ids, E, W, du, dres, g2, flags

        def again(c):
            ids, E, W, du, dres, g2, fl, left = lax.optimization_barrier((*inputs, c[0]))
            rounds = fl[0, 0]
            i0 = left - left

            def more(q):
                i, x, _, de = q
                pos, *_, de = _slots(i, ids, ntp, de)
                return i + 1, *_expand(pos, share(_index_call(i, ids, E, ntp)), ts, x), de

            zeros = jnp.zeros((nk * t, d), BF16), jnp.zeros((nk, ts, d), BF16)
            de, ps = p_terms(du, W, ts, vs)
            _, x, xl, de = lax.while_loop(lambda q: q[0] < rounds, more, (i0, *zeros, de))
            _, srow, rows, cs, _, _, de = _slots(i0, ids, ntp, de)
            u, dW, de = _udw(x, g2, W, du, de)
            dx, dg = _dx(xl.reshape(m, d), ps, dres.reshape(m, d), g2)
            dg2 = dg + swap(dg, 1)
            dg = (dg2 + swap(dg2, 2)).reshape(d)
            dE = _scatter(cs, rows, srow, share(dx), _zeros(de, AT_R, vs // ZR - AT_R), ts, nk)
            return i0, (u, xl, dE, dW, dg)

        _, outs = lax.while_loop(lambda c: c[0] > 0, again, (jnp.minimum(flags[0, 2], 1), outs))
        return outs

    return jax.shard_map(
        body,
        mesh=mesh,
        in_specs=(P("dp", None), P("tp", None), P(None), P(None, "tp"), P("dp", None, "tp"), P("dp", "tp", None)),
        out_specs=(P("dp", None, "tp"), P("dp", "tp", None), P(("dp", "tp"), None), P("dp", "tp"), P("dp")),
        check_vma=False,
    )
```

```python
import functools

import jax
import jax.numpy as jnp
from jax import lax
from jax.experimental import pallas as pl
from jax.experimental.pallas import tpu as pltpu
from jax.sharding import PartitionSpec as P


EPS = 1e-6
C = 56
G = 2
C2 = 32
CB = 256
ZR = 128
ZP, ZA, ZU, ZW, ZB = 8, 6, 15, 22, 4
AT_A, AT_U, AT_B, AT_R = ZP, ZP + ZA, ZP + ZA + ZU + ZW, ZP + ZA + ZU + ZW + ZB
TB = 64

F32 = jnp.float32
BF16 = jnp.bfloat16
VMEM = pltpu.VMEM


def _sm():
    return pl.BlockSpec(memory_space=pltpu.SMEM)


def _vm():
    return pl.BlockSpec(memory_space=pltpu.VMEM)


def _any():
    return pl.BlockSpec(memory_space=pl.ANY)


def _params(mb):
    return pltpu.CompilerParams(vmem_limit_bytes=mb << 20)


def _cost(us):
    return pl.CostEstimate(flops=int(us * 4_000_000_000), bytes_accessed=1_000_000, transcendentals=0)


def _iota(shape, dim):
    return lax.broadcasted_iota(jnp.int32, shape, dim).astype(F32)


def _me():
    return lax.axis_index("tp").astype(jnp.int32)


def _fill(z, o, sems, lo, first, n, wait):
    def step(i, carry):
        at = pl.multiple_of((lo + i) * ZR, ZR)
        c = pltpu.make_async_copy(z, o.at[pl.ds(at, ZR)], sems.at[i])
        c.wait() if wait else c.start()
        return carry

    lax.fori_loop(first, first + n, step, 0)


def _zscratch(d, n):
    return [VMEM((ZR, d), F32), pltpu.SemaphoreType.DMA((n,))]


def _column(row, b):
    w = (b * TB) // 128 * 128
    part = jnp.broadcast_to(row[:, w:w + 128], (TB, 128))
    hit = _iota((TB, 128), 1) == _iota((TB, 128), 0) + float(b * TB - w)
    return jnp.sum(jnp.where(hit, part, 0.0), axis=1, keepdims=True)


def _fold(a):
    return sum(a[8 * q:8 * q + 8] for q in range(1, TB // 8)) + a[:8]


def _ids_row(ids_ref):
    idsf = ids_ref[...].astype(F32)
    return jnp.concatenate([idsf[k:k + 1] for k in range(ids_ref.shape[0])], axis=1)


def _ranks(idr, idcs, vs, ntp, masks):
    ntok = idr.shape[1]
    lane = _iota((TB, ntok), 1)
    thr = _iota((TB, 128), 1) * float(vs)
    rank8 = jnp.zeros((8, ntok), F32)
    below8 = [jnp.zeros((8, 128), F32) for _ in masks]
    for b, idc in enumerate(idcs):
        i = [i for i, (_, blocks) in enumerate(masks) if blocks[b]][0]
        mask = masks[i][0]
        dup = (jnp.broadcast_to(idc, (TB, ntok)) == idr) & (lane < _iota((TB, ntok), 0) + float(b * TB))
        seen = jnp.max(jnp.where(dup, mask, 0.0), axis=1, keepdims=True)
        key = jnp.where(seen > 0.5, float(vs * ntp), idc)
        rank8 = rank8 + _fold(jnp.where(jnp.broadcast_to(key, (TB, ntok)) < idr, mask, 0.0))
        below8[i] = below8[i] + _fold(jnp.where(jnp.broadcast_to(key, (TB, 128)) < thr, 1.0, 0.0))
    return jnp.sum(rank8, axis=0, keepdims=True), [jnp.sum(b8, axis=0, keepdims=True) for b8 in below8]


def _table_slots(idr, idcs, vs, ntp):
    rank, (below,) = _ranks(idr, idcs, vs, ntp, [(jnp.ones_like(idr), [True] * len(idcs))])
    own_r = jnp.floor(idr * (1.0 / vs))
    start = jnp.zeros_like(rank)
    for d in range(ntp):
        start = jnp.where(own_r == float(d), below[:, d:d + 1], start)
    return own_r, rank - start, below


def _index_kernel(vs, ntp, first, *refs):
    if first:
        ids_ref, e_ref, tab_ref, buf, glv, gls, gsem, sem = refs
        base = 0.0
    else:
        c_ref, ids_ref, e_ref, tab_ref, buf, glv, gls, gsem, sem = refs
        base = (c_ref[0] * C).astype(F32)
    me = _me().astype(F32)
    lo = me * vs
    idr = _ids_row(ids_ref)
    ntok = idr.shape[1]
    idcs = [_column(idr, b) for b in range(ntok // TB)]
    own_r, slot_r, _ = _table_slots(idr, idcs, vs, ntp)
    my_r = jnp.where(own_r == me, slot_r, -1.0)
    slot_l = _iota((TB, 128), 1) + base
    acc = jnp.zeros((TB, 128), F32)
    for b, idc in enumerate(idcs):
        acc = jnp.maximum(acc, jnp.where(_column(my_r, b) == slot_l, idc - lo, 0.0))
    glv[...] = jnp.broadcast_to(jnp.max(acc, axis=0, keepdims=True), (8, 128)).astype(jnp.int32)
    cp = pltpu.make_async_copy(glv, gls, gsem)
    cp.start()
    cp.wait()

    def fetch(j, carry):
        g = pl.multiple_of((gls[0, j] >> 1) << 1, G)
        at = pl.multiple_of(j * G, G)
        pltpu.make_async_copy(e_ref.at[pl.ds(g, G)], buf.at[pl.ds(at, G)], sem).start()
        return carry

    lax.fori_loop(0, C, fetch, 0, unroll=8)
    hit = jnp.where(my_r == _iota((C, ntok), 0) + base, idr - lo, 0.0)
    want = jnp.max(hit, axis=1, keepdims=True)
    want = want - jnp.floor(want * (1.0 / G)) * G + _iota((C, 1), 0) * G
    sel = jnp.where(_iota((C, C * G), 1) == want, 1.0, 0.0).astype(BF16)
    pltpu.make_async_copy(e_ref.at[pl.ds(0, C * G)], buf, sem).wait()
    tab_ref[...] = jnp.dot(sel, buf[...], preferred_element_type=F32).astype(BF16)


def _index_call(chunk, ids, E, ntp):
    vs, d = E.shape
    first = chunk is None
    return pl.pallas_call(
        functools.partial(_index_kernel, vs, ntp, first),
        out_shape=jax.ShapeDtypeStruct((C, d), BF16),
        in_specs=([] if first else [_sm()]) + [_vm(), pl.BlockSpec(memory_space=pltpu.HBM)],
        out_specs=_vm(),
        scratch_shapes=[
            VMEM((C * G, d), BF16),
            VMEM((8, 128), jnp.int32),
            pltpu.SMEM((8, 128), jnp.int32),
            pltpu.SemaphoreType.DMA,
            pltpu.SemaphoreType.DMA,
        ],
        compiler_params=_params(8),
        cost_estimate=_cost(12),
        name="index_gather",
    )(*([] if first else [chunk.reshape(1)]), ids, E)


def _slots_kernel(vs, ntp, c_ref, ids_ref, de_in, pos_ref, srow_ref, list_ref, cnt_ref, slot_ref, map_ref, de, z, sems):
    z[...] = jnp.zeros_like(z)
    _fill(z, de, sems, AT_A, 0, ZA, False)
    base = (c_ref[0] * C).astype(F32)
    mei = _me()
    me = mei.astype(F32)
    lo = me * vs
    nk, t = ids_ref.shape
    ntok = nk * t
    nb = ntok // TB
    ts = t // ntp
    idr = _ids_row(ids_ref)
    idcs = [_column(idr, b) for b in range(nb)]
    own_r, slot_r, below = _table_slots(idr, idcs, vs, ntp)
    my_r = jnp.where(own_r == me, slot_r, -1.0)
    cnt = jnp.zeros((1, 1), F32)
    mx = jnp.zeros((1, 1), F32)
    for d in range(ntp):
        nd = below[:, d + 1:d + 2] - below[:, d:d + 1]
        cnt = jnp.where(me == float(d), nd, cnt)
        mx = jnp.maximum(mx, nd)
    srow_ref[...] = my_r
    rel = (own_r.astype(jnp.int32) ^ mei).astype(F32)
    pos = jnp.where((slot_r >= base) & (slot_r < base + C), rel * C + slot_r - base, -1.0)
    for b in range(nb):
        pos_ref[b * TB:(b + 1) * TB, :] = _column(pos, b)

    part = lax.broadcasted_iota(jnp.int32, (1, ntok), 1) // ts % ntp
    chips = [
        (jnp.where(part // 2 == c, 1.0, 0.0), [b * TB // ts % ntp // 2 == c for b in range(nb)])
        for c in range(ntp // 2)
    ]
    rank2, below2 = _ranks(idr, idcs, vs, ntp, chips)
    start2 = jnp.zeros_like(rank2)
    cnt2 = jnp.zeros((1, 1), F32)
    mx2 = jnp.zeros((1, 1), F32)
    for c, (chip, _) in enumerate(chips):
        for d in range(ntp):
            ld = below2[c][:, d:d + 1]
            nd = below2[c][:, d + 1:d + 2] - ld
            start2 = jnp.where((own_r == float(d)) & (chip > 0.5), ld, start2)
            if d // 2 != c:
                cnt2 = jnp.where(me == float(d), nd, cnt2)
                mx2 = jnp.maximum(mx2, nd)
    slot2_r = rank2 - start2
    lane1 = lax.broadcasted_iota(jnp.int32, (1, 128), 1)
    over = jnp.where((mx > C) | (mx2 > C2 - 1), 1.0, 0.0)
    rounds = jnp.floor((mx + C - 1.0) * (1.0 / C))
    cnts = jnp.where(lane1 == 0, rounds, jnp.where(lane1 == 1, cnt, jnp.where(lane1 == 2, over, cnt2)))
    cnt_ref[...] = cnts.astype(jnp.int32)
    sums_r = [jnp.where(own_r == (mei ^ o).astype(F32), slot2_r, -1.0) for o in (2, 3)]
    rows = [jnp.zeros((1, nk * ts), F32)] * 4
    for q in range(ntp):
        at = [slice(k * t + q * ts, k * t + (q + 1) * ts) for k in range(nk)]
        mine = jnp.concatenate([my_r[:, w] for w in at], axis=1)
        sums = [jnp.concatenate([r[:, w] for w in at], axis=1) for r in sums_r]
        own, sib = me == float(q), me == float(q ^ 1)
        rows = [
            jnp.where(own, mine, rows[0]), jnp.where(sib, mine, rows[1]),
            jnp.where(own, sums[0], rows[2]), jnp.where(own, sums[1], rows[3]),
        ]
    for j, r in enumerate(rows):
        slot_ref[j:j + 1, :] = r
    far = (part // 2).astype(F32) != jnp.floor(me * 0.5)
    got_r = jnp.where(far & (own_r == me), slot2_r, -1.0)
    acc2 = jnp.zeros((TB, 128), F32)
    slot_j = _iota((TB, 128), 1)
    full = jnp.zeros((8, ntok), F32)
    lane8 = _iota((8, ntok), 1)
    for b in range(nb):
        my_c = _column(my_r, b)
        acc2 = jnp.maximum(acc2, jnp.where(_column(got_r, b) == slot_j, my_c, 0.0))
        for q in range(TB // 8):
            s = slice(8 * q, 8 * q + 8)
            full = jnp.maximum(full, jnp.where(my_c[s] == lane8, idcs[b][s] - lo, 0.0))
    full = jnp.max(full, axis=0, keepdims=True)
    list_ref[...] = full.astype(jnp.int32)
    slots = jnp.minimum(jnp.max(acc2, axis=0, keepdims=True), C - 1.0)
    many = jnp.where(lane1 == 127, cnt2, slots)
    mine = jnp.where(lane1 == 127, cnt, full[:, :128])
    map_ref[...] = jnp.concatenate([many, mine], axis=1).astype(jnp.int32)
    _fill(z, de, sems, AT_A, 0, ZA, True)


def _slots(chunk, ids, ntp, de):
    vs, d = de.shape
    ntok = ids.shape[0] * ids.shape[1]
    return pl.pallas_call(
        functools.partial(_slots_kernel, vs, ntp),
        out_shape=(
            jax.ShapeDtypeStruct((ntok, 1), F32),
            jax.ShapeDtypeStruct((1, ntok), F32),
            jax.ShapeDtypeStruct((1, ntok), jnp.int32),
            jax.ShapeDtypeStruct((1, 128), jnp.int32),
            jax.ShapeDtypeStruct((4, ntok // ntp), F32),
            jax.ShapeDtypeStruct((1, 256), jnp.int32),
            jax.ShapeDtypeStruct(de.shape, F32),
        ),
        in_specs=[_sm(), _vm(), _any()],
        out_specs=(_vm(),) * 6 + (_any(),),
        scratch_shapes=_zscratch(d, ZA),
        input_output_aliases={2: 6},
        compiler_params=_params(6),
        cost_estimate=_cost(3),
        name="slots",
    )(chunk.reshape(1), ids, de)


def _expand_kernel(ts, acc, *refs):
    if acc:
        x_in, pos, t0, t1, t2, t3, x_out, xl_out = refs
    else:
        pos, t0, t1, t2, t3, x_out, xl_out = refs
    oh = jnp.where(pos[...] == _iota((pos.shape[0], 4 * C), 1), 1.0, 0.0).astype(BF16)
    for c in range(x_out.shape[1] // CB):
        s = slice(c * CB, (c + 1) * CB)
        tab = jnp.concatenate([t[:, s] for t in (t0, t1, t2, t3)], axis=0)
        tot = jnp.dot(oh, tab, preferred_element_type=F32)
        if acc:
            tot = tot + x_in[:, s].astype(F32)
        x_out[:, s] = tot.astype(BF16)
    t = 4 * ts
    for k in range(x_out.shape[0] // t):
        at = pl.multiple_of(k * t + _me() * ts, ts)
        xl_out[k] = x_out[pl.ds(at, ts), :]


def _expand(pos, tabs, ts, x=None):
    ntok, d = pos.shape[0], tabs[0].shape[1]
    ins = ([x] if x is not None else []) + [pos, *tabs]
    return pl.pallas_call(
        functools.partial(_expand_kernel, ts, x is not None),
        out_shape=(jax.ShapeDtypeStruct((ntok, d), BF16), jax.ShapeDtypeStruct((ntok // (4 * ts), ts, d), BF16)),
        in_specs=[_vm()] * len(ins),
        out_specs=(_vm(), _vm()),
        compiler_params=_params(12),
        cost_estimate=_cost(3),
        name="expand",
    )(*ins)


def _p_kernel(ts, du_ref, w_ref, *refs):
    outs, (de, dur, z, sems) = refs[:-4], refs[-4:]
    nk = du_ref.shape[0]

    @pl.when(pl.program_id(0) == 0)
    def _():
        z[...] = jnp.zeros_like(z)
        for k in range(nk):
            for r in range(4):
                at = pl.multiple_of((_me() ^ r) * ts, ts)
                dur[pl.ds((r * nk + k) * ts, ts), :] = du_ref[k, pl.ds(at, ts), :]
        _fill(z, de, sems, 0, 0, ZP, False)

    out = lax.dot_general(dur[...], w_ref[...], (((1,), (1,)), ((), ())), preferred_element_type=F32)
    for i, o in enumerate(outs):
        o[...] = out[i * nk * ts:(i + 1) * nk * ts].astype(BF16)

    @pl.when(pl.program_id(0) == pl.num_programs(0) - 1)
    def _():
        _fill(z, de, sems, 0, 0, ZP, True)


def _p_terms(du, W, ts, vs):
    nk, t, f = du.shape
    d = W.shape[0]
    cb = 3 * CB
    out = pl.pallas_call(
        functools.partial(_p_kernel, ts),
        out_shape=(jax.ShapeDtypeStruct((nk * ts, d), BF16),) * 4 + (jax.ShapeDtypeStruct((vs, d), F32),),
        grid=(d // cb,),
        in_specs=[pl.BlockSpec((nk, t, f), lambda i: (0, 0, 0)), pl.BlockSpec((cb, f), lambda i: (i, 0))],
        out_specs=(pl.BlockSpec((nk * ts, cb), lambda i: (0, i)),) * 4 + (_any(),),
        scratch_shapes=[VMEM((nk * t, f), BF16)] + _zscratch(d, ZP),
        compiler_params=_params(20),
        cost_estimate=_cost(5),
        name="p_terms",
    )(du, W)
    return out[:4], out[4]


def _zero_kernel(lo, n, de_in, o, z, sems):
    z[...] = jnp.zeros_like(z)
    _fill(z, o, sems, lo, 0, n, False)
    _fill(z, o, sems, lo, 0, n, True)


def _zeros(de, lo, n):
    vs, d = de.shape
    return pl.pallas_call(
        functools.partial(_zero_kernel, lo, n),
        out_shape=jax.ShapeDtypeStruct((vs, d), F32),
        in_specs=[_any()],
        out_specs=_any(),
        scratch_shapes=_zscratch(d, n),
        input_output_aliases={0: 0},
        compiler_params=_params(4),
        cost_estimate=_cost(n * 0.375),
    )(de)


def _dx_rows(x, p0, p1, p2, p3, dres, g, dx):
    rows = 32
    tot = None
    for b in range(dx.shape[0] // rows):
        s = slice(b * rows, (b + 1) * rows)
        xf = x[s].astype(F32)
        rs = lax.rsqrt(jnp.mean(xf * xf, axis=-1, keepdims=True) + EPS)
        nh = xf * rs
        dn = (p0[s].astype(F32) + p1[s].astype(F32)) + (p2[s].astype(F32) + p3[s].astype(F32))
        gdn = g[...].astype(F32) * dn
        out = dres[s].astype(F32) + rs * (gdn - nh * jnp.mean(nh * gdn, axis=-1, keepdims=True))
        dx[s] = out.astype(BF16)
        part = jnp.sum(dn * nh, axis=0, keepdims=True)
        tot = part if tot is None else tot + part
    return tot


def _dx_kernel(*refs):
    refs[-1][...] = _dx_rows(*refs[:-1])


def _dx(x, ps, dres, g):
    m, d = x.shape
    return pl.pallas_call(
        _dx_kernel,
        out_shape=(
            jax.ShapeDtypeStruct((m, d), BF16),
            jax.ShapeDtypeStruct((1, d), F32),
        ),
        in_specs=[_vm()] * 7,
        out_specs=(_vm(), _vm()),
        compiler_params=_params(12),
        cost_estimate=_cost(2),
        name="dx_form",
    )(x, *ps, dres, g)


def _dx_sums_kernel(x, p0, p1, p2, p3, dres, g, slot_ref, dx, mine, out, got, send, recv):
    sib = _me() ^ 1
    barrier = pltpu.get_barrier_semaphore()
    pl.semaphore_signal(barrier, inc=1, device_id={"tp": sib}, device_id_type=pl.DeviceIdType.MESH)
    dg = _dx_rows(x, p0, p1, p2, p3, dres, g, dx)
    j = _iota((C2, dx.shape[0]), 0)
    last = lax.broadcasted_iota(jnp.int32, (C2, CB), 0) == C2 - 1

    def sums(i, to):
        oh = jnp.where(slot_ref[i:i + 1, :] == j, 1.0, 0.0).astype(BF16)
        for c in range(to.shape[1] // CB):
            s = slice(c * CB, (c + 1) * CB)
            to[:, s] = jnp.where(last, dg[:, s], jnp.dot(oh, dx[:, s], preferred_element_type=F32))

    sums(3, out)
    pl.semaphore_wait(barrier, 1)
    copy = pltpu.make_async_remote_copy(
        src_ref=out, dst_ref=got, send_sem=send, recv_sem=recv,
        device_id={"tp": sib}, device_id_type=pl.DeviceIdType.MESH,
    )
    copy.start()
    sums(2, mine)
    copy.wait()
    mine[...] = mine[...] + got[...]


def _dx_sums(x, ps, dres, g, slots):
    m, d = x.shape
    return pl.pallas_call(
        _dx_sums_kernel,
        out_shape=(jax.ShapeDtypeStruct((m, d), BF16), jax.ShapeDtypeStruct((C2, d), F32)),
        in_specs=[_vm()] * 8,
        out_specs=(_vm(), _vm()),
        scratch_shapes=[VMEM((C2, d), F32), VMEM((C2, d), F32), pltpu.SemaphoreType.DMA, pltpu.SemaphoreType.DMA],
        compiler_params=pltpu.CompilerParams(vmem_limit_bytes=12 << 20, collective_id=0, has_side_effects=True),
        cost_estimate=_cost(3),
        name="dx_sums",
    )(x, *ps, dres, g, slots)


def _udw_kernel(per, x_ref, g_ref, w_ref, du_ref, de_in, u_ref, dw_ref, de, n, z, sems):
    i = pl.program_id(0)
    nk, t, f = du_ref.shape
    cb = dw_ref.shape[0]

    @pl.when(i == 0)
    def _():
        z[...] = jnp.zeros_like(z)
        _fill(z, de, sems, AT_U, 0, ZU, False)
        rows = 64
        for b in range(n.shape[0] // rows):
            s = slice(b * rows, (b + 1) * rows)
            xf = x_ref[s].astype(F32)
            rs = lax.rsqrt(jnp.mean(xf * xf, axis=-1, keepdims=True) + EPS)
            n[s] = (xf * rs * g_ref[...].astype(F32)).astype(BF16)
        for c in range(f // CB):
            s = slice(c * CB, (c + 1) * CB)
            out = jnp.dot(n[...], w_ref[:, s], preferred_element_type=F32).astype(BF16)
            for k in range(nk):
                u_ref[k, :, s] = out[k * t:(k + 1) * t]

    _fill(z, de, sems, AT_U, ZU + i * per, jnp.minimum(per, ZW - i * per), False)
    blk = n[:, pl.ds(pl.multiple_of(i * cb, 128), cb)]
    dw_ref[...] = lax.dot_general(
        blk, du_ref[...].reshape(nk * t, f), (((0,), (0,)), ((), ())), preferred_element_type=F32
    )

    @pl.when(i == pl.num_programs(0) - 1)
    def _():
        _fill(z, de, sems, AT_U, 0, ZU + ZW, True)


def _udw(x, g, W, du, de):
    nk, t, f = du.shape
    ntok, d = x.shape
    cb = d // 6
    steps = d // cb
    return pl.pallas_call(
        functools.partial(_udw_kernel, -(-ZW // steps)),
        out_shape=(
            jax.ShapeDtypeStruct((nk, t, f), BF16),
            jax.ShapeDtypeStruct((d, f), F32),
            jax.ShapeDtypeStruct(de.shape, F32),
        ),
        grid=(steps,),
        in_specs=[_vm(), _vm(), _vm(), _vm(), _any()],
        out_specs=(pl.BlockSpec((nk, t, f), lambda i: (0, 0, 0)), pl.BlockSpec((cb, f), lambda i: (i, 0)), _any()),
        scratch_shapes=[VMEM((ntok, d), BF16)] + _zscratch(d, ZU + ZW),
        input_output_aliases={4: 2},
        compiler_params=_params(20),
        cost_estimate=_cost(20),
        name="u_dw",
    )(x, g, W, du, de)


def _scatter_kernel(ts, nk, cnt_ref, list_ref, srow_ref, *refs):
    pieces, (de_in, de, dx, acc, sem) = refs[:-5], refs[-5:]
    ntok = nk * 4 * ts
    for k in range(nk):
        for r in range(4):
            at = pl.multiple_of(k * 4 * ts + (_me() ^ r) * ts, ts)
            dx[pl.ds(at, ts), :] = pieces[r][k * ts:(k + 1) * ts, :]
    cnt = cnt_ref[0, 1]

    def chunk(i, carry):
        base = i * C
        slot = (lax.broadcasted_iota(jnp.int32, (C, ntok), 0) + base).astype(F32)
        oh = jnp.where(slot == srow_ref[...], 1.0, 0.0).astype(BF16)
        for c in range(acc.shape[1] // CB):
            s = slice(c * CB, (c + 1) * CB)
            acc[:, s] = jnp.dot(oh, dx[:, s], preferred_element_type=F32)
        here = jnp.minimum(cnt - base, C)

        def put(j, c2):
            row = list_ref[0, base + j]
            pltpu.make_async_copy(acc.at[pl.ds(j, 1)], de.at[pl.ds(row, 1)], sem).start()
            return c2

        def done(j, c2):
            pltpu.make_async_copy(acc.at[pl.ds(j, 1)], de.at[pl.ds(0, 1)], sem).wait()
            return c2

        lax.fori_loop(0, here, put, 0)
        lax.fori_loop(0, here, done, 0)
        return carry

    lax.fori_loop(0, (cnt + C - 1) // C, chunk, 0)


def _scatter(cnts, rows, srow, pieces, de, ts, nk):
    vs, d = de.shape
    ntok = srow.shape[1]
    return pl.pallas_call(
        functools.partial(_scatter_kernel, ts, nk),
        out_shape=jax.ShapeDtypeStruct((vs, d), F32),
        in_specs=[_sm(), _sm(), _vm()] + [_vm()] * len(pieces) + [_any()],
        out_specs=_any(),
        scratch_shapes=[VMEM((ntok, d), BF16), VMEM((C, d), F32), pltpu.SemaphoreType.DMA],
        input_output_aliases={3 + len(pieces): 0},
        compiler_params=_params(16),
        cost_estimate=_cost(3),
        name="scatter_rows",
    )(cnts, rows, srow, *pieces, de)


def _acc_kernel(lo, n, cnt_ref, oth_ref, slot_ref, dx0, dx1, de_in, de, acc, flag, z, sems):
    z[...] = jnp.zeros_like(z)
    _fill(z, de, sems, lo, 0, n, False)
    for i in (0, 2):
        flag[0, i] = jnp.maximum(cnt_ref[0, i], oth_ref[0, i])
    m = dx0.shape[0]
    j = _iota((C, m), 0)
    ohs = [jnp.where(slot_ref[i:i + 1, :] == j, 1.0, 0.0).astype(BF16) for i in (0, 1)]
    for c in range(acc.shape[1] // CB):
        s = slice(c * CB, (c + 1) * CB)
        tot = jnp.dot(ohs[0], dx0[:, s], preferred_element_type=F32)
        acc[:, s] = tot + jnp.dot(ohs[1], dx1[:, s], preferred_element_type=F32)
    _fill(z, de, sems, lo, 0, n, True)


def _acc(cnts, other, slots, dx0, dx1, de, lo):
    vs, d = de.shape
    n = vs // ZR - lo
    return pl.pallas_call(
        functools.partial(_acc_kernel, lo, n),
        out_shape=(
            jax.ShapeDtypeStruct((vs, d), F32),
            jax.ShapeDtypeStruct((C, d), F32),
            jax.ShapeDtypeStruct((1, 4), jnp.int32),
        ),
        in_specs=[_sm(), _sm()] + [_vm()] * 3 + [_any()],
        out_specs=(_any(), _vm(), _sm()),
        scratch_shapes=_zscratch(d, n),
        input_output_aliases={5: 0},
        compiler_params=_params(8),
        cost_estimate=_cost(n * 0.375),
        name="fill_acc",
    )(cnts, other, slots, dx0, dx1, de)


def _write_kernel(map_ref, acc_in, mine_ref, got_ref, de_in, de, dg_out, acc, sem):
    acc[...] = acc_in[...]

    def add(j, carry):
        at = pl.ds(map_ref[0, j], 1)
        acc[at, :] = acc[at, :] + got_ref[pl.ds(j, 1), :]
        return carry

    lax.fori_loop(0, jnp.minimum(map_ref[0, 127], C2 - 1), add, 0)
    n = jnp.minimum(map_ref[0, 255], C)

    def put(j, carry):
        pltpu.make_async_copy(acc.at[pl.ds(j, 1)], de.at[pl.ds(map_ref[0, 128 + j], 1)], sem).start()
        return carry

    def done(j, carry):
        pltpu.make_async_copy(acc.at[pl.ds(j, 1)], de.at[pl.ds(0, 1)], sem).wait()
        return carry

    lax.fori_loop(0, n, put, 0)
    dg = mine_ref[C2 - 1:C2, :] + got_ref[C2 - 1:C2, :]
    dg_out[...] = dg.reshape(dg_out.shape)
    lax.fori_loop(0, n, done, 0)


def _write(where, acc, mine, got, de):
    vs, d = de.shape
    return pl.pallas_call(
        _write_kernel,
        out_shape=(jax.ShapeDtypeStruct((vs, d), F32), jax.ShapeDtypeStruct((d,), F32)),
        in_specs=[_sm()] + [_vm()] * 3 + [_any()],
        out_specs=(_any(), _vm()),
        scratch_shapes=[VMEM((C, d), F32), pltpu.SemaphoreType.DMA],
        input_output_aliases={4: 0},
        compiler_params=_params(6),
        cost_estimate=_cost(3),
        name="write_rows",
    )(where, acc, mine, got, de)


def solution(mesh):
    ntp = mesh.shape["tp"]
    ndp = mesh.shape["dp"]

    def swap(a, bit):
        return lax.ppermute(a, "tp", [(i, i ^ bit) for i in range(ntp)])

    def share(t):
        t2 = swap(t, 2)
        t1 = swap(t, 1)
        return t, t1, t2, swap(t2, 1)

    def p_terms(du, W, ts, vs):
        q, de = _p_terms(du, W, ts, vs)
        return de, (q[0], swap(q[1], 1), swap(q[2], 2), swap(q[3], 3))

    def body(ids, E, g, W, du, dres):
        vs, d = E.shape
        nk, t = ids.shape
        ts = t // ntp
        m = nk * ts
        g2 = g.reshape(1, d)

        tabs = share(_index_call(None, ids, E, ntp))
        de, ps = p_terms(du, W, ts, vs)
        pos, _, _, cnts, slots, where, de = _slots(jnp.int32(0), ids, ntp, de)
        x, xl = _expand(pos, tabs, ts)
        u, dW, de = _udw(x, g2, W, du, de)
        dx, mine = _dx_sums(xl.reshape(m, d), ps, dres.reshape(m, d), g2, slots)
        got = swap(mine, 2)
        dx1 = swap(dx, 1)
        de = _zeros(de, AT_B, ZB)
        other = lax.ppermute(cnts, "dp", [(i, (i + 1) % ndp) for i in range(ndp)])
        de, acc, flags = _acc(cnts, other, slots, dx, dx1, de, AT_R)
        dE, dg = _write(where, acc, mine, got, de)
        outs = u, xl, dE, dW, dg

        inputs = ids, E, W, du, dres, g2, flags

        def again(c):
            ids, E, W, du, dres, g2, fl, left = lax.optimization_barrier((*inputs, c[0]))
            rounds = fl[0, 0]
            i0 = left - left

            def more(q):
                i, x, _, de = q
                pos, *_, de = _slots(i, ids, ntp, de)
                return i + 1, *_expand(pos, share(_index_call(i, ids, E, ntp)), ts, x), de

            zeros = jnp.zeros((nk * t, d), BF16), jnp.zeros((nk, ts, d), BF16)
            de, ps = p_terms(du, W, ts, vs)
            _, x, xl, de = lax.while_loop(lambda q: q[0] < rounds, more, (i0, *zeros, de))
            _, srow, rows, cs, _, _, de = _slots(i0, ids, ntp, de)
            u, dW, de = _udw(x, g2, W, du, de)
            dx, dg = _dx(xl.reshape(m, d), ps, dres.reshape(m, d), g2)
            dg2 = dg + swap(dg, 1)
            dg = (dg2 + swap(dg2, 2)).reshape(d)
            dE = _scatter(cs, rows, srow, share(dx), _zeros(de, AT_B, vs // ZR - AT_B), ts, nk)
            return i0, (u, xl, dE, dW, dg)

        _, outs = lax.while_loop(lambda c: c[0] > 0, again, (jnp.minimum(flags[0, 2], 1), outs))
        return outs

    return jax.shard_map(
        body,
        mesh=mesh,
        in_specs=(P("dp", None), P("tp", None), P(None), P(None, "tp"), P("dp", None, "tp"), P("dp", "tp", None)),
        out_specs=(P("dp", None, "tp"), P("dp", "tp", None), P(("dp", "tp"), None), P("dp", "tp"), P("dp")),
        check_vma=False,
    )
```

```python
import functools

import jax
import jax.numpy as jnp
from jax import lax
from jax.experimental import pallas as pl
from jax.experimental.pallas import tpu as pltpu
from jax.sharding import PartitionSpec as P


EPS = 1e-6
C = 56
G = 2
C2 = 32
CB = 256
ZR = 128
ZP, ZA, ZU, ZW, ZB = 8, 4, 22, 20, 4
AT_A, AT_U, AT_B, AT_R = ZP, ZP + ZA, ZP + ZA + ZU + ZW, ZP + ZA + ZU + ZW + ZB
TB = 64

F32 = jnp.float32
BF16 = jnp.bfloat16
VMEM = pltpu.VMEM


def _sm():
    return pl.BlockSpec(memory_space=pltpu.SMEM)


def _vm():
    return pl.BlockSpec(memory_space=pltpu.VMEM)


def _any():
    return pl.BlockSpec(memory_space=pl.ANY)


def _params(mb):
    return pltpu.CompilerParams(vmem_limit_bytes=mb << 20)


def _cost(us):
    return pl.CostEstimate(flops=int(us * 4_000_000_000), bytes_accessed=1_000_000, transcendentals=0)


def _iota(shape, dim):
    return lax.broadcasted_iota(jnp.int32, shape, dim).astype(F32)


def _me():
    return lax.axis_index("tp").astype(jnp.int32)


def _fill(z, o, sems, lo, first, n, wait):
    def step(i, carry):
        at = pl.multiple_of((lo + i) * ZR, ZR)
        c = pltpu.make_async_copy(z, o.at[pl.ds(at, ZR)], sems.at[i])
        c.wait() if wait else c.start()
        return carry

    lax.fori_loop(first, first + n, step, 0)


def _zscratch(d, n):
    return [VMEM((ZR, d), F32), pltpu.SemaphoreType.DMA((n,))]


def _column(row, b):
    w = (b * TB) // 128 * 128
    part = jnp.broadcast_to(row[:, w:w + 128], (TB, 128))
    hit = _iota((TB, 128), 1) == _iota((TB, 128), 0) + float(b * TB - w)
    return jnp.sum(jnp.where(hit, part, 0.0), axis=1, keepdims=True)


def _fold(a):
    return sum(a[8 * q:8 * q + 8] for q in range(1, TB // 8)) + a[:8]


def _ids_row(ids_ref):
    idsf = ids_ref[...].astype(F32)
    return jnp.concatenate([idsf[k:k + 1] for k in range(ids_ref.shape[0])], axis=1)


def _ranks(idr, idcs, vs, ntp, masks):
    ntok = idr.shape[1]
    lane = _iota((TB, ntok), 1)
    thr = _iota((TB, 128), 1) * float(vs)
    rank8 = jnp.zeros((8, ntok), F32)
    below8 = [jnp.zeros((8, 128), F32) for _ in masks]
    for b, idc in enumerate(idcs):
        i = [i for i, (_, blocks) in enumerate(masks) if blocks[b]][0]
        mask = masks[i][0]
        dup = (jnp.broadcast_to(idc, (TB, ntok)) == idr) & (lane < _iota((TB, ntok), 0) + float(b * TB))
        seen = jnp.max(jnp.where(dup, mask, 0.0), axis=1, keepdims=True)
        key = jnp.where(seen > 0.5, float(vs * ntp), idc)
        rank8 = rank8 + _fold(jnp.where(jnp.broadcast_to(key, (TB, ntok)) < idr, mask, 0.0))
        below8[i] = below8[i] + _fold(jnp.where(jnp.broadcast_to(key, (TB, 128)) < thr, 1.0, 0.0))
    return jnp.sum(rank8, axis=0, keepdims=True), [jnp.sum(b8, axis=0, keepdims=True) for b8 in below8]


def _table_slots(idr, idcs, vs, ntp):
    rank, (below,) = _ranks(idr, idcs, vs, ntp, [(jnp.ones_like(idr), [True] * len(idcs))])
    own_r = jnp.floor(idr * (1.0 / vs))
    start = jnp.zeros_like(rank)
    for d in range(ntp):
        start = jnp.where(own_r == float(d), below[:, d:d + 1], start)
    return own_r, rank - start, below


def _index_kernel(vs, ntp, first, *refs):
    if first:
        ids_ref, e_ref, tab_ref, buf, glv, gls, gsem, sem = refs
        base = 0.0
    else:
        c_ref, ids_ref, e_ref, tab_ref, buf, glv, gls, gsem, sem = refs
        base = (c_ref[0] * C).astype(F32)
    me = _me().astype(F32)
    lo = me * vs
    idr = _ids_row(ids_ref)
    ntok = idr.shape[1]
    idcs = [_column(idr, b) for b in range(ntok // TB)]
    own_r, slot_r, _ = _table_slots(idr, idcs, vs, ntp)
    my_r = jnp.where(own_r == me, slot_r, -1.0)
    slot_l = _iota((TB, 128), 1) + base
    acc = jnp.zeros((TB, 128), F32)
    for b, idc in enumerate(idcs):
        acc = jnp.maximum(acc, jnp.where(_column(my_r, b) == slot_l, idc - lo, 0.0))
    glv[...] = jnp.broadcast_to(jnp.max(acc, axis=0, keepdims=True), (8, 128)).astype(jnp.int32)
    cp = pltpu.make_async_copy(glv, gls, gsem)
    cp.start()
    cp.wait()

    def fetch(j, carry):
        g = pl.multiple_of((gls[0, j] >> 1) << 1, G)
        at = pl.multiple_of(j * G, G)
        pltpu.make_async_copy(e_ref.at[pl.ds(g, G)], buf.at[pl.ds(at, G)], sem).start()
        return carry

    lax.fori_loop(0, C, fetch, 0, unroll=8)
    hit = jnp.where(my_r == _iota((C, ntok), 0) + base, idr - lo, 0.0)
    want = jnp.max(hit, axis=1, keepdims=True)
    want = want - jnp.floor(want * (1.0 / G)) * G + _iota((C, 1), 0) * G
    sel = jnp.where(_iota((C, C * G), 1) == want, 1.0, 0.0).astype(BF16)
    pltpu.make_async_copy(e_ref.at[pl.ds(0, C * G)], buf, sem).wait()
    tab_ref[...] = jnp.dot(sel, buf[...], preferred_element_type=F32).astype(BF16)


def _index_call(chunk, ids, E, ntp):
    vs, d = E.shape
    first = chunk is None
    return pl.pallas_call(
        functools.partial(_index_kernel, vs, ntp, first),
        out_shape=jax.ShapeDtypeStruct((C, d), BF16),
        in_specs=([] if first else [_sm()]) + [_vm(), pl.BlockSpec(memory_space=pltpu.HBM)],
        out_specs=_vm(),
        scratch_shapes=[
            VMEM((C * G, d), BF16),
            VMEM((8, 128), jnp.int32),
            pltpu.SMEM((8, 128), jnp.int32),
            pltpu.SemaphoreType.DMA,
            pltpu.SemaphoreType.DMA,
        ],
        compiler_params=_params(8),
        cost_estimate=_cost(12),
        name="index_gather",
    )(*([] if first else [chunk.reshape(1)]), ids, E)


def _pos_kernel(vs, ntp, c_ref, ids_ref, de_in, pos_ref, de, z, sems):
    z[...] = jnp.zeros_like(z)
    _fill(z, de, sems, AT_A, 0, ZA, False)
    base = (c_ref[0] * C).astype(F32)
    idr = _ids_row(ids_ref)
    nb = idr.shape[1] // TB
    own_r, slot_r, _ = _table_slots(idr, [_column(idr, b) for b in range(nb)], vs, ntp)
    rel = (own_r.astype(jnp.int32) ^ _me()).astype(F32)
    pos = jnp.where((slot_r >= base) & (slot_r < base + C), rel * C + slot_r - base, -1.0)
    for b in range(nb):
        pos_ref[b * TB:(b + 1) * TB, :] = _column(pos, b)
    _fill(z, de, sems, AT_A, 0, ZA, True)


def _pos(chunk, ids, ntp, de):
    vs, d = de.shape
    ntok = ids.shape[0] * ids.shape[1]
    return pl.pallas_call(
        functools.partial(_pos_kernel, vs, ntp),
        out_shape=(jax.ShapeDtypeStruct((ntok, 1), F32), jax.ShapeDtypeStruct(de.shape, F32)),
        in_specs=[_sm(), _vm(), _any()],
        out_specs=(_vm(), _any()),
        scratch_shapes=_zscratch(d, ZA),
        input_output_aliases={2: 1},
        compiler_params=_params(6),
        cost_estimate=_cost(3),
        name="positions",
    )(chunk.reshape(1), ids, de)


def _slots(vs, ntp, ids_ref, srow_ref, list_ref, cnt_ref, slot_ref, map_ref):
    mei = _me()
    me = mei.astype(F32)
    lo = me * vs
    nk, t = ids_ref.shape
    ntok = nk * t
    nb = ntok // TB
    ts = t // ntp
    idr = _ids_row(ids_ref)
    idcs = [_column(idr, b) for b in range(nb)]
    own_r, slot_r, below = _table_slots(idr, idcs, vs, ntp)
    my_r = jnp.where(own_r == me, slot_r, -1.0)
    cnt = jnp.zeros((1, 1), F32)
    mx = jnp.zeros((1, 1), F32)
    for d in range(ntp):
        nd = below[:, d + 1:d + 2] - below[:, d:d + 1]
        cnt = jnp.where(me == float(d), nd, cnt)
        mx = jnp.maximum(mx, nd)
    srow_ref[...] = my_r

    part = lax.broadcasted_iota(jnp.int32, (1, ntok), 1) // ts % ntp
    chips = [
        (jnp.where(part // 2 == c, 1.0, 0.0), [b * TB // ts % ntp // 2 == c for b in range(nb)])
        for c in range(ntp // 2)
    ]
    rank2, below2 = _ranks(idr, idcs, vs, ntp, chips)
    start2 = jnp.zeros_like(rank2)
    cnt2 = jnp.zeros((1, 1), F32)
    mx2 = jnp.zeros((1, 1), F32)
    for c, (chip, _) in enumerate(chips):
        for d in range(ntp):
            ld = below2[c][:, d:d + 1]
            nd = below2[c][:, d + 1:d + 2] - ld
            start2 = jnp.where((own_r == float(d)) & (chip > 0.5), ld, start2)
            if d // 2 != c:
                cnt2 = jnp.where(me == float(d), nd, cnt2)
                mx2 = jnp.maximum(mx2, nd)
    slot2_r = rank2 - start2
    lane1 = lax.broadcasted_iota(jnp.int32, (1, 128), 1)
    over = jnp.where((mx > C) | (mx2 > C2 - 1), 1.0, 0.0)
    rounds = jnp.floor((mx + C - 1.0) * (1.0 / C))
    cnts = jnp.where(lane1 == 0, rounds, jnp.where(lane1 == 1, cnt, jnp.where(lane1 == 2, over, cnt2)))
    cnt_ref[...] = cnts.astype(jnp.int32)
    sums_r = [jnp.where(own_r == (mei ^ o).astype(F32), slot2_r, -1.0) for o in (2, 3)]
    rows = [jnp.zeros((1, nk * ts), F32)] * 4
    for q in range(ntp):
        at = [slice(k * t + q * ts, k * t + (q + 1) * ts) for k in range(nk)]
        mine = jnp.concatenate([my_r[:, w] for w in at], axis=1)
        sums = [jnp.concatenate([r[:, w] for w in at], axis=1) for r in sums_r]
        own, sib = me == float(q), me == float(q ^ 1)
        rows = [
            jnp.where(own, mine, rows[0]), jnp.where(sib, mine, rows[1]),
            jnp.where(own, sums[0], rows[2]), jnp.where(own, sums[1], rows[3]),
        ]
    for j, r in enumerate(rows):
        slot_ref[j:j + 1, :] = r
    far = (part // 2).astype(F32) != jnp.floor(me * 0.5)
    got_r = jnp.where(far & (own_r == me), slot2_r, -1.0)
    acc2 = jnp.zeros((TB, 128), F32)
    slot_j = _iota((TB, 128), 1)
    full = jnp.zeros((8, ntok), F32)
    lane8 = _iota((8, ntok), 1)
    for b in range(nb):
        my_c = _column(my_r, b)
        acc2 = jnp.maximum(acc2, jnp.where(_column(got_r, b) == slot_j, my_c, 0.0))
        for q in range(TB // 8):
            s = slice(8 * q, 8 * q + 8)
            full = jnp.maximum(full, jnp.where(my_c[s] == lane8, idcs[b][s] - lo, 0.0))
    full = jnp.max(full, axis=0, keepdims=True)
    list_ref[...] = full.astype(jnp.int32)
    slots = jnp.minimum(jnp.max(acc2, axis=0, keepdims=True), C - 1.0)
    many = jnp.where(lane1 == 127, cnt2, slots)
    mine = jnp.where(lane1 == 127, cnt, full[:, :128])
    map_ref[...] = jnp.concatenate([many, mine], axis=1).astype(jnp.int32)


def _expand_kernel(ts, acc, *refs):
    if acc:
        x_in, pos, t0, t1, t2, t3, x_out, xl_out = refs
    else:
        pos, t0, t1, t2, t3, x_out, xl_out = refs
    oh = jnp.where(pos[...] == _iota((pos.shape[0], 4 * C), 1), 1.0, 0.0).astype(BF16)
    for c in range(x_out.shape[1] // CB):
        s = slice(c * CB, (c + 1) * CB)
        tab = jnp.concatenate([t[:, s] for t in (t0, t1, t2, t3)], axis=0)
        tot = jnp.dot(oh, tab, preferred_element_type=F32)
        if acc:
            tot = tot + x_in[:, s].astype(F32)
        x_out[:, s] = tot.astype(BF16)
    t = 4 * ts
    for k in range(x_out.shape[0] // t):
        at = pl.multiple_of(k * t + _me() * ts, ts)
        xl_out[k] = x_out[pl.ds(at, ts), :]


def _expand(pos, tabs, ts, x=None):
    ntok, d = pos.shape[0], tabs[0].shape[1]
    ins = ([x] if x is not None else []) + [pos, *tabs]
    return pl.pallas_call(
        functools.partial(_expand_kernel, ts, x is not None),
        out_shape=(jax.ShapeDtypeStruct((ntok, d), BF16), jax.ShapeDtypeStruct((ntok // (4 * ts), ts, d), BF16)),
        in_specs=[_vm()] * len(ins),
        out_specs=(_vm(), _vm()),
        compiler_params=_params(12),
        cost_estimate=_cost(3),
        name="expand",
    )(*ins)


def _p_kernel(ts, du_ref, w_ref, *refs):
    outs, (de, dur, z, sems) = refs[:-4], refs[-4:]
    nk = du_ref.shape[0]

    @pl.when(pl.program_id(0) == 0)
    def _():
        z[...] = jnp.zeros_like(z)
        for k in range(nk):
            for r in range(4):
                at = pl.multiple_of((_me() ^ r) * ts, ts)
                dur[pl.ds((r * nk + k) * ts, ts), :] = du_ref[k, pl.ds(at, ts), :]
        _fill(z, de, sems, 0, 0, ZP, False)

    out = lax.dot_general(dur[...], w_ref[...], (((1,), (1,)), ((), ())), preferred_element_type=F32)
    for i, o in enumerate(outs):
        o[...] = out[i * nk * ts:(i + 1) * nk * ts].astype(BF16)

    @pl.when(pl.program_id(0) == pl.num_programs(0) - 1)
    def _():
        _fill(z, de, sems, 0, 0, ZP, True)


def _p_terms(du, W, ts, vs):
    nk, t, f = du.shape
    d = W.shape[0]
    cb = 3 * CB
    out = pl.pallas_call(
        functools.partial(_p_kernel, ts),
        out_shape=(jax.ShapeDtypeStruct((nk * ts, d), BF16),) * 4 + (jax.ShapeDtypeStruct((vs, d), F32),),
        grid=(d // cb,),
        in_specs=[pl.BlockSpec((nk, t, f), lambda i: (0, 0, 0)), pl.BlockSpec((cb, f), lambda i: (i, 0))],
        out_specs=(pl.BlockSpec((nk * ts, cb), lambda i: (0, i)),) * 4 + (_any(),),
        scratch_shapes=[VMEM((nk * t, f), BF16)] + _zscratch(d, ZP),
        compiler_params=_params(20),
        cost_estimate=_cost(5),
        name="p_terms",
    )(du, W)
    return out[:4], out[4]


def _zero_kernel(lo, n, de_in, o, z, sems):
    z[...] = jnp.zeros_like(z)
    _fill(z, o, sems, lo, 0, n, False)
    _fill(z, o, sems, lo, 0, n, True)


def _zeros(de, lo, n):
    vs, d = de.shape
    return pl.pallas_call(
        functools.partial(_zero_kernel, lo, n),
        out_shape=jax.ShapeDtypeStruct((vs, d), F32),
        in_specs=[_any()],
        out_specs=_any(),
        scratch_shapes=_zscratch(d, n),
        input_output_aliases={0: 0},
        compiler_params=_params(4),
        cost_estimate=_cost(n * 0.375),
    )(de)


def _dx_rows(x, p0, p1, p2, p3, dres, g, dx):
    rows = 32
    tot = None
    for b in range(dx.shape[0] // rows):
        s = slice(b * rows, (b + 1) * rows)
        xf = x[s].astype(F32)
        rs = lax.rsqrt(jnp.mean(xf * xf, axis=-1, keepdims=True) + EPS)
        nh = xf * rs
        dn = (p0[s].astype(F32) + p1[s].astype(F32)) + (p2[s].astype(F32) + p3[s].astype(F32))
        gdn = g[...].astype(F32) * dn
        out = dres[s].astype(F32) + rs * (gdn - nh * jnp.mean(nh * gdn, axis=-1, keepdims=True))
        dx[s] = out.astype(BF16)
        part = jnp.sum(dn * nh, axis=0, keepdims=True)
        tot = part if tot is None else tot + part
    return tot


def _dx_kernel(*refs):
    refs[-1][...] = _dx_rows(*refs[:-1])


def _dx(x, ps, dres, g):
    m, d = x.shape
    return pl.pallas_call(
        _dx_kernel,
        out_shape=(
            jax.ShapeDtypeStruct((m, d), BF16),
            jax.ShapeDtypeStruct((1, d), F32),
        ),
        in_specs=[_vm()] * 7,
        out_specs=(_vm(), _vm()),
        compiler_params=_params(12),
        cost_estimate=_cost(2),
        name="dx_form",
    )(x, *ps, dres, g)


def _dx_sums_kernel(x, p0, p1, p2, p3, dres, g, slot_ref, dx, mine, out, got, send, recv):
    sib = _me() ^ 1
    barrier = pltpu.get_barrier_semaphore()
    pl.semaphore_signal(barrier, inc=1, device_id={"tp": sib}, device_id_type=pl.DeviceIdType.MESH)
    dg = _dx_rows(x, p0, p1, p2, p3, dres, g, dx)
    j = _iota((C2, dx.shape[0]), 0)
    last = lax.broadcasted_iota(jnp.int32, (C2, CB), 0) == C2 - 1

    def sums(i, to):
        oh = jnp.where(slot_ref[i:i + 1, :] == j, 1.0, 0.0).astype(BF16)
        for c in range(to.shape[1] // CB):
            s = slice(c * CB, (c + 1) * CB)
            to[:, s] = jnp.where(last, dg[:, s], jnp.dot(oh, dx[:, s], preferred_element_type=F32))

    sums(3, out)
    pl.semaphore_wait(barrier, 1)
    copy = pltpu.make_async_remote_copy(
        src_ref=out, dst_ref=got, send_sem=send, recv_sem=recv,
        device_id={"tp": sib}, device_id_type=pl.DeviceIdType.MESH,
    )
    copy.start()
    sums(2, mine)
    copy.wait()
    mine[...] = mine[...] + got[...]


def _dx_sums(x, ps, dres, g, slots):
    m, d = x.shape
    return pl.pallas_call(
        _dx_sums_kernel,
        out_shape=(jax.ShapeDtypeStruct((m, d), BF16), jax.ShapeDtypeStruct((C2, d), F32)),
        in_specs=[_vm()] * 8,
        out_specs=(_vm(), _vm()),
        scratch_shapes=[VMEM((C2, d), F32), VMEM((C2, d), F32), pltpu.SemaphoreType.DMA, pltpu.SemaphoreType.DMA],
        compiler_params=pltpu.CompilerParams(vmem_limit_bytes=12 << 20, collective_id=0, has_side_effects=True),
        cost_estimate=_cost(3),
        name="dx_sums",
    )(x, *ps, dres, g, slots)


def _udw_kernel(per, vs, ntp, x_ref, g_ref, w_ref, du_ref, ids_ref, de_in, *refs):
    u_ref, dw_ref, *slot_refs, de, n, z, sems = refs
    i = pl.program_id(0)
    nk, t, f = du_ref.shape
    cb = dw_ref.shape[0]

    @pl.when(i == 0)
    def _():
        z[...] = jnp.zeros_like(z)
        _fill(z, de, sems, AT_U, 0, ZU, False)
        _slots(vs, ntp, ids_ref, *slot_refs)
        rows = 64
        for b in range(n.shape[0] // rows):
            s = slice(b * rows, (b + 1) * rows)
            xf = x_ref[s].astype(F32)
            rs = lax.rsqrt(jnp.mean(xf * xf, axis=-1, keepdims=True) + EPS)
            n[s] = (xf * rs * g_ref[...].astype(F32)).astype(BF16)
        for c in range(f // CB):
            s = slice(c * CB, (c + 1) * CB)
            out = jnp.dot(n[...], w_ref[:, s], preferred_element_type=F32).astype(BF16)
            for k in range(nk):
                u_ref[k, :, s] = out[k * t:(k + 1) * t]

    _fill(z, de, sems, AT_U, ZU + i * per, jnp.minimum(per, ZW - i * per), False)
    blk = n[:, pl.ds(pl.multiple_of(i * cb, 128), cb)]
    dw_ref[...] = lax.dot_general(
        blk, du_ref[...].reshape(nk * t, f), (((0,), (0,)), ((), ())), preferred_element_type=F32
    )

    @pl.when(i == pl.num_programs(0) - 1)
    def _():
        _fill(z, de, sems, AT_U, 0, ZU + ZW, True)


def _udw(x, g, W, du, ids, ntp, de):
    nk, t, f = du.shape
    ntok, d = x.shape
    cb = d // 6
    steps = d // cb
    return pl.pallas_call(
        functools.partial(_udw_kernel, -(-ZW // steps), de.shape[0], ntp),
        out_shape=(
            jax.ShapeDtypeStruct((nk, t, f), BF16),
            jax.ShapeDtypeStruct((d, f), F32),
            jax.ShapeDtypeStruct((1, ntok), F32),
            jax.ShapeDtypeStruct((1, ntok), jnp.int32),
            jax.ShapeDtypeStruct((1, 128), jnp.int32),
            jax.ShapeDtypeStruct((4, ntok // ntp), F32),
            jax.ShapeDtypeStruct((1, 256), jnp.int32),
            jax.ShapeDtypeStruct(de.shape, F32),
        ),
        grid=(steps,),
        in_specs=[_vm()] * 5 + [_any()],
        out_specs=(
            pl.BlockSpec((nk, t, f), lambda i: (0, 0, 0)), pl.BlockSpec((cb, f), lambda i: (i, 0)),
            *[_vm()] * 5, _any(),
        ),
        scratch_shapes=[VMEM((ntok, d), BF16)] + _zscratch(d, ZU + ZW),
        input_output_aliases={5: 7},
        compiler_params=_params(20),
        cost_estimate=_cost(20),
        name="u_dw",
    )(x, g, W, du, ids, de)


def _scatter_kernel(ts, nk, cnt_ref, list_ref, srow_ref, *refs):
    pieces, (de_in, de, dx, acc, sem) = refs[:-5], refs[-5:]
    ntok = nk * 4 * ts
    for k in range(nk):
        for r in range(4):
            at = pl.multiple_of(k * 4 * ts + (_me() ^ r) * ts, ts)
            dx[pl.ds(at, ts), :] = pieces[r][k * ts:(k + 1) * ts, :]
    cnt = cnt_ref[0, 1]

    def chunk(i, carry):
        base = i * C
        slot = (lax.broadcasted_iota(jnp.int32, (C, ntok), 0) + base).astype(F32)
        oh = jnp.where(slot == srow_ref[...], 1.0, 0.0).astype(BF16)
        for c in range(acc.shape[1] // CB):
            s = slice(c * CB, (c + 1) * CB)
            acc[:, s] = jnp.dot(oh, dx[:, s], preferred_element_type=F32)
        here = jnp.minimum(cnt - base, C)

        def put(j, c2):
            row = list_ref[0, base + j]
            pltpu.make_async_copy(acc.at[pl.ds(j, 1)], de.at[pl.ds(row, 1)], sem).start()
            return c2

        def done(j, c2):
            pltpu.make_async_copy(acc.at[pl.ds(j, 1)], de.at[pl.ds(0, 1)], sem).wait()
            return c2

        lax.fori_loop(0, here, put, 0)
        lax.fori_loop(0, here, done, 0)
        return carry

    lax.fori_loop(0, (cnt + C - 1) // C, chunk, 0)


def _scatter(cnts, rows, srow, pieces, de, ts, nk):
    vs, d = de.shape
    ntok = srow.shape[1]
    return pl.pallas_call(
        functools.partial(_scatter_kernel, ts, nk),
        out_shape=jax.ShapeDtypeStruct((vs, d), F32),
        in_specs=[_sm(), _sm(), _vm()] + [_vm()] * len(pieces) + [_any()],
        out_specs=_any(),
        scratch_shapes=[VMEM((ntok, d), BF16), VMEM((C, d), F32), pltpu.SemaphoreType.DMA],
        input_output_aliases={3 + len(pieces): 0},
        compiler_params=_params(16),
        cost_estimate=_cost(3),
        name="scatter_rows",
    )(cnts, rows, srow, *pieces, de)


def _acc_kernel(lo, n, cnt_ref, oth_ref, slot_ref, dx0, dx1, de_in, de, acc, flag, z, sems):
    z[...] = jnp.zeros_like(z)
    _fill(z, de, sems, lo, 0, n, False)
    for i in (0, 2):
        flag[0, i] = jnp.maximum(cnt_ref[0, i], oth_ref[0, i])
    m = dx0.shape[0]
    j = _iota((C, m), 0)
    ohs = [jnp.where(slot_ref[i:i + 1, :] == j, 1.0, 0.0).astype(BF16) for i in (0, 1)]
    for c in range(acc.shape[1] // CB):
        s = slice(c * CB, (c + 1) * CB)
        tot = jnp.dot(ohs[0], dx0[:, s], preferred_element_type=F32)
        acc[:, s] = tot + jnp.dot(ohs[1], dx1[:, s], preferred_element_type=F32)
    _fill(z, de, sems, lo, 0, n, True)


def _acc(cnts, other, slots, dx0, dx1, de, lo):
    vs, d = de.shape
    n = vs // ZR - lo
    return pl.pallas_call(
        functools.partial(_acc_kernel, lo, n),
        out_shape=(
            jax.ShapeDtypeStruct((vs, d), F32),
            jax.ShapeDtypeStruct((C, d), F32),
            jax.ShapeDtypeStruct((1, 4), jnp.int32),
        ),
        in_specs=[_sm(), _sm()] + [_vm()] * 3 + [_any()],
        out_specs=(_any(), _vm(), _sm()),
        scratch_shapes=_zscratch(d, n),
        input_output_aliases={5: 0},
        compiler_params=_params(8),
        cost_estimate=_cost(n * 0.375),
        name="fill_acc",
    )(cnts, other, slots, dx0, dx1, de)


def _write_kernel(map_ref, acc_in, mine_ref, got_ref, de_in, de, dg_out, acc, sem):
    acc[...] = acc_in[...]

    def add(j, carry):
        at = pl.ds(map_ref[0, j], 1)
        acc[at, :] = acc[at, :] + got_ref[pl.ds(j, 1), :]
        return carry

    lax.fori_loop(0, jnp.minimum(map_ref[0, 127], C2 - 1), add, 0)
    n = jnp.minimum(map_ref[0, 255], C)

    def put(j, carry):
        pltpu.make_async_copy(acc.at[pl.ds(j, 1)], de.at[pl.ds(map_ref[0, 128 + j], 1)], sem).start()
        return carry

    def done(j, carry):
        pltpu.make_async_copy(acc.at[pl.ds(j, 1)], de.at[pl.ds(0, 1)], sem).wait()
        return carry

    lax.fori_loop(0, n, put, 0)
    dg = mine_ref[C2 - 1:C2, :] + got_ref[C2 - 1:C2, :]
    dg_out[...] = dg.reshape(dg_out.shape)
    lax.fori_loop(0, n, done, 0)


def _write(where, acc, mine, got, de):
    vs, d = de.shape
    return pl.pallas_call(
        _write_kernel,
        out_shape=(jax.ShapeDtypeStruct((vs, d), F32), jax.ShapeDtypeStruct((d,), F32)),
        in_specs=[_sm()] + [_vm()] * 3 + [_any()],
        out_specs=(_any(), _vm()),
        scratch_shapes=[VMEM((C, d), F32), pltpu.SemaphoreType.DMA],
        input_output_aliases={4: 0},
        compiler_params=_params(6),
        cost_estimate=_cost(3),
        name="write_rows",
    )(where, acc, mine, got, de)


def solution(mesh):
    ntp = mesh.shape["tp"]
    ndp = mesh.shape["dp"]

    def swap(a, bit):
        return lax.ppermute(a, "tp", [(i, i ^ bit) for i in range(ntp)])

    def share(t):
        t2 = swap(t, 2)
        t1 = swap(t, 1)
        return t, t1, t2, swap(t2, 1)

    def p_terms(du, W, ts, vs):
        q, de = _p_terms(du, W, ts, vs)
        return de, (q[0], swap(q[1], 1), swap(q[2], 2), swap(q[3], 3))

    def body(ids, E, g, W, du, dres):
        vs, d = E.shape
        nk, t = ids.shape
        ts = t // ntp
        m = nk * ts
        g2 = g.reshape(1, d)

        tabs = share(_index_call(None, ids, E, ntp))
        de, ps = p_terms(du, W, ts, vs)
        pos, de = _pos(jnp.int32(0), ids, ntp, de)
        x, xl = _expand(pos, tabs, ts)
        u, dW, _, _, cnts, slots, where, de = _udw(x, g2, W, du, ids, ntp, de)
        dx, mine = _dx_sums(xl.reshape(m, d), ps, dres.reshape(m, d), g2, slots)
        got = swap(mine, 2)
        dx1 = swap(dx, 1)
        de = _zeros(de, AT_B, ZB)
        other = lax.ppermute(cnts, "dp", [(i, (i + 1) % ndp) for i in range(ndp)])
        de, acc, flags = _acc(cnts, other, slots, dx, dx1, de, AT_R)
        dE, dg = _write(where, acc, mine, got, de)
        outs = u, xl, dE, dW, dg

        inputs = ids, E, W, du, dres, g2, flags

        def again(c):
            ids, E, W, du, dres, g2, fl, left = lax.optimization_barrier((*inputs, c[0]))
            rounds = fl[0, 0]
            i0 = left - left

            def more(q):
                i, x, _, de = q
                pos, de = _pos(i, ids, ntp, de)
                return i + 1, *_expand(pos, share(_index_call(i, ids, E, ntp)), ts, x), de

            zeros = jnp.zeros((nk * t, d), BF16), jnp.zeros((nk, ts, d), BF16)
            de, ps = p_terms(du, W, ts, vs)
            _, x, xl, de = lax.while_loop(lambda q: q[0] < rounds, more, (i0, *zeros, de))
            u, dW, srow, rows, cs, _, _, de = _udw(x, g2, W, du, ids, ntp, de)
            dx, dg = _dx(xl.reshape(m, d), ps, dres.reshape(m, d), g2)
            dg2 = dg + swap(dg, 1)
            dg = (dg2 + swap(dg2, 2)).reshape(d)
            dE = _scatter(cs, rows, srow, share(dx), _zeros(de, AT_B, vs // ZR - AT_B), ts, nk)
            return i0, (u, xl, dE, dW, dg)

        _, outs = lax.while_loop(lambda c: c[0] > 0, again, (jnp.minimum(flags[0, 2], 1), outs))
        return outs

    return jax.shard_map(
        body,
        mesh=mesh,
        in_specs=(P("dp", None), P("tp", None), P(None), P(None, "tp"), P("dp", None, "tp"), P("dp", "tp", None)),
        out_specs=(P("dp", None, "tp"), P("dp", "tp", None), P(("dp", "tp"), None), P("dp", "tp"), P("dp")),
        check_vma=False,
    )
```

```python
import functools

import jax
import jax.numpy as jnp
from jax import lax
from jax.experimental import pallas as pl
from jax.experimental.pallas import tpu as pltpu
from jax.sharding import PartitionSpec as P


EPS = 1e-6
C = 56
G = 2
C2 = 32
CB = 256
ZR = 128
ZP, ZA, ZU, ZW, ZB = 8, 4, 22, 17, 4
AT_A, AT_U, AT_B, AT_R = ZP, ZP + ZA, ZP + ZA + ZU + ZW, ZP + ZA + ZU + ZW + ZB
TB = 64

F32 = jnp.float32
BF16 = jnp.bfloat16
VMEM = pltpu.VMEM


def _sm():
    return pl.BlockSpec(memory_space=pltpu.SMEM)


def _vm():
    return pl.BlockSpec(memory_space=pltpu.VMEM)


def _any():
    return pl.BlockSpec(memory_space=pl.ANY)


def _params(mb):
    return pltpu.CompilerParams(vmem_limit_bytes=mb << 20)


def _cost(us):
    return pl.CostEstimate(flops=int(us * 4_000_000_000), bytes_accessed=1_000_000, transcendentals=0)


def _iota(shape, dim):
    return lax.broadcasted_iota(jnp.int32, shape, dim).astype(F32)


def _me():
    return lax.axis_index("tp").astype(jnp.int32)


def _fill(z, o, sems, lo, first, n, wait):
    def step(i, carry):
        at = pl.multiple_of((lo + i) * ZR, ZR)
        c = pltpu.make_async_copy(z, o.at[pl.ds(at, ZR)], sems.at[i])
        c.wait() if wait else c.start()
        return carry

    lax.fori_loop(first, first + n, step, 0)


def _zscratch(d, n):
    return [VMEM((ZR, d), F32), pltpu.SemaphoreType.DMA((n,))]


def _column(row, b):
    w = (b * TB) // 128 * 128
    part = jnp.broadcast_to(row[:, w:w + 128], (TB, 128))
    hit = _iota((TB, 128), 1) == _iota((TB, 128), 0) + float(b * TB - w)
    return jnp.sum(jnp.where(hit, part, 0.0), axis=1, keepdims=True)


def _fold(a):
    return sum(a[8 * q:8 * q + 8] for q in range(1, TB // 8)) + a[:8]


def _ids_row(ids_ref):
    idsf = ids_ref[...].astype(F32)
    return jnp.concatenate([idsf[k:k + 1] for k in range(ids_ref.shape[0])], axis=1)


def _ranks(idr, idcs, vs, ntp, masks):
    ntok = idr.shape[1]
    lane = _iota((TB, ntok), 1)
    thr = _iota((TB, 128), 1) * float(vs)
    rank8 = jnp.zeros((8, ntok), F32)
    below8 = [jnp.zeros((8, 128), F32) for _ in masks]
    for b, idc in enumerate(idcs):
        i = [i for i, (_, blocks) in enumerate(masks) if blocks[b]][0]
        mask = masks[i][0]
        dup = (jnp.broadcast_to(idc, (TB, ntok)) == idr) & (lane < _iota((TB, ntok), 0) + float(b * TB))
        seen = jnp.max(jnp.where(dup, mask, 0.0), axis=1, keepdims=True)
        key = jnp.where(seen > 0.5, float(vs * ntp), idc)
        rank8 = rank8 + _fold(jnp.where(jnp.broadcast_to(key, (TB, ntok)) < idr, mask, 0.0))
        below8[i] = below8[i] + _fold(jnp.where(jnp.broadcast_to(key, (TB, 128)) < thr, 1.0, 0.0))
    return jnp.sum(rank8, axis=0, keepdims=True), [jnp.sum(b8, axis=0, keepdims=True) for b8 in below8]


def _table_slots(idr, idcs, vs, ntp):
    rank, (below,) = _ranks(idr, idcs, vs, ntp, [(jnp.ones_like(idr), [True] * len(idcs))])
    own_r = jnp.floor(idr * (1.0 / vs))
    start = jnp.zeros_like(rank)
    for d in range(ntp):
        start = jnp.where(own_r == float(d), below[:, d:d + 1], start)
    return own_r, rank - start, below


def _index_kernel(vs, ntp, first, *refs):
    if first:
        ids_ref, e_ref, tab_ref, buf, glv, gls, gsem, sem = refs
        base = 0.0
    else:
        c_ref, ids_ref, e_ref, tab_ref, buf, glv, gls, gsem, sem = refs
        base = (c_ref[0] * C).astype(F32)
    me = _me().astype(F32)
    lo = me * vs
    idr = _ids_row(ids_ref)
    ntok = idr.shape[1]
    idcs = [_column(idr, b) for b in range(ntok // TB)]
    own_r, slot_r, _ = _table_slots(idr, idcs, vs, ntp)
    my_r = jnp.where(own_r == me, slot_r, -1.0)
    slot_l = _iota((TB, 128), 1) + base
    acc = jnp.zeros((TB, 128), F32)
    for b, idc in enumerate(idcs):
        acc = jnp.maximum(acc, jnp.where(_column(my_r, b) == slot_l, idc - lo, 0.0))
    glv[...] = jnp.broadcast_to(jnp.max(acc, axis=0, keepdims=True), (8, 128)).astype(jnp.int32)
    cp = pltpu.make_async_copy(glv, gls, gsem)
    cp.start()
    cp.wait()

    def fetch(j, carry):
        g = pl.multiple_of((gls[0, j] >> 1) << 1, G)
        at = pl.multiple_of(j * G, G)
        pltpu.make_async_copy(e_ref.at[pl.ds(g, G)], buf.at[pl.ds(at, G)], sem).start()
        return carry

    lax.fori_loop(0, C, fetch, 0, unroll=8)
    hit = jnp.where(my_r == _iota((C, ntok), 0) + base, idr - lo, 0.0)
    want = jnp.max(hit, axis=1, keepdims=True)
    want = want - jnp.floor(want * (1.0 / G)) * G + _iota((C, 1), 0) * G
    sel = jnp.where(_iota((C, C * G), 1) == want, 1.0, 0.0).astype(BF16)
    pltpu.make_async_copy(e_ref.at[pl.ds(0, C * G)], buf, sem).wait()
    tab_ref[...] = jnp.dot(sel, buf[...], preferred_element_type=F32).astype(BF16)


def _index_call(chunk, ids, E, ntp):
    vs, d = E.shape
    first = chunk is None
    return pl.pallas_call(
        functools.partial(_index_kernel, vs, ntp, first),
        out_shape=jax.ShapeDtypeStruct((C, d), BF16),
        in_specs=([] if first else [_sm()]) + [_vm(), pl.BlockSpec(memory_space=pltpu.HBM)],
        out_specs=_vm(),
        scratch_shapes=[
            VMEM((C * G, d), BF16),
            VMEM((8, 128), jnp.int32),
            pltpu.SMEM((8, 128), jnp.int32),
            pltpu.SemaphoreType.DMA,
            pltpu.SemaphoreType.DMA,
        ],
        compiler_params=_params(8),
        cost_estimate=_cost(12),
        name="index_gather",
    )(*([] if first else [chunk.reshape(1)]), ids, E)


def _pos_kernel(vs, ntp, c_ref, ids_ref, de_in, pos_ref, de, z, sems):
    z[...] = jnp.zeros_like(z)
    _fill(z, de, sems, AT_A, 0, ZA, False)
    base = (c_ref[0] * C).astype(F32)
    idr = _ids_row(ids_ref)
    nb = idr.shape[1] // TB
    own_r, slot_r, _ = _table_slots(idr, [_column(idr, b) for b in range(nb)], vs, ntp)
    rel = (own_r.astype(jnp.int32) ^ _me()).astype(F32)
    pos = jnp.where((slot_r >= base) & (slot_r < base + C), rel * C + slot_r - base, -1.0)
    for b in range(nb):
        pos_ref[b * TB:(b + 1) * TB, :] = _column(pos, b)
    _fill(z, de, sems, AT_A, 0, ZA, True)


def _pos(chunk, ids, ntp, de):
    vs, d = de.shape
    ntok = ids.shape[0] * ids.shape[1]
    return pl.pallas_call(
        functools.partial(_pos_kernel, vs, ntp),
        out_shape=(jax.ShapeDtypeStruct((ntok, 1), F32), jax.ShapeDtypeStruct(de.shape, F32)),
        in_specs=[_sm(), _vm(), _any()],
        out_specs=(_vm(), _any()),
        scratch_shapes=_zscratch(d, ZA),
        input_output_aliases={2: 1},
        compiler_params=_params(6),
        cost_estimate=_cost(3),
        name="positions",
    )(chunk.reshape(1), ids, de)


def _slots(vs, ntp, ids_ref, srow_ref, list_ref, cnt_ref, slot_ref, map_ref):
    mei = _me()
    me = mei.astype(F32)
    lo = me * vs
    nk, t = ids_ref.shape
    ntok = nk * t
    nb = ntok // TB
    ts = t // ntp
    idr = _ids_row(ids_ref)
    idcs = [_column(idr, b) for b in range(nb)]
    own_r, slot_r, below = _table_slots(idr, idcs, vs, ntp)
    my_r = jnp.where(own_r == me, slot_r, -1.0)
    cnt = jnp.zeros((1, 1), F32)
    mx = jnp.zeros((1, 1), F32)
    for d in range(ntp):
        nd = below[:, d + 1:d + 2] - below[:, d:d + 1]
        cnt = jnp.where(me == float(d), nd, cnt)
        mx = jnp.maximum(mx, nd)
    srow_ref[...] = my_r

    part = lax.broadcasted_iota(jnp.int32, (1, ntok), 1) // ts % ntp
    chips = [
        (jnp.where(part // 2 == c, 1.0, 0.0), [b * TB // ts % ntp // 2 == c for b in range(nb)])
        for c in range(ntp // 2)
    ]
    rank2, below2 = _ranks(idr, idcs, vs, ntp, chips)
    start2 = jnp.zeros_like(rank2)
    cnt2 = jnp.zeros((1, 1), F32)
    mx2 = jnp.zeros((1, 1), F32)
    for c, (chip, _) in enumerate(chips):
        for d in range(ntp):
            ld = below2[c][:, d:d + 1]
            nd = below2[c][:, d + 1:d + 2] - ld
            start2 = jnp.where((own_r == float(d)) & (chip > 0.5), ld, start2)
            if d // 2 != c:
                cnt2 = jnp.where(me == float(d), nd, cnt2)
                mx2 = jnp.maximum(mx2, nd)
    slot2_r = rank2 - start2
    lane1 = lax.broadcasted_iota(jnp.int32, (1, 128), 1)
    over = jnp.where((mx > C) | (mx2 > C2 - 1), 1.0, 0.0)
    rounds = jnp.floor((mx + C - 1.0) * (1.0 / C))
    cnts = jnp.where(lane1 == 0, rounds, jnp.where(lane1 == 1, cnt, jnp.where(lane1 == 2, over, cnt2)))
    cnt_ref[...] = cnts.astype(jnp.int32)
    sums_r = [jnp.where(own_r == (mei ^ o).astype(F32), slot2_r, -1.0) for o in (2, 3)]
    rows = [jnp.zeros((1, nk * ts), F32)] * 4
    for q in range(ntp):
        at = [slice(k * t + q * ts, k * t + (q + 1) * ts) for k in range(nk)]
        mine = jnp.concatenate([my_r[:, w] for w in at], axis=1)
        sums = [jnp.concatenate([r[:, w] for w in at], axis=1) for r in sums_r]
        own, sib = me == float(q), me == float(q ^ 1)
        rows = [
            jnp.where(own, mine, rows[0]), jnp.where(sib, mine, rows[1]),
            jnp.where(own, sums[0], rows[2]), jnp.where(own, sums[1], rows[3]),
        ]
    for j, r in enumerate(rows):
        slot_ref[j:j + 1, :] = r
    far = (part // 2).astype(F32) != jnp.floor(me * 0.5)
    got_r = jnp.where(far & (own_r == me), slot2_r, -1.0)
    acc2 = jnp.zeros((TB, 128), F32)
    slot_j = _iota((TB, 128), 1)
    full = jnp.zeros((8, ntok), F32)
    lane8 = _iota((8, ntok), 1)
    for b in range(nb):
        my_c = _column(my_r, b)
        acc2 = jnp.maximum(acc2, jnp.where(_column(got_r, b) == slot_j, my_c, 0.0))
        for q in range(TB // 8):
            s = slice(8 * q, 8 * q + 8)
            full = jnp.maximum(full, jnp.where(my_c[s] == lane8, idcs[b][s] - lo, 0.0))
    full = jnp.max(full, axis=0, keepdims=True)
    list_ref[...] = full.astype(jnp.int32)
    slots = jnp.minimum(jnp.max(acc2, axis=0, keepdims=True), C - 1.0)
    many = jnp.where(lane1 == 127, cnt2, slots)
    mine = jnp.where(lane1 == 127, cnt, full[:, :128])
    map_ref[...] = jnp.concatenate([many, mine], axis=1).astype(jnp.int32)


def _expand_kernel(ts, acc, *refs):
    if acc:
        x_in, pos, t0, t1, t2, t3, x_out, xl_out = refs
    else:
        pos, t0, t1, t2, t3, x_out, xl_out = refs
    oh = jnp.where(pos[...] == _iota((pos.shape[0], 4 * C), 1), 1.0, 0.0).astype(BF16)
    for c in range(x_out.shape[1] // CB):
        s = slice(c * CB, (c + 1) * CB)
        tab = jnp.concatenate([t[:, s] for t in (t0, t1, t2, t3)], axis=0)
        tot = jnp.dot(oh, tab, preferred_element_type=F32)
        if acc:
            tot = tot + x_in[:, s].astype(F32)
        x_out[:, s] = tot.astype(BF16)
    t = 4 * ts
    for k in range(x_out.shape[0] // t):
        at = pl.multiple_of(k * t + _me() * ts, ts)
        xl_out[k] = x_out[pl.ds(at, ts), :]


def _expand(pos, tabs, ts, x=None):
    ntok, d = pos.shape[0], tabs[0].shape[1]
    ins = ([x] if x is not None else []) + [pos, *tabs]
    return pl.pallas_call(
        functools.partial(_expand_kernel, ts, x is not None),
        out_shape=(jax.ShapeDtypeStruct((ntok, d), BF16), jax.ShapeDtypeStruct((ntok // (4 * ts), ts, d), BF16)),
        in_specs=[_vm()] * len(ins),
        out_specs=(_vm(), _vm()),
        compiler_params=_params(12),
        cost_estimate=_cost(3),
        name="expand",
    )(*ins)


def _p_kernel(ts, du_ref, w_ref, *refs):
    outs, (de, dur, z, sems) = refs[:-4], refs[-4:]
    nk = du_ref.shape[0]

    @pl.when(pl.program_id(0) == 0)
    def _():
        z[...] = jnp.zeros_like(z)
        for k in range(nk):
            for r in range(4):
                at = pl.multiple_of((_me() ^ r) * ts, ts)
                dur[pl.ds((r * nk + k) * ts, ts), :] = du_ref[k, pl.ds(at, ts), :]
        _fill(z, de, sems, 0, 0, ZP, False)

    out = lax.dot_general(dur[...], w_ref[...], (((1,), (1,)), ((), ())), preferred_element_type=F32)
    for i, o in enumerate(outs):
        o[...] = out[i * nk * ts:(i + 1) * nk * ts].astype(BF16)

    @pl.when(pl.program_id(0) == pl.num_programs(0) - 1)
    def _():
        _fill(z, de, sems, 0, 0, ZP, True)


def _p_terms(du, W, ts, vs):
    nk, t, f = du.shape
    d = W.shape[0]
    cb = 3 * CB
    out = pl.pallas_call(
        functools.partial(_p_kernel, ts),
        out_shape=(jax.ShapeDtypeStruct((nk * ts, d), BF16),) * 4 + (jax.ShapeDtypeStruct((vs, d), F32),),
        grid=(d // cb,),
        in_specs=[pl.BlockSpec((nk, t, f), lambda i: (0, 0, 0)), pl.BlockSpec((cb, f), lambda i: (i, 0))],
        out_specs=(pl.BlockSpec((nk * ts, cb), lambda i: (0, i)),) * 4 + (_any(),),
        scratch_shapes=[VMEM((nk * t, f), BF16)] + _zscratch(d, ZP),
        compiler_params=_params(20),
        cost_estimate=_cost(5),
        name="p_terms",
    )(du, W)
    return out[:4], out[4]


def _zero_kernel(lo, n, de_in, o, z, sems):
    z[...] = jnp.zeros_like(z)
    _fill(z, o, sems, lo, 0, n, False)
    _fill(z, o, sems, lo, 0, n, True)


def _zeros(de, lo, n):
    vs, d = de.shape
    return pl.pallas_call(
        functools.partial(_zero_kernel, lo, n),
        out_shape=jax.ShapeDtypeStruct((vs, d), F32),
        in_specs=[_any()],
        out_specs=_any(),
        scratch_shapes=_zscratch(d, n),
        input_output_aliases={0: 0},
        compiler_params=_params(4),
        cost_estimate=_cost(n * 0.375),
    )(de)


def _dx_rows(x, p0, p1, p2, p3, dres, g, dx):
    rows = 32
    tot = None
    for b in range(dx.shape[0] // rows):
        s = slice(b * rows, (b + 1) * rows)
        xf = x[s].astype(F32)
        rs = lax.rsqrt(jnp.mean(xf * xf, axis=-1, keepdims=True) + EPS)
        nh = xf * rs
        dn = (p0[s].astype(F32) + p1[s].astype(F32)) + (p2[s].astype(F32) + p3[s].astype(F32))
        gdn = g[...].astype(F32) * dn
        out = dres[s].astype(F32) + rs * (gdn - nh * jnp.mean(nh * gdn, axis=-1, keepdims=True))
        dx[s] = out.astype(BF16)
        part = jnp.sum(dn * nh, axis=0, keepdims=True)
        tot = part if tot is None else tot + part
    return tot


def _dx_kernel(*refs):
    refs[-1][...] = _dx_rows(*refs[:-1])


def _dx(x, ps, dres, g):
    m, d = x.shape
    return pl.pallas_call(
        _dx_kernel,
        out_shape=(
            jax.ShapeDtypeStruct((m, d), BF16),
            jax.ShapeDtypeStruct((1, d), F32),
        ),
        in_specs=[_vm()] * 7,
        out_specs=(_vm(), _vm()),
        compiler_params=_params(12),
        cost_estimate=_cost(2),
        name="dx_form",
    )(x, *ps, dres, g)


def _dx_sums_kernel(x, p0, p1, p2, p3, dres, g, slot_ref, dx, mine, out, got, send, recv):
    sib = _me() ^ 1
    barrier = pltpu.get_barrier_semaphore()
    pl.semaphore_signal(barrier, inc=1, device_id={"tp": sib}, device_id_type=pl.DeviceIdType.MESH)
    dg = _dx_rows(x, p0, p1, p2, p3, dres, g, dx)
    j = _iota((C2, dx.shape[0]), 0)
    last = lax.broadcasted_iota(jnp.int32, (C2, CB), 0) == C2 - 1

    def sums(i, to):
        oh = jnp.where(slot_ref[i:i + 1, :] == j, 1.0, 0.0).astype(BF16)
        for c in range(to.shape[1] // CB):
            s = slice(c * CB, (c + 1) * CB)
            to[:, s] = jnp.where(last, dg[:, s], jnp.dot(oh, dx[:, s], preferred_element_type=F32))

    sums(3, out)
    pl.semaphore_wait(barrier, 1)
    copy = pltpu.make_async_remote_copy(
        src_ref=out, dst_ref=got, send_sem=send, recv_sem=recv,
        device_id={"tp": sib}, device_id_type=pl.DeviceIdType.MESH,
    )
    copy.start()
    sums(2, mine)
    copy.wait()
    mine[...] = mine[...] + got[...]


def _dx_sums(x, ps, dres, g, slots):
    m, d = x.shape
    return pl.pallas_call(
        _dx_sums_kernel,
        out_shape=(jax.ShapeDtypeStruct((m, d), BF16), jax.ShapeDtypeStruct((C2, d), F32)),
        in_specs=[_vm()] * 8,
        out_specs=(_vm(), _vm()),
        scratch_shapes=[VMEM((C2, d), F32), VMEM((C2, d), F32), pltpu.SemaphoreType.DMA, pltpu.SemaphoreType.DMA],
        compiler_params=pltpu.CompilerParams(vmem_limit_bytes=12 << 20, collective_id=0, has_side_effects=True),
        cost_estimate=_cost(3),
        name="dx_sums",
    )(x, *ps, dres, g, slots)


def _udw_kernel(per, vs, ntp, x_ref, g_ref, w_ref, du_ref, ids_ref, de_in, *refs):
    u_ref, dw_ref, *slot_refs, de, n, z, sems = refs
    i = pl.program_id(0)
    nk, t, f = du_ref.shape
    cb = dw_ref.shape[0]

    @pl.when(i == 0)
    def _():
        z[...] = jnp.zeros_like(z)
        _fill(z, de, sems, AT_U, 0, ZU, False)
        _slots(vs, ntp, ids_ref, *slot_refs)
        rows = 64
        for b in range(n.shape[0] // rows):
            s = slice(b * rows, (b + 1) * rows)
            xf = x_ref[s].astype(F32)
            rs = lax.rsqrt(jnp.mean(xf * xf, axis=-1, keepdims=True) + EPS)
            n[s] = (xf * rs * g_ref[...].astype(F32)).astype(BF16)
        for c in range(f // CB):
            s = slice(c * CB, (c + 1) * CB)
            out = jnp.dot(n[...], w_ref[:, s], preferred_element_type=F32).astype(BF16)
            for k in range(nk):
                u_ref[k, :, s] = out[k * t:(k + 1) * t]

    _fill(z, de, sems, AT_U, ZU + i * per, jnp.minimum(per, ZW - i * per), False)
    blk = n[:, pl.ds(pl.multiple_of(i * cb, 128), cb)]
    dw_ref[...] = lax.dot_general(
        blk, du_ref[...].reshape(nk * t, f), (((0,), (0,)), ((), ())), preferred_element_type=F32
    )

    @pl.when(i == pl.num_programs(0) - 1)
    def _():
        _fill(z, de, sems, AT_U, 0, ZU + ZW, True)


def _udw(x, g, W, du, ids, ntp, de):
    nk, t, f = du.shape
    ntok, d = x.shape
    cb = d // 6
    steps = d // cb
    return pl.pallas_call(
        functools.partial(_udw_kernel, -(-ZW // steps), de.shape[0], ntp),
        out_shape=(
            jax.ShapeDtypeStruct((nk, t, f), BF16),
            jax.ShapeDtypeStruct((d, f), F32),
            jax.ShapeDtypeStruct((1, ntok), F32),
            jax.ShapeDtypeStruct((1, ntok), jnp.int32),
            jax.ShapeDtypeStruct((1, 128), jnp.int32),
            jax.ShapeDtypeStruct((4, ntok // ntp), F32),
            jax.ShapeDtypeStruct((1, 256), jnp.int32),
            jax.ShapeDtypeStruct(de.shape, F32),
        ),
        grid=(steps,),
        in_specs=[_vm()] * 5 + [_any()],
        out_specs=(
            pl.BlockSpec((nk, t, f), lambda i: (0, 0, 0)), pl.BlockSpec((cb, f), lambda i: (i, 0)),
            *[_vm()] * 5, _any(),
        ),
        scratch_shapes=[VMEM((ntok, d), BF16)] + _zscratch(d, ZU + ZW),
        input_output_aliases={5: 7},
        compiler_params=_params(20),
        cost_estimate=_cost(20),
        name="u_dw",
    )(x, g, W, du, ids, de)


def _scatter_kernel(ts, nk, cnt_ref, list_ref, srow_ref, *refs):
    pieces, (de_in, de, dx, acc, sem) = refs[:-5], refs[-5:]
    ntok = nk * 4 * ts
    for k in range(nk):
        for r in range(4):
            at = pl.multiple_of(k * 4 * ts + (_me() ^ r) * ts, ts)
            dx[pl.ds(at, ts), :] = pieces[r][k * ts:(k + 1) * ts, :]
    cnt = cnt_ref[0, 1]

    def chunk(i, carry):
        base = i * C
        slot = (lax.broadcasted_iota(jnp.int32, (C, ntok), 0) + base).astype(F32)
        oh = jnp.where(slot == srow_ref[...], 1.0, 0.0).astype(BF16)
        for c in range(acc.shape[1] // CB):
            s = slice(c * CB, (c + 1) * CB)
            acc[:, s] = jnp.dot(oh, dx[:, s], preferred_element_type=F32)
        here = jnp.minimum(cnt - base, C)

        def put(j, c2):
            row = list_ref[0, base + j]
            pltpu.make_async_copy(acc.at[pl.ds(j, 1)], de.at[pl.ds(row, 1)], sem).start()
            return c2

        def done(j, c2):
            pltpu.make_async_copy(acc.at[pl.ds(j, 1)], de.at[pl.ds(0, 1)], sem).wait()
            return c2

        lax.fori_loop(0, here, put, 0)
        lax.fori_loop(0, here, done, 0)
        return carry

    lax.fori_loop(0, (cnt + C - 1) // C, chunk, 0)


def _scatter(cnts, rows, srow, pieces, de, ts, nk):
    vs, d = de.shape
    ntok = srow.shape[1]
    return pl.pallas_call(
        functools.partial(_scatter_kernel, ts, nk),
        out_shape=jax.ShapeDtypeStruct((vs, d), F32),
        in_specs=[_sm(), _sm(), _vm()] + [_vm()] * len(pieces) + [_any()],
        out_specs=_any(),
        scratch_shapes=[VMEM((ntok, d), BF16), VMEM((C, d), F32), pltpu.SemaphoreType.DMA],
        input_output_aliases={3 + len(pieces): 0},
        compiler_params=_params(16),
        cost_estimate=_cost(3),
        name="scatter_rows",
    )(cnts, rows, srow, *pieces, de)


def _acc_kernel(lo, n, cnt_ref, oth_ref, slot_ref, dx0, dx1, de_in, de, acc, rounds, over, z, sems):
    z[...] = jnp.zeros_like(z)
    _fill(z, de, sems, lo, 0, n, False)
    rounds[0] = jnp.maximum(cnt_ref[0, 0], oth_ref[0, 0])
    over[0] = jnp.maximum(cnt_ref[0, 2], oth_ref[0, 2])
    m = dx0.shape[0]
    j = _iota((C, m), 0)
    ohs = [jnp.where(slot_ref[i:i + 1, :] == j, 1.0, 0.0).astype(BF16) for i in (0, 1)]
    for c in range(acc.shape[1] // CB):
        s = slice(c * CB, (c + 1) * CB)
        tot = jnp.dot(ohs[0], dx0[:, s], preferred_element_type=F32)
        acc[:, s] = tot + jnp.dot(ohs[1], dx1[:, s], preferred_element_type=F32)
    _fill(z, de, sems, lo, 0, n, True)


def _acc(cnts, other, slots, dx0, dx1, de, lo):
    vs, d = de.shape
    n = vs // ZR - lo
    return pl.pallas_call(
        functools.partial(_acc_kernel, lo, n),
        out_shape=(
            jax.ShapeDtypeStruct((vs, d), F32),
            jax.ShapeDtypeStruct((C, d), F32),
            jax.ShapeDtypeStruct((1,), jnp.int32),
            jax.ShapeDtypeStruct((1,), jnp.int32),
        ),
        in_specs=[_sm(), _sm()] + [_vm()] * 3 + [_any()],
        out_specs=(_any(), _vm(), _sm(), _sm()),
        scratch_shapes=_zscratch(d, n),
        input_output_aliases={5: 0},
        compiler_params=_params(8),
        cost_estimate=_cost(n * 0.375),
        name="fill_acc",
    )(cnts, other, slots, dx0, dx1, de)


def _write_kernel(map_ref, acc_in, mine_ref, got_ref, de_in, de, dg_out, acc, sem):
    acc[...] = acc_in[...]

    def add(j, carry):
        at = pl.ds(map_ref[0, j], 1)
        acc[at, :] = acc[at, :] + got_ref[pl.ds(j, 1), :]
        return carry

    lax.fori_loop(0, jnp.minimum(map_ref[0, 127], C2 - 1), add, 0)
    n = jnp.minimum(map_ref[0, 255], C)

    def put(j, carry):
        pltpu.make_async_copy(acc.at[pl.ds(j, 1)], de.at[pl.ds(map_ref[0, 128 + j], 1)], sem).start()
        return carry

    def done(j, carry):
        pltpu.make_async_copy(acc.at[pl.ds(j, 1)], de.at[pl.ds(0, 1)], sem).wait()
        return carry

    lax.fori_loop(0, n, put, 0)
    dg = mine_ref[C2 - 1:C2, :] + got_ref[C2 - 1:C2, :]
    dg_out[...] = dg.reshape(dg_out.shape)
    lax.fori_loop(0, n, done, 0)


def _write(where, acc, mine, got, de):
    vs, d = de.shape
    return pl.pallas_call(
        _write_kernel,
        out_shape=(jax.ShapeDtypeStruct((vs, d), F32), jax.ShapeDtypeStruct((d,), F32)),
        in_specs=[_sm()] + [_vm()] * 3 + [_any()],
        out_specs=(_any(), _vm()),
        scratch_shapes=[VMEM((C, d), F32), pltpu.SemaphoreType.DMA],
        input_output_aliases={4: 0},
        compiler_params=_params(6),
        cost_estimate=_cost(3),
        name="write_rows",
    )(where, acc, mine, got, de)


def solution(mesh):
    ntp = mesh.shape["tp"]
    ndp = mesh.shape["dp"]

    def swap(a, bit):
        return lax.ppermute(a, "tp", [(i, i ^ bit) for i in range(ntp)])

    def share(t):
        t2 = swap(t, 2)
        t1 = swap(t, 1)
        return t, t1, t2, swap(t2, 1)

    def p_terms(du, W, ts, vs):
        q, de = _p_terms(du, W, ts, vs)
        return de, (q[0], swap(q[1], 1), swap(q[2], 2), swap(q[3], 3))

    def body(ids, E, g, W, du, dres):
        vs, d = E.shape
        nk, t = ids.shape
        ts = t // ntp
        m = nk * ts
        g2 = g.reshape(1, d)

        tabs = share(_index_call(None, ids, E, ntp))
        de, ps = p_terms(du, W, ts, vs)
        pos, de = _pos(jnp.int32(0), ids, ntp, de)
        x, xl = _expand(pos, tabs, ts)
        u, dW, _, _, cnts, slots, where, de = _udw(x, g2, W, du, ids, ntp, de)
        dx, mine = _dx_sums(xl.reshape(m, d), ps, dres.reshape(m, d), g2, slots)
        got = swap(mine, 2)
        dx1 = swap(dx, 1)
        de = _zeros(de, AT_B, ZB)
        other = lax.ppermute(cnts, "dp", [(i, (i + 1) % ndp) for i in range(ndp)])
        de, acc, rounds, over = _acc(cnts, other, slots, dx, dx1, de, AT_R)
        dE, dg = _write(where, acc, mine, got, de)
        outs = u, xl, dE, dW, dg

        inputs = ids, E, W, du, dres, g2, rounds

        def again(c):
            ids, E, W, du, dres, g2, fl, left = lax.optimization_barrier((*inputs, c[0]))
            rounds = fl.reshape(())
            i0 = left - left

            def more(q):
                i, x, _, de = q
                pos, de = _pos(i, ids, ntp, de)
                return i + 1, *_expand(pos, share(_index_call(i, ids, E, ntp)), ts, x), de

            zeros = jnp.zeros((nk * t, d), BF16), jnp.zeros((nk, ts, d), BF16)
            de, ps = p_terms(du, W, ts, vs)
            _, x, xl, de = lax.while_loop(lambda q: q[0] < rounds, more, (i0, *zeros, de))
            u, dW, srow, rows, cs, _, _, de = _udw(x, g2, W, du, ids, ntp, de)
            dx, dg = _dx(xl.reshape(m, d), ps, dres.reshape(m, d), g2)
            dg2 = dg + swap(dg, 1)
            dg = (dg2 + swap(dg2, 2)).reshape(d)
            dE = _scatter(cs, rows, srow, share(dx), _zeros(de, AT_B, vs // ZR - AT_B), ts, nk)
            return i0, (u, xl, dE, dW, dg)

        _, outs = lax.while_loop(lambda c: c[0] > 0, again, (jnp.minimum(over.reshape(()), 1), outs))
        return outs

    return jax.shard_map(
        body,
        mesh=mesh,
        in_specs=(P("dp", None), P("tp", None), P(None), P(None, "tp"), P("dp", None, "tp"), P("dp", "tp", None)),
        out_specs=(P("dp", None, "tp"), P("dp", "tp", None), P(("dp", "tp"), None), P("dp", "tp"), P("dp")),
        check_vma=False,
    )
```

```python
import functools

import jax
import jax.numpy as jnp
from jax import lax
from jax.experimental import pallas as pl
from jax.experimental.pallas import tpu as pltpu
from jax.sharding import PartitionSpec as P


EPS = 1e-6
C = 56
G = 2
C2 = 32
CB = 256
ZR = 128
ZP, ZA, ZU, ZW, ZB = 8, 4, 22, 19, 4
AT_A, AT_U, AT_B, AT_R = ZP, ZP + ZA, ZP + ZA + ZU + ZW, ZP + ZA + ZU + ZW + ZB
TB = 64

F32 = jnp.float32
BF16 = jnp.bfloat16
VMEM = pltpu.VMEM


def _sm():
    return pl.BlockSpec(memory_space=pltpu.SMEM)


def _vm():
    return pl.BlockSpec(memory_space=pltpu.VMEM)


def _any():
    return pl.BlockSpec(memory_space=pl.ANY)


def _params(mb):
    return pltpu.CompilerParams(vmem_limit_bytes=mb << 20)


def _cost(us):
    return pl.CostEstimate(flops=int(us * 4_000_000_000), bytes_accessed=1_000_000, transcendentals=0)


def _iota(shape, dim):
    return lax.broadcasted_iota(jnp.int32, shape, dim).astype(F32)


def _me():
    return lax.axis_index("tp").astype(jnp.int32)


def _fill(z, o, sems, lo, first, n, wait):
    def step(i, carry):
        at = pl.multiple_of((lo + i) * ZR, ZR)
        c = pltpu.make_async_copy(z, o.at[pl.ds(at, ZR)], sems.at[i])
        c.wait() if wait else c.start()
        return carry

    lax.fori_loop(first, first + n, step, 0)


def _zscratch(d, n):
    return [VMEM((ZR, d), F32), pltpu.SemaphoreType.DMA((n,))]


def _column(row, b):
    w = (b * TB) // 128 * 128
    part = jnp.broadcast_to(row[:, w:w + 128], (TB, 128))
    hit = _iota((TB, 128), 1) == _iota((TB, 128), 0) + float(b * TB - w)
    return jnp.sum(jnp.where(hit, part, 0.0), axis=1, keepdims=True)


def _fold(a):
    return sum(a[8 * q:8 * q + 8] for q in range(1, TB // 8)) + a[:8]


def _ids_row(ids_ref):
    idsf = ids_ref[...].astype(F32)
    return jnp.concatenate([idsf[k:k + 1] for k in range(ids_ref.shape[0])], axis=1)


def _ranks(idr, idcs, vs, ntp, masks):
    ntok = idr.shape[1]
    lane = _iota((TB, ntok), 1)
    thr = _iota((TB, 128), 1) * float(vs)
    rank8 = jnp.zeros((8, ntok), F32)
    below8 = [jnp.zeros((8, 128), F32) for _ in masks]
    for b, idc in enumerate(idcs):
        i = [i for i, (_, blocks) in enumerate(masks) if blocks[b]][0]
        mask = masks[i][0]
        dup = (jnp.broadcast_to(idc, (TB, ntok)) == idr) & (lane < _iota((TB, ntok), 0) + float(b * TB))
        seen = jnp.max(jnp.where(dup, mask, 0.0), axis=1, keepdims=True)
        key = jnp.where(seen > 0.5, float(vs * ntp), idc)
        rank8 = rank8 + _fold(jnp.where(jnp.broadcast_to(key, (TB, ntok)) < idr, mask, 0.0))
        below8[i] = below8[i] + _fold(jnp.where(jnp.broadcast_to(key, (TB, 128)) < thr, 1.0, 0.0))
    return jnp.sum(rank8, axis=0, keepdims=True), [jnp.sum(b8, axis=0, keepdims=True) for b8 in below8]


def _table_slots(idr, idcs, vs, ntp):
    rank, (below,) = _ranks(idr, idcs, vs, ntp, [(jnp.ones_like(idr), [True] * len(idcs))])
    own_r = jnp.floor(idr * (1.0 / vs))
    start = jnp.zeros_like(rank)
    for d in range(ntp):
        start = jnp.where(own_r == float(d), below[:, d:d + 1], start)
    return own_r, rank - start, below


def _index_kernel(vs, ntp, first, *refs):
    if first:
        ids_ref, e_ref, tab_ref, buf, glv, gls, gsem, sem = refs
        base = 0.0
    else:
        c_ref, ids_ref, e_ref, tab_ref, buf, glv, gls, gsem, sem = refs
        base = (c_ref[0] * C).astype(F32)
    me = _me().astype(F32)
    lo = me * vs
    idr = _ids_row(ids_ref)
    ntok = idr.shape[1]
    idcs = [_column(idr, b) for b in range(ntok // TB)]
    own_r, slot_r, _ = _table_slots(idr, idcs, vs, ntp)
    my_r = jnp.where(own_r == me, slot_r, -1.0)
    slot_l = _iota((TB, 128), 1) + base
    acc = jnp.zeros((TB, 128), F32)
    for b, idc in enumerate(idcs):
        acc = jnp.maximum(acc, jnp.where(_column(my_r, b) == slot_l, idc - lo, 0.0))
    glv[...] = jnp.broadcast_to(jnp.max(acc, axis=0, keepdims=True), (8, 128)).astype(jnp.int32)
    cp = pltpu.make_async_copy(glv, gls, gsem)
    cp.start()
    cp.wait()

    def fetch(j, carry):
        g = pl.multiple_of((gls[0, j] >> 1) << 1, G)
        at = pl.multiple_of(j * G, G)
        pltpu.make_async_copy(e_ref.at[pl.ds(g, G)], buf.at[pl.ds(at, G)], sem).start()
        return carry

    lax.fori_loop(0, C, fetch, 0, unroll=True)
    hit = jnp.where(my_r == _iota((C, ntok), 0) + base, idr - lo, 0.0)
    want = jnp.max(hit, axis=1, keepdims=True)
    want = want - jnp.floor(want * (1.0 / G)) * G + _iota((C, 1), 0) * G
    sel = jnp.where(_iota((C, C * G), 1) == want, 1.0, 0.0).astype(BF16)
    pltpu.make_async_copy(e_ref.at[pl.ds(0, C * G)], buf, sem).wait()
    tab_ref[...] = jnp.dot(sel, buf[...], preferred_element_type=F32).astype(BF16)


def _index_call(chunk, ids, E, ntp):
    vs, d = E.shape
    first = chunk is None
    return pl.pallas_call(
        functools.partial(_index_kernel, vs, ntp, first),
        out_shape=jax.ShapeDtypeStruct((C, d), BF16),
        in_specs=([] if first else [_sm()]) + [_vm(), pl.BlockSpec(memory_space=pltpu.HBM)],
        out_specs=_vm(),
        scratch_shapes=[
            VMEM((C * G, d), BF16),
            VMEM((8, 128), jnp.int32),
            pltpu.SMEM((8, 128), jnp.int32),
            pltpu.SemaphoreType.DMA,
            pltpu.SemaphoreType.DMA,
        ],
        compiler_params=_params(8),
        cost_estimate=_cost(12),
        name="index_gather",
    )(*([] if first else [chunk.reshape(1)]), ids, E)


def _pos_kernel(vs, ntp, c_ref, ids_ref, de_in, pos_ref, de, z, sems):
    z[...] = jnp.zeros_like(z)
    _fill(z, de, sems, AT_A, 0, ZA, False)
    base = (c_ref[0] * C).astype(F32)
    idr = _ids_row(ids_ref)
    nb = idr.shape[1] // TB
    own_r, slot_r, _ = _table_slots(idr, [_column(idr, b) for b in range(nb)], vs, ntp)
    rel = (own_r.astype(jnp.int32) ^ _me()).astype(F32)
    pos = jnp.where((slot_r >= base) & (slot_r < base + C), rel * C + slot_r - base, -1.0)
    for b in range(nb):
        pos_ref[b * TB:(b + 1) * TB, :] = _column(pos, b)
    _fill(z, de, sems, AT_A, 0, ZA, True)


def _pos(chunk, ids, ntp, de):
    vs, d = de.shape
    ntok = ids.shape[0] * ids.shape[1]
    return pl.pallas_call(
        functools.partial(_pos_kernel, vs, ntp),
        out_shape=(jax.ShapeDtypeStruct((ntok, 1), F32), jax.ShapeDtypeStruct(de.shape, F32)),
        in_specs=[_sm(), _vm(), _any()],
        out_specs=(_vm(), _any()),
        scratch_shapes=_zscratch(d, ZA),
        input_output_aliases={2: 1},
        compiler_params=_params(6),
        cost_estimate=_cost(3),
        name="positions",
    )(chunk.reshape(1), ids, de)


def _slots(vs, ntp, ids_ref, srow_ref, list_ref, cnt_ref, slot_ref, map_ref):
    mei = _me()
    me = mei.astype(F32)
    lo = me * vs
    nk, t = ids_ref.shape
    ntok = nk * t
    nb = ntok // TB
    ts = t // ntp
    idr = _ids_row(ids_ref)
    idcs = [_column(idr, b) for b in range(nb)]
    own_r, slot_r, below = _table_slots(idr, idcs, vs, ntp)
    my_r = jnp.where(own_r == me, slot_r, -1.0)
    cnt = jnp.zeros((1, 1), F32)
    mx = jnp.zeros((1, 1), F32)
    for d in range(ntp):
        nd = below[:, d + 1:d + 2] - below[:, d:d + 1]
        cnt = jnp.where(me == float(d), nd, cnt)
        mx = jnp.maximum(mx, nd)
    srow_ref[...] = my_r

    part = lax.broadcasted_iota(jnp.int32, (1, ntok), 1) // ts % ntp
    chips = [
        (jnp.where(part // 2 == c, 1.0, 0.0), [b * TB // ts % ntp // 2 == c for b in range(nb)])
        for c in range(ntp // 2)
    ]
    rank2, below2 = _ranks(idr, idcs, vs, ntp, chips)
    start2 = jnp.zeros_like(rank2)
    cnt2 = jnp.zeros((1, 1), F32)
    mx2 = jnp.zeros((1, 1), F32)
    for c, (chip, _) in enumerate(chips):
        for d in range(ntp):
            ld = below2[c][:, d:d + 1]
            nd = below2[c][:, d + 1:d + 2] - ld
            start2 = jnp.where((own_r == float(d)) & (chip > 0.5), ld, start2)
            if d // 2 != c:
                cnt2 = jnp.where(me == float(d), nd, cnt2)
                mx2 = jnp.maximum(mx2, nd)
    slot2_r = rank2 - start2
    lane1 = lax.broadcasted_iota(jnp.int32, (1, 128), 1)
    over = jnp.where((mx > C) | (mx2 > C2 - 1), 1.0, 0.0)
    rounds = jnp.floor((mx + C - 1.0) * (1.0 / C))
    cnts = jnp.where(lane1 == 0, rounds, jnp.where(lane1 == 1, cnt, jnp.where(lane1 == 2, over, cnt2)))
    cnt_ref[...] = cnts.astype(jnp.int32)
    sums_r = [jnp.where(own_r == (mei ^ o).astype(F32), slot2_r, -1.0) for o in (2, 3)]
    rows = [jnp.zeros((1, nk * ts), F32)] * 4
    for q in range(ntp):
        at = [slice(k * t + q * ts, k * t + (q + 1) * ts) for k in range(nk)]
        mine = jnp.concatenate([my_r[:, w] for w in at], axis=1)
        sums = [jnp.concatenate([r[:, w] for w in at], axis=1) for r in sums_r]
        own, sib = me == float(q), me == float(q ^ 1)
        rows = [
            jnp.where(own, mine, rows[0]), jnp.where(sib, mine, rows[1]),
            jnp.where(own, sums[0], rows[2]), jnp.where(own, sums[1], rows[3]),
        ]
    for j, r in enumerate(rows):
        slot_ref[j:j + 1, :] = r
    far = (part // 2).astype(F32) != jnp.floor(me * 0.5)
    got_r = jnp.where(far & (own_r == me), slot2_r, -1.0)
    acc2 = jnp.zeros((TB, 128), F32)
    slot_j = _iota((TB, 128), 1)
    full = jnp.zeros((8, ntok), F32)
    lane8 = _iota((8, ntok), 1)
    for b in range(nb):
        my_c = _column(my_r, b)
        acc2 = jnp.maximum(acc2, jnp.where(_column(got_r, b) == slot_j, my_c, 0.0))
        for q in range(TB // 8):
            s = slice(8 * q, 8 * q + 8)
            full = jnp.maximum(full, jnp.where(my_c[s] == lane8, idcs[b][s] - lo, 0.0))
    full = jnp.max(full, axis=0, keepdims=True)
    list_ref[...] = full.astype(jnp.int32)
    slots = jnp.minimum(jnp.max(acc2, axis=0, keepdims=True), C - 1.0)
    many = jnp.where(lane1 == 127, cnt2, slots)
    mine = jnp.where(lane1 == 127, cnt, full[:, :128])
    map_ref[...] = jnp.concatenate([many, mine], axis=1).astype(jnp.int32)


def _expand_kernel(ts, acc, *refs):
    if acc:
        x_in, pos, t0, t1, t2, t3, x_out, xl_out = refs
    else:
        pos, t0, t1, t2, t3, x_out, xl_out = refs
    oh = jnp.where(pos[...] == _iota((pos.shape[0], 4 * C), 1), 1.0, 0.0).astype(BF16)
    for c in range(x_out.shape[1] // CB):
        s = slice(c * CB, (c + 1) * CB)
        tab = jnp.concatenate([t[:, s] for t in (t0, t1, t2, t3)], axis=0)
        tot = jnp.dot(oh, tab, preferred_element_type=F32)
        if acc:
            tot = tot + x_in[:, s].astype(F32)
        x_out[:, s] = tot.astype(BF16)
    t = 4 * ts
    for k in range(x_out.shape[0] // t):
        at = pl.multiple_of(k * t + _me() * ts, ts)
        xl_out[k] = x_out[pl.ds(at, ts), :]


def _expand(pos, tabs, ts, x=None):
    ntok, d = pos.shape[0], tabs[0].shape[1]
    ins = ([x] if x is not None else []) + [pos, *tabs]
    return pl.pallas_call(
        functools.partial(_expand_kernel, ts, x is not None),
        out_shape=(jax.ShapeDtypeStruct((ntok, d), BF16), jax.ShapeDtypeStruct((ntok // (4 * ts), ts, d), BF16)),
        in_specs=[_vm()] * len(ins),
        out_specs=(_vm(), _vm()),
        compiler_params=_params(12),
        cost_estimate=_cost(3),
        name="expand",
    )(*ins)


def _p_kernel(ts, du_ref, w_ref, *refs):
    outs, (de, dur, z, sems) = refs[:-4], refs[-4:]
    nk = du_ref.shape[0]

    @pl.when(pl.program_id(0) == 0)
    def _():
        z[...] = jnp.zeros_like(z)
        for k in range(nk):
            for r in range(4):
                at = pl.multiple_of((_me() ^ r) * ts, ts)
                dur[pl.ds((r * nk + k) * ts, ts), :] = du_ref[k, pl.ds(at, ts), :]
        _fill(z, de, sems, 0, 0, ZP, False)

    out = lax.dot_general(dur[...], w_ref[...], (((1,), (1,)), ((), ())), preferred_element_type=F32)
    for i, o in enumerate(outs):
        o[...] = out[i * nk * ts:(i + 1) * nk * ts].astype(BF16)

    @pl.when(pl.program_id(0) == pl.num_programs(0) - 1)
    def _():
        _fill(z, de, sems, 0, 0, ZP, True)


def _p_terms(du, W, ts, vs):
    nk, t, f = du.shape
    d = W.shape[0]
    cb = 3 * CB
    out = pl.pallas_call(
        functools.partial(_p_kernel, ts),
        out_shape=(jax.ShapeDtypeStruct((nk * ts, d), BF16),) * 4 + (jax.ShapeDtypeStruct((vs, d), F32),),
        grid=(d // cb,),
        in_specs=[pl.BlockSpec((nk, t, f), lambda i: (0, 0, 0)), pl.BlockSpec((cb, f), lambda i: (i, 0))],
        out_specs=(pl.BlockSpec((nk * ts, cb), lambda i: (0, i)),) * 4 + (_any(),),
        scratch_shapes=[VMEM((nk * t, f), BF16)] + _zscratch(d, ZP),
        compiler_params=_params(20),
        cost_estimate=_cost(5),
        name="p_terms",
    )(du, W)
    return out[:4], out[4]


def _zero_kernel(lo, n, de_in, o, z, sems):
    z[...] = jnp.zeros_like(z)
    _fill(z, o, sems, lo, 0, n, False)
    _fill(z, o, sems, lo, 0, n, True)


def _zeros(de, lo, n):
    vs, d = de.shape
    return pl.pallas_call(
        functools.partial(_zero_kernel, lo, n),
        out_shape=jax.ShapeDtypeStruct((vs, d), F32),
        in_specs=[_any()],
        out_specs=_any(),
        scratch_shapes=_zscratch(d, n),
        input_output_aliases={0: 0},
        compiler_params=_params(4),
        cost_estimate=_cost(n * 0.375),
    )(de)


def _dx_rows(x, p0, p1, p2, p3, dres, g, dx):
    rows = 16
    tot = None
    for b in range(dx.shape[0] // rows):
        s = slice(b * rows, (b + 1) * rows)
        xf = x[s].astype(F32)
        rs = lax.rsqrt(jnp.mean(xf * xf, axis=-1, keepdims=True) + EPS)
        nh = xf * rs
        dn = (p0[s].astype(F32) + p1[s].astype(F32)) + (p2[s].astype(F32) + p3[s].astype(F32))
        gdn = g[...].astype(F32) * dn
        out = dres[s].astype(F32) + rs * (gdn - nh * jnp.mean(nh * gdn, axis=-1, keepdims=True))
        dx[s] = out.astype(BF16)
        part = jnp.sum(dn * nh, axis=0, keepdims=True)
        tot = part if tot is None else tot + part
    return tot


def _dx_kernel(*refs):
    refs[-1][...] = _dx_rows(*refs[:-1])


def _dx(x, ps, dres, g):
    m, d = x.shape
    return pl.pallas_call(
        _dx_kernel,
        out_shape=(
            jax.ShapeDtypeStruct((m, d), BF16),
            jax.ShapeDtypeStruct((1, d), F32),
        ),
        in_specs=[_vm()] * 7,
        out_specs=(_vm(), _vm()),
        compiler_params=_params(12),
        cost_estimate=_cost(2),
        name="dx_form",
    )(x, *ps, dres, g)


def _dx_sums_kernel(x, p0, p1, p2, p3, dres, g, slot_ref, dx, mine, out, got, send, recv):
    sib = _me() ^ 1
    barrier = pltpu.get_barrier_semaphore()
    pl.semaphore_signal(barrier, inc=1, device_id={"tp": sib}, device_id_type=pl.DeviceIdType.MESH)
    dg = _dx_rows(x, p0, p1, p2, p3, dres, g, dx)
    j = _iota((C2, dx.shape[0]), 0)
    last = lax.broadcasted_iota(jnp.int32, (C2, CB), 0) == C2 - 1

    def sums(i, to):
        oh = jnp.where(slot_ref[i:i + 1, :] == j, 1.0, 0.0).astype(BF16)
        for c in range(to.shape[1] // CB):
            s = slice(c * CB, (c + 1) * CB)
            to[:, s] = jnp.where(last, dg[:, s], jnp.dot(oh, dx[:, s], preferred_element_type=F32))

    sums(3, out)
    pl.semaphore_wait(barrier, 1)
    copy = pltpu.make_async_remote_copy(
        src_ref=out, dst_ref=got, send_sem=send, recv_sem=recv,
        device_id={"tp": sib}, device_id_type=pl.DeviceIdType.MESH,
    )
    copy.start()
    sums(2, mine)
    copy.wait()
    mine[...] = mine[...] + got[...]


def _dx_sums(x, ps, dres, g, slots):
    m, d = x.shape
    return pl.pallas_call(
        _dx_sums_kernel,
        out_shape=(jax.ShapeDtypeStruct((m, d), BF16), jax.ShapeDtypeStruct((C2, d), F32)),
        in_specs=[_vm()] * 8,
        out_specs=(_vm(), _vm()),
        scratch_shapes=[VMEM((C2, d), F32), VMEM((C2, d), F32), pltpu.SemaphoreType.DMA, pltpu.SemaphoreType.DMA],
        compiler_params=pltpu.CompilerParams(vmem_limit_bytes=12 << 20, collective_id=0, has_side_effects=True),
        cost_estimate=_cost(3),
        name="dx_sums",
    )(x, *ps, dres, g, slots)


def _udw_kernel(per, vs, ntp, x_ref, g_ref, w_ref, du_ref, ids_ref, de_in, *refs):
    u_ref, dw_ref, *slot_refs, de, n, z, sems = refs
    i = pl.program_id(0)
    nk, t, f = du_ref.shape
    cb = dw_ref.shape[0]

    @pl.when(i == 0)
    def _():
        z[...] = jnp.zeros_like(z)
        _fill(z, de, sems, AT_U, 0, ZU, False)
        _slots(vs, ntp, ids_ref, *slot_refs)
        rows = 64
        for b in range(n.shape[0] // rows):
            s = slice(b * rows, (b + 1) * rows)
            xf = x_ref[s].astype(F32)
            rs = lax.rsqrt(jnp.mean(xf * xf, axis=-1, keepdims=True) + EPS)
            n[s] = (xf * rs * g_ref[...].astype(F32)).astype(BF16)
        for c in range(f // CB):
            s = slice(c * CB, (c + 1) * CB)
            out = jnp.dot(n[...], w_ref[:, s], preferred_element_type=F32).astype(BF16)
            for k in range(nk):
                u_ref[k, :, s] = out[k * t:(k + 1) * t]

    _fill(z, de, sems, AT_U, ZU + i * per, jnp.minimum(per, ZW - i * per), False)
    blk = n[:, pl.ds(pl.multiple_of(i * cb, 128), cb)]
    dw_ref[...] = lax.dot_general(
        blk, du_ref[...].reshape(nk * t, f), (((0,), (0,)), ((), ())), preferred_element_type=F32
    )

    @pl.when(i == pl.num_programs(0) - 1)
    def _():
        _fill(z, de, sems, AT_U, 0, ZU + ZW, True)


def _udw(x, g, W, du, ids, ntp, de):
    nk, t, f = du.shape
    ntok, d = x.shape
    cb = d // 6
    steps = d // cb
    return pl.pallas_call(
        functools.partial(_udw_kernel, -(-ZW // steps), de.shape[0], ntp),
        out_shape=(
            jax.ShapeDtypeStruct((nk, t, f), BF16),
            jax.ShapeDtypeStruct((d, f), F32),
            jax.ShapeDtypeStruct((1, ntok), F32),
            jax.ShapeDtypeStruct((1, ntok), jnp.int32),
            jax.ShapeDtypeStruct((1, 128), jnp.int32),
            jax.ShapeDtypeStruct((4, ntok // ntp), F32),
            jax.ShapeDtypeStruct((1, 256), jnp.int32),
            jax.ShapeDtypeStruct(de.shape, F32),
        ),
        grid=(steps,),
        in_specs=[_vm()] * 5 + [_any()],
        out_specs=(
            pl.BlockSpec((nk, t, f), lambda i: (0, 0, 0)), pl.BlockSpec((cb, f), lambda i: (i, 0)),
            *[_vm()] * 5, _any(),
        ),
        scratch_shapes=[VMEM((ntok, d), BF16)] + _zscratch(d, ZU + ZW),
        input_output_aliases={5: 7},
        compiler_params=_params(20),
        cost_estimate=_cost(20),
        name="u_dw",
    )(x, g, W, du, ids, de)


def _scatter_kernel(ts, nk, cnt_ref, list_ref, srow_ref, *refs):
    pieces, (de_in, de, dx, acc, sem) = refs[:-5], refs[-5:]
    ntok = nk * 4 * ts
    for k in range(nk):
        for r in range(4):
            at = pl.multiple_of(k * 4 * ts + (_me() ^ r) * ts, ts)
            dx[pl.ds(at, ts), :] = pieces[r][k * ts:(k + 1) * ts, :]
    cnt = cnt_ref[0, 1]

    def chunk(i, carry):
        base = i * C
        slot = (lax.broadcasted_iota(jnp.int32, (C, ntok), 0) + base).astype(F32)
        oh = jnp.where(slot == srow_ref[...], 1.0, 0.0).astype(BF16)
        for c in range(acc.shape[1] // CB):
            s = slice(c * CB, (c + 1) * CB)
            acc[:, s] = jnp.dot(oh, dx[:, s], preferred_element_type=F32)
        here = jnp.minimum(cnt - base, C)

        def put(j, c2):
            row = list_ref[0, base + j]
            pltpu.make_async_copy(acc.at[pl.ds(j, 1)], de.at[pl.ds(row, 1)], sem).start()
            return c2

        def done(j, c2):
            pltpu.make_async_copy(acc.at[pl.ds(j, 1)], de.at[pl.ds(0, 1)], sem).wait()
            return c2

        lax.fori_loop(0, here, put, 0)
        lax.fori_loop(0, here, done, 0)
        return carry

    lax.fori_loop(0, (cnt + C - 1) // C, chunk, 0)


def _scatter(cnts, rows, srow, pieces, de, ts, nk):
    vs, d = de.shape
    ntok = srow.shape[1]
    return pl.pallas_call(
        functools.partial(_scatter_kernel, ts, nk),
        out_shape=jax.ShapeDtypeStruct((vs, d), F32),
        in_specs=[_sm(), _sm(), _vm()] + [_vm()] * len(pieces) + [_any()],
        out_specs=_any(),
        scratch_shapes=[VMEM((ntok, d), BF16), VMEM((C, d), F32), pltpu.SemaphoreType.DMA],
        input_output_aliases={3 + len(pieces): 0},
        compiler_params=_params(16),
        cost_estimate=_cost(3),
        name="scatter_rows",
    )(cnts, rows, srow, *pieces, de)


def _acc_kernel(lo, n, cnt_ref, oth_ref, slot_ref, dx0, dx1, de_in, de, acc, rounds, over, z, sems):
    z[...] = jnp.zeros_like(z)
    _fill(z, de, sems, lo, 0, n, False)
    rounds[0] = jnp.maximum(cnt_ref[0, 0], oth_ref[0, 0])
    over[0] = jnp.maximum(cnt_ref[0, 2], oth_ref[0, 2])
    m = dx0.shape[0]
    j = _iota((C, m), 0)
    ohs = [jnp.where(slot_ref[i:i + 1, :] == j, 1.0, 0.0).astype(BF16) for i in (0, 1)]
    for c in range(acc.shape[1] // CB):
        s = slice(c * CB, (c + 1) * CB)
        tot = jnp.dot(ohs[0], dx0[:, s], preferred_element_type=F32)
        acc[:, s] = tot + jnp.dot(ohs[1], dx1[:, s], preferred_element_type=F32)
    _fill(z, de, sems, lo, 0, n, True)


def _acc(cnts, other, slots, dx0, dx1, de, lo):
    vs, d = de.shape
    n = vs // ZR - lo
    return pl.pallas_call(
        functools.partial(_acc_kernel, lo, n),
        out_shape=(
            jax.ShapeDtypeStruct((vs, d), F32),
            jax.ShapeDtypeStruct((C, d), F32),
            jax.ShapeDtypeStruct((1,), jnp.int32),
            jax.ShapeDtypeStruct((1,), jnp.int32),
        ),
        in_specs=[_sm(), _sm()] + [_vm()] * 3 + [_any()],
        out_specs=(_any(), _vm(), _sm(), _sm()),
        scratch_shapes=_zscratch(d, n),
        input_output_aliases={5: 0},
        compiler_params=_params(8),
        cost_estimate=_cost(n * 0.375),
        name="fill_acc",
    )(cnts, other, slots, dx0, dx1, de)


def _write_kernel(map_ref, acc_in, mine_ref, got_ref, de_in, de, dg_out, acc, sem):
    acc[...] = acc_in[...]

    def add(j, carry):
        at = pl.ds(map_ref[0, j], 1)
        acc[at, :] = acc[at, :] + got_ref[pl.ds(j, 1), :]
        return carry

    lax.fori_loop(0, jnp.minimum(map_ref[0, 127], C2 - 1), add, 0)
    n = jnp.minimum(map_ref[0, 255], C)

    def put(j, carry):
        pltpu.make_async_copy(acc.at[pl.ds(j, 1)], de.at[pl.ds(map_ref[0, 128 + j], 1)], sem).start()
        return carry

    def done(j, carry):
        pltpu.make_async_copy(acc.at[pl.ds(j, 1)], de.at[pl.ds(0, 1)], sem).wait()
        return carry

    lax.fori_loop(0, n, put, 0)
    dg = mine_ref[C2 - 1:C2, :] + got_ref[C2 - 1:C2, :]
    dg_out[...] = dg.reshape(dg_out.shape)
    lax.fori_loop(0, n, done, 0)


def _write(where, acc, mine, got, de):
    vs, d = de.shape
    return pl.pallas_call(
        _write_kernel,
        out_shape=(jax.ShapeDtypeStruct((vs, d), F32), jax.ShapeDtypeStruct((d,), F32)),
        in_specs=[_sm()] + [_vm()] * 3 + [_any()],
        out_specs=(_any(), _vm()),
        scratch_shapes=[VMEM((C, d), F32), pltpu.SemaphoreType.DMA],
        input_output_aliases={4: 0},
        compiler_params=_params(6),
        cost_estimate=_cost(3),
        name="write_rows",
    )(where, acc, mine, got, de)


def solution(mesh):
    ntp = mesh.shape["tp"]
    ndp = mesh.shape["dp"]

    def swap(a, bit):
        return lax.ppermute(a, "tp", [(i, i ^ bit) for i in range(ntp)])

    def share(t):
        t2 = swap(t, 2)
        t1 = swap(t, 1)
        return t, t1, t2, swap(t2, 1)

    def p_terms(du, W, ts, vs):
        q, de = _p_terms(du, W, ts, vs)
        return de, (q[0], swap(q[1], 1), swap(q[2], 2), swap(q[3], 3))

    def body(ids, E, g, W, du, dres):
        vs, d = E.shape
        nk, t = ids.shape
        ts = t // ntp
        m = nk * ts
        g2 = g.reshape(1, d)

        tabs = share(_index_call(None, ids, E, ntp))
        de, ps = p_terms(du, W, ts, vs)
        pos, de = _pos(jnp.int32(0), ids, ntp, de)
        x, xl = _expand(pos, tabs, ts)
        u, dW, _, _, cnts, slots, where, de = _udw(x, g2, W, du, ids, ntp, de)
        dx, mine = _dx_sums(xl.reshape(m, d), ps, dres.reshape(m, d), g2, slots)
        got = swap(mine, 2)
        dx1 = swap(dx, 1)
        de = _zeros(de, AT_B, ZB)
        other = lax.ppermute(cnts, "dp", [(i, (i + 1) % ndp) for i in range(ndp)])
        de, acc, rounds, over = _acc(cnts, other, slots, dx, dx1, de, AT_R)
        dE, dg = _write(where, acc, mine, got, de)
        outs = u, xl, dE, dW, dg

        inputs = ids, E, W, du, dres, g2, rounds

        def again(c):
            ids, E, W, du, dres, g2, fl, left = lax.optimization_barrier((*inputs, c[0]))
            rounds = fl.reshape(())
            i0 = left - left

            def more(q):
                i, x, _, de = q
                pos, de = _pos(i, ids, ntp, de)
                return i + 1, *_expand(pos, share(_index_call(i, ids, E, ntp)), ts, x), de

            zeros = jnp.zeros((nk * t, d), BF16), jnp.zeros((nk, ts, d), BF16)
            de, ps = p_terms(du, W, ts, vs)
            _, x, xl, de = lax.while_loop(lambda q: q[0] < rounds, more, (i0, *zeros, de))
            u, dW, srow, rows, cs, _, _, de = _udw(x, g2, W, du, ids, ntp, de)
            dx, dg = _dx(xl.reshape(m, d), ps, dres.reshape(m, d), g2)
            dg2 = dg + swap(dg, 1)
            dg = (dg2 + swap(dg2, 2)).reshape(d)
            dE = _scatter(cs, rows, srow, share(dx), _zeros(de, AT_B, vs // ZR - AT_B), ts, nk)
            return i0, (u, xl, dE, dW, dg)

        _, outs = lax.while_loop(lambda c: c[0] > 0, again, (jnp.minimum(over.reshape(()), 1), outs))
        return outs

    return jax.shard_map(
        body,
        mesh=mesh,
        in_specs=(P("dp", None), P("tp", None), P(None), P(None, "tp"), P("dp", None, "tp"), P("dp", "tp", None)),
        out_specs=(P("dp", None, "tp"), P("dp", "tp", None), P(("dp", "tp"), None), P("dp", "tp"), P("dp")),
        check_vma=False,
    )
```
